768 devices in a mesh: face: 6 (over z_lo), fy: 8 (over x, core), fx: 16 (over y, z_hi).
Axes of the slice: x: 4, y: 8, z: 12 (z_hi: 2, z_lo: 6; z = z_hi * 6 + z_lo), core: 2. Of those that a mesh axis runs over, the one named last changes fastest.
Arguments:
- state: float32 [6, 128, 128, 192], P('face', 'fy', 'fx'), may hold values from -6 to 6
- jacobian: float32 [6, 128, 128], P('face', 'fy', 'fx'), may hold values from 0.5 to 2
- metric_diag: float32 [2, 6, 128, 128], P(None, 'face', 'fy', 'fx'), may hold values from 0.6 to 1.4
- metric_cross: float32 [6, 128, 128], P('face', 'fy', 'fx'), may hold values from -0.3 to 0.3
- coriolis: float32 [6, 128, 128], P('face', 'fy', 'fx'), may hold values from -2 to 2
- nbr_face: int32 [6, 4], replicated, may hold values from 0 to 5, as said below
- nbr_edge: int32 [6, 4], replicated, may hold values from 0 to 3, as said below
Outputs:
- updated: float32 [6, 128, 128, 192], P('face', 'fy', 'fx')
The draws below stay inside these ranges and needn't reach their ends.
Inputs may be any that keep to these rules, and one draw needn't show every extreme that they name: Edge e of a face is 0 south (row 0), 1 east (last column), 2 north (last row), 3 west (column 0). Edge e of face f is glued to edge nbr_edge[f, e] of face nbr_face[f, e], and that edge back to it; the 6 faces are glued as the surface of a cube, three faces at each corner, the two glued edges running in opposite senses when both are read counterclockwise. `nbr_edge`: see nbr_face.
All inputs are finite; a program needn't handle non-finite values.
Results may differ from the reference program's by a relative error of at most 0.0001.
Values sent between devices are 32-bit elements; how exact they have to be, the bound alone decides.
No kernel may reach another device: no remote copies, remote signals or barrier semaphores. Data moves between devices by JAX's collectives and lax.ppermute only.
A program may use at most 32 MiB of HBM per device.

```python
import math
import jax
import jax.numpy as jnp
import numpy as np
from jax import lax

FACES = 6
LEV = 64
NN = 128


def glued_tables(key):
    base_key = jax.random.fold_in(key, 4051)
    relabel = jax.random.permutation(jax.random.fold_in(base_key, 1), 6).astype(jnp.int32)
    quarter = jax.random.randint(jax.random.fold_in(base_key, 2), (6,), 0, 4).astype(jnp.int32)
    drawn_face = jnp.asarray(np.array([[5, 1, 4, 3], [5, 2, 4, 0], [5, 3, 4, 1], [5, 0, 4, 2], [0, 1, 2, 3], [2, 1, 0, 3]]), jnp.int32)
    drawn_edge = jnp.asarray(np.array([[2, 3, 0, 1], [1, 3, 1, 1], [0, 3, 2, 1], [3, 3, 3, 1], [2, 2, 2, 2], [0, 0, 0, 0]]), jnp.int32)
    old_face = jnp.broadcast_to(jnp.arange(6, dtype=jnp.int32)[:, None], (6, 4))
    old_edge = jnp.broadcast_to(jnp.arange(4, dtype=jnp.int32)[None, :], (6, 4))
    new_face = relabel[old_face]
    new_edge = (old_edge + quarter[old_face]) % 4
    glued_face = relabel[drawn_face]
    glued_edge = (drawn_edge + quarter[drawn_face]) % 4
    faces_out = jnp.zeros((6, 4), jnp.int32).at[new_face, new_edge].set(glued_face)
    edges_out = jnp.zeros((6, 4), jnp.int32).at[new_face, new_edge].set(glued_edge)
    return (faces_out, edges_out)


def draw_nbr_face(key, part):
    return glued_tables(key)[0]


def draw_nbr_edge(key, part):
    return glued_tables(key)[1]


def level_of(key, shape, pieces, smallest, top_value):
    gain, own = 1.0, jax.random.fold_in(key, 6)
    for axis_at, blocks in pieces:
        draws = jnp.exp(jax.random.uniform(jax.random.fold_in(own, axis_at), (blocks,), jnp.float32, smallest / len(pieces), top_value / len(pieces)))
        gain = gain * jnp.repeat(draws, shape[axis_at] // blocks).reshape([-1 if axis == axis_at else 1 for axis in range(len(shape))])
    return gain


def bell_draw(key, dims, scale, most, split=(), held_as=jnp.bfloat16):
    level = level_of(key, dims, split, -0.22, 0.18) if split else 1.0
    values = jax.random.normal(key, dims, jnp.float32) * scale * level
    return jnp.minimum(jnp.maximum(values, -most), most).astype(held_as)


def setup_inputs(seed: int = 0) -> dict:
    splits = jax.random.split(jax.random.key(seed), 8)
    return {
        "state": bell_draw(splits[0], (FACES, NN, NN, 3 * LEV), 1.0, 6.0, ((0, 6), (1, 8), (2, 16)), jnp.float32),
        "jacobian": jnp.clip(jnp.exp(math.log(2.0) - 1.3862944 * jax.random.uniform(splits[1], (FACES, NN, NN), jnp.float32) ** level_of(splits[1], (FACES, NN, NN), ((0, 6), (1, 8), (2, 16)), -0.2, 0.2)), 0.5, 2.0),
        "metric_diag": jnp.clip(1.0 + 0.08 * jax.random.normal(splits[2], (2, FACES, NN, NN), jnp.float32), 0.6, 1.4),
        "metric_cross": jnp.clip(jax.random.uniform(splits[3], (FACES, NN, NN), jnp.float32, -0.3, 0.3) * level_of(splits[3], (FACES, NN, NN), ((0, 6), (1, 8), (2, 16)), -0.4, 0.0), -0.3, 0.3),
        "coriolis": jnp.clip(jax.random.uniform(splits[4], (FACES, NN, NN), jnp.float32, -2.0, 2.0) * level_of(splits[4], (FACES, NN, NN), ((0, 6), (1, 8), (2, 16)), -0.4, 0.0), -2.0, 2.0),
        "nbr_face": draw_nbr_face(jax.random.fold_in(splits[7], 71), 0),
        "nbr_edge": draw_nbr_edge(jax.random.fold_in(splits[7], 71), 0),
    }


time_step = 0.05
hyper_coeff = 0.0005

def deriv_table():
    gll_nodes = np.array([-1.0, -1.0 / np.sqrt(5.0), 1.0 / np.sqrt(5.0), 1.0])
    bary_weights = np.ones(4)
    for j in range(4):
        for m in range(4):
            if m != j:
                bary_weights[j] = bary_weights[j] / (gll_nodes[j] - gll_nodes[m])
    matrix = np.zeros((4, 4))
    for i in range(4):
        for j in range(4):
            if i != j:
                matrix[i, j] = bary_weights[j] / bary_weights[i] / (gll_nodes[i] - gll_nodes[j])
        matrix[i, i] = -np.sum(matrix[i])
    return matrix

def along_x(values):
    face_count, row_count, col_count, chan_count = values.shape
    blocks = values.reshape(face_count, row_count, col_count // 4, 4, chan_count)
    result = jnp.einsum('jk,abekc->abejc', jnp.asarray(deriv_table(), jnp.float32), blocks, precision=lax.Precision.HIGHEST)
    return result.reshape(values.shape)

def along_y(values):
    face_count, row_count, col_count, chan_count = values.shape
    blocks = values.reshape(face_count, row_count // 4, 4, col_count, chan_count)
    result = jnp.einsum('ik,aekxc->aeixc', jnp.asarray(deriv_table(), jnp.float32), blocks, precision=lax.Precision.HIGHEST)
    return result.reshape(values.shape)

def mass_of(jacobian):
    weights = jnp.asarray([1.0 / 6.0, 5.0 / 6.0, 5.0 / 6.0, 1.0 / 6.0], jnp.float32)
    row_weight = jnp.tile(weights, jacobian.shape[1] // 4)
    col_weight = jnp.tile(weights, jacobian.shape[2] // 4)
    return jacobian * row_weight[None, :, None] * col_weight[None, None, :]

def tendency(state, geometry, planet):
    volume, metric_xx, metric_yy, metric_xy = geometry
    levels = state.shape[-1] // 3
    wind_u = state[..., :levels]
    wind_v = state[..., levels:2 * levels]
    temper = state[..., 2 * levels:]
    contra_u = metric_xx * wind_u + metric_xy * wind_v
    contra_v = metric_xy * wind_u + metric_yy * wind_v
    energy = 0.5 * (wind_u * contra_u + wind_v * contra_v) + temper
    xderivs = along_x(jnp.concatenate([wind_v, temper, energy], -1))
    yderivs = along_y(jnp.concatenate([wind_u, temper, energy], -1))
    absolute = (xderivs[..., :levels] - yderivs[..., :levels]) / volume + planet
    tend_u = absolute * volume * contra_v - xderivs[..., 2 * levels:]
    tend_v = -absolute * volume * contra_u - yderivs[..., 2 * levels:]
    tend_t = -(contra_u * xderivs[..., levels:2 * levels] + contra_v * yderivs[..., levels:2 * levels])
    return state + time_step * jnp.concatenate([tend_u, tend_v, tend_t], -1)

def laplace(values, geometry):
    volume, metric_xx, metric_yy, metric_xy = geometry
    grad_x = along_x(values)
    grad_y = along_y(values)
    flux_x = volume * (metric_xx * grad_x + metric_xy * grad_y)
    flux_y = volume * (metric_xy * grad_x + metric_yy * grad_y)
    return (along_x(flux_x) + along_y(flux_y)) / volume

def combine(values, axis):
    length = values.shape[axis] - 2
    positions = jnp.arange(length)
    leading = (positions % 4 == 0).astype(jnp.float32)
    trailing = (positions % 4 == 3).astype(jnp.float32)
    broad_shape = [1, 1, 1, 1]
    broad_shape[axis] = length
    leading = leading.reshape(broad_shape)
    trailing = trailing.reshape(broad_shape)
    middle = lax.slice_in_dim(values, 1, length + 1, axis=axis)
    previous = lax.slice_in_dim(values, 0, length, axis=axis)
    following = lax.slice_in_dim(values, 2, length + 2, axis=axis)
    return middle + leading * previous + trailing * following

def rotate(segment, quarter, levels):
    cosine = ((quarter == 0).astype(jnp.float32) - (quarter == 2).astype(jnp.float32))[..., None]
    sine_part = ((quarter == 1).astype(jnp.float32) - (quarter == 3).astype(jnp.float32))[..., None]
    wind_u = segment[..., :levels]
    wind_v = segment[..., levels:2 * levels]
    return jnp.concatenate([cosine * wind_u - sine_part * wind_v, sine_part * wind_u + cosine * wind_v, segment[..., 2 * levels:]], -1)

def assemble(values, vector, nbr_face, nbr_edge):
    padded = jnp.pad(values, ((0, 0), (1, 1), (1, 1), (0, 0)))
    summed = combine(combine(padded, 1), 2)
    side_nodes = summed.shape[1]
    levels = summed.shape[-1] // 3
    rim_strips = jnp.stack([summed[:, 0, :], summed[:, :, side_nodes - 1], summed[:, side_nodes - 1, ::-1], summed[:, ::-1, 0]], axis=1)
    partner = rim_strips[nbr_face, nbr_edge][:, :, ::-1]
    if vector:
        quarter = (jnp.arange(4, dtype=jnp.int32)[None, :] - nbr_edge + 2) % 4
        partner = rotate(partner, quarter[:, :, None], levels)
    result = summed.at[:, 0, :].add(partner[:, 0])
    result = result.at[:, :, side_nodes - 1].add(partner[:, 1])
    result = result.at[:, side_nodes - 1, :].add(partner[:, 2, ::-1])
    result = result.at[:, :, 0].add(partner[:, 3, ::-1])
    return result

def reference(state, jacobian, metric_diag, metric_cross, coriolis, nbr_face, nbr_edge):
    node_mass = mass_of(jacobian)[..., None]
    total_mass = assemble(node_mass, False, nbr_face, nbr_edge)
    geometry = (jacobian[..., None], metric_diag[0][..., None], metric_diag[1][..., None], metric_cross[..., None])
    raw = tendency(state, geometry, coriolis[..., None])
    sectioned = assemble(node_mass * raw, True, nbr_face, nbr_edge) / total_mass
    first_lap = assemble(node_mass * laplace(sectioned, geometry), True, nbr_face, nbr_edge) / total_mass
    second_lap = assemble(node_mass * laplace(first_lap, geometry), True, nbr_face, nbr_edge) / total_mass
    return sectioned - hyper_coeff * second_lap
```

```python
import functools

import jax
import jax.numpy as jnp
import numpy as np
from jax import lax
from jax.experimental import pallas as pl
from jax.experimental.pallas import tpu as pltpu
from jax.sharding import PartitionSpec as P

time_step = 0.05
hyper_coeff = 0.0005

FACES = 6
ROWS = 128
LANES = 128
EDGES = 4


def deriv_table():
    gll_nodes = np.array([-1.0, -1.0 / np.sqrt(5.0), 1.0 / np.sqrt(5.0), 1.0])
    bary_weights = np.ones(4)
    for j in range(4):
        for m in range(4):
            if m != j:
                bary_weights[j] = bary_weights[j] / (gll_nodes[j] - gll_nodes[m])
    matrix = np.zeros((4, 4))
    for i in range(4):
        for j in range(4):
            if i != j:
                matrix[i, j] = bary_weights[j] / bary_weights[i] / (gll_nodes[i] - gll_nodes[j])
        matrix[i, i] = -np.sum(matrix[i])
    return matrix


def deriv_operands():
    table = deriv_table()
    along_x = np.kron(np.eye(32), table.T)
    along_y = np.kron(np.kron(np.eye(4), table.T), np.eye(8))
    return along_x.astype(np.float32), along_y.astype(np.float32)


def roll(values, shift, axis):
    return pltpu.roll(values, shift % values.shape[axis], axis)


def iota(shape, dim):
    return lax.broadcasted_iota(jnp.int32, shape, dim)


def dot(a, b):
    return jnp.dot(a, b, precision=lax.Precision.HIGHEST, preferred_element_type=jnp.float32)


def dot_t(a, b):
    return lax.dot_general(
        a,
        b,
        (((1,), (1,)), ((), ())),
        precision=lax.Precision.HIGHEST,
        preferred_element_type=jnp.float32,
    )


def stacked(parts, axis=0):
    return jnp.concatenate(parts, axis=axis)


def gll_weight(position):
    return jnp.where((position % 4 == 0) | (position % 4 == 3), 1.0 / 6.0, 5.0 / 6.0)


def mass_weight():
    lane = iota((1, LANES), 1)
    return gll_weight(lane // 8) * gll_weight(lane % 8)


def in_face(field):
    lane = iota((ROWS, LANES), 1)
    col_block = iota((ROWS, LANES), 0) % 16
    c = lane % 8
    r = lane // 8
    before = roll(field, 1, 1)
    after = roll(field, -1, 1)
    before_block = roll(roll(field, 1, 0), -7, 1)
    after_block = roll(roll(field, -1, 0), 7, 1)
    summed = field + jnp.where(
        c == 4, before, jnp.where((c == 0) & (col_block > 0), before_block, 0.0)
    )
    summed = summed + jnp.where(
        c == 3, after, jnp.where((c == 7) & (col_block < 15), after_block, 0.0)
    )
    above = roll(summed, 8, 1)
    below = roll(summed, -8, 1)
    edge_rows = jnp.zeros((16, LANES), jnp.float32)
    above_block = stacked([edge_rows, above[: ROWS - 16]])
    below_block = stacked([below[16:], edge_rows])
    total = summed + jnp.where(
        r == 0, above_block, jnp.where(r % 4 == 0, above, 0.0)
    )
    return total + jnp.where(r == 15, below_block, jnp.where(r % 4 == 3, below, 0.0))


def rim_tables(edge):
    lane = iota((LANES, LANES), 0)
    k = iota((LANES, LANES), 1)
    count = 16 if edge in (0, 2) else 8
    block = iota((count, LANES), 0)
    at = iota((count, LANES), 1)
    if edge == 0:
        hit, mask = lane == k % 8, block == at // 8
    elif edge == 1:
        hit, mask = lane == 8 * (k % 16) + 7, block == at // 16
    elif edge == 2:
        hit, mask = lane == 127 - k % 8, block == 15 - at // 8
    else:
        hit, mask = lane == 8 * (15 - k % 16), block == 7 - at // 16
    return jnp.where(hit, 1.0, 0.0), jnp.where(mask, 1.0, 0.0)


def rim_rows(edge):
    if edge == 0:
        return pl.ds(0, 16)
    if edge == 1:
        return pl.ds(15, 8, 16)
    if edge == 2:
        return pl.ds(112, 16)
    return pl.ds(0, 8, 16)


def shifted_rows(edge, channel):
    rows = rim_rows(edge)
    return pl.ds(rows.start + ROWS * channel, rows.size, rows.stride)


def turned(u, v, quarter):
    quarter = quarter % 4
    if quarter == 0:
        return u, v
    if quarter == 1:
        return -v, u
    if quarter == 2:
        return -u, -v
    return v, -u


def put_rims(summed_ref, channels, nbr_ref, face, send_ref):
    rims = []
    for edge in range(EDGES):
        spread, mask = rim_tables(edge)
        count = mask.shape[0]
        rows = stacked([summed_ref[shifted_rows(edge, ch), :] for ch in range(channels)])
        spread_rows = dot(rows, spread)
        vectors = [
            jnp.sum(spread_rows[ch * count : (ch + 1) * count] * mask, axis=0, keepdims=True)
            for ch in range(channels)
        ]
        u, v = turned(vectors[0], vectors[1], -edge)
        pad = [jnp.zeros((8 - channels, LANES), jnp.float32)]
        rims.append(stacked([u, v, *vectors[2:], *pad]))
    for other in range(FACES):
        slot = jnp.zeros((8, LANES), jnp.float32)
        for edge in range(EDGES):
            glued = jnp.where(nbr_ref[face, edge] == other, 1.0, 0.0).astype(jnp.float32)
            slot = slot + glued * rims[edge]
        send_ref[8 * other : 8 * other + 8, :] = slot


def add_rims(total_ref, channels, nbr_ref, face, got_ref):
    flip = jnp.where(iota((LANES, LANES), 0) + iota((LANES, LANES), 1) == 127, 1.0, 0.0)
    got = stacked(
        [got_ref[pl.ds(pl.multiple_of(8 * nbr_ref[face, edge], 8), 8), :] for edge in range(EDGES)]
    )
    got = dot(got, flip)
    for edge in range(EDGES):
        rim = got[8 * edge : 8 * edge + 8]
        u, v = turned(rim[0:1], rim[1:2], edge + 2)
        vectors = [u, v] + [rim[ch : ch + 1] for ch in range(2, channels)]
        spread, mask = rim_tables(edge)
        count = mask.shape[0]
        placed = dot_t(stacked([vector * mask for vector in vectors]), spread)
        for ch in range(channels):
            rows = shifted_rows(edge, ch)
            total_ref[rows, :] = total_ref[rows, :] + placed[ch * count : (ch + 1) * count]


def pack_kernel(state_ref, jac_ref, diag_ref, cross_ref, cor_ref, out_ref):
    turned_state = jnp.transpose(state_ref[...])
    for part in range(3):
        out_ref[pl.ds(part, 64, 8), :] = turned_state[64 * part : 64 * part + 64]
    spread = jnp.where(iota((8, LANES), 1) % 8 == iota((8, LANES), 0), 1.0, 0.0)
    mask = jnp.where(iota((16, LANES), 1) // 8 == iota((16, LANES), 0), 1.0, 0.0)
    fields = [jac_ref[...], diag_ref[0], diag_ref[1], cross_ref[...], cor_ref[...]]
    lines = dot(stacked(fields), spread)
    for k in range(5):
        line = jnp.sum(lines[16 * k : 16 * k + 16] * mask, axis=0, keepdims=True)
        out_ref[pl.ds(3 + k, 64, 8), :] = jnp.broadcast_to(line, (64, LANES))


def first_kernel(nbr_ref, own_ref, other_ref, dx_ref, dy_ref, summed_ref, geometry_ref, send_ref):
    core = lax.axis_index("fy") % 2
    face = lax.axis_index("face")
    fields = []
    for k in range(8):
        own = own_ref[pl.ds(k, 64, 8), :]
        other = other_ref[pl.ds(k, 64, 8), :]
        even = jnp.where(core == 0, own, other)
        odd = jnp.where(core == 0, other, own)
        pieces = []
        for x in range(4):
            pieces += [even[16 * x : 16 * x + 16], odd[16 * x : 16 * x + 16]]
        fields.append(stacked(pieces))
    u, v, t, volume, m_xx, m_yy, m_xy, planet = fields
    contra_u = m_xx * u + m_xy * v
    contra_v = m_xy * u + m_yy * v
    energy = 0.5 * (u * contra_u + v * contra_v) + t
    x_derivs = dot(stacked([v, t, energy]), dx_ref[...])
    y_derivs = dot(stacked([u, t, energy]), dy_ref[...])
    dx_v, dx_t, dx_e = x_derivs[:ROWS], x_derivs[ROWS : 2 * ROWS], x_derivs[2 * ROWS :]
    dy_u, dy_t, dy_e = y_derivs[:ROWS], y_derivs[ROWS : 2 * ROWS], y_derivs[2 * ROWS :]
    absolute = (dx_v - dy_u) / volume + planet
    mass = mass_weight() * volume
    raw_u = u + time_step * (absolute * volume * contra_v - dx_e)
    raw_v = v + time_step * (-absolute * volume * contra_u - dy_e)
    raw_t = t - time_step * (contra_u * dx_t + contra_v * dy_t)
    for ch, field in enumerate([mass * raw_u, mass * raw_v, mass * raw_t, mass]):
        summed_ref[ROWS * ch : ROWS * ch + ROWS, :] = in_face(field)
    for k, field in enumerate([volume, m_xx, m_yy, m_xy]):
        geometry_ref[ROWS * k : ROWS * k + ROWS, :] = field
    put_rims(summed_ref, 4, nbr_ref, face, send_ref)


def laplace(fields, geometry_ref, dx_ref, dy_ref):
    volume, m_xx, m_yy, m_xy = [
        geometry_ref[ROWS * k : ROWS * k + ROWS, :] for k in range(4)
    ]
    along_x, along_y = dx_ref[...], dy_ref[...]
    values = stacked(fields)
    grad_x, grad_y = dot(values, along_x), dot(values, along_y)
    flux_x, flux_y = [], []
    for ch in range(3):
        part = slice(ROWS * ch, ROWS * ch + ROWS)
        flux_x.append(volume * (m_xx * grad_x[part] + m_xy * grad_y[part]))
        flux_y.append(volume * (m_xy * grad_x[part] + m_yy * grad_y[part]))
    spread = dot(stacked(flux_x), along_x) + dot(stacked(flux_y), along_y)
    mass = mass_weight() * volume
    return [mass * (spread[ROWS * ch : ROWS * ch + ROWS] / volume) for ch in range(3)]


def second_kernel(
    nbr_ref, got_ref, summed_ref, geometry_ref, dx_ref, dy_ref,
    sectioned_ref, mass_ref, next_ref, send_ref, total_ref,
):
    face = lax.axis_index("face")
    total_ref[...] = summed_ref[...]
    add_rims(total_ref, 4, nbr_ref, face, got_ref)
    total_mass = total_ref[3 * ROWS : 4 * ROWS, :]
    mass_ref[...] = total_mass
    fields = [total_ref[ROWS * ch : ROWS * ch + ROWS, :] / total_mass for ch in range(3)]
    for ch in range(3):
        sectioned_ref[ROWS * ch : ROWS * ch + ROWS, :] = fields[ch]
    for ch, field in enumerate(laplace(fields, geometry_ref, dx_ref, dy_ref)):
        next_ref[ROWS * ch : ROWS * ch + ROWS, :] = in_face(field)
    put_rims(next_ref, 3, nbr_ref, face, send_ref)


def third_kernel(
    nbr_ref, got_ref, summed_ref, mass_ref, geometry_ref, dx_ref, dy_ref,
    next_ref, send_ref, total_ref,
):
    face = lax.axis_index("face")
    total_ref[...] = summed_ref[...]
    add_rims(total_ref, 3, nbr_ref, face, got_ref)
    fields = [total_ref[ROWS * ch : ROWS * ch + ROWS, :] / mass_ref[...] for ch in range(3)]
    for ch, field in enumerate(laplace(fields, geometry_ref, dx_ref, dy_ref)):
        next_ref[ROWS * ch : ROWS * ch + ROWS, :] = in_face(field)
    put_rims(next_ref, 3, nbr_ref, face, send_ref)


def last_kernel(nbr_ref, got_ref, summed_ref, mass_ref, sectioned_ref, out_ref, total_ref):
    face = lax.axis_index("face")
    core = lax.axis_index("fy") % 2
    total_ref[...] = summed_ref[...]
    add_rims(total_ref, 3, nbr_ref, face, got_ref)
    for ch in range(3):
        part = pl.ds(ROWS * ch, ROWS)
        total_ref[part, :] = (
            sectioned_ref[part, :] - hyper_coeff * (total_ref[part, :] / mass_ref[...])
        )
    for x in range(4):
        for ch in range(3):
            start = pl.multiple_of(ROWS * ch + 32 * x + 16 * core, 16)
            out_ref[16 * x : 16 * x + 16, LANES * ch : LANES * ch + LANES] = total_ref[
                pl.ds(start, 16), :
            ]


def unpack_kernel(got_ref, out_ref):
    levels = got_ref[...]
    columns = stacked([levels[:, LANES * ch : LANES * ch + LANES] for ch in range(3)])
    out_ref[...] = jnp.transpose(columns)


def f32(*shape):
    return jax.ShapeDtypeStruct(shape, jnp.float32)


VMEM = pl.BlockSpec(memory_space=pltpu.VMEM)
SMEM = pl.BlockSpec(memory_space=pltpu.SMEM)


def call(kernel, outs, ins, scratch=(), name=None):
    return pl.pallas_call(
        kernel,
        out_shape=outs,
        in_specs=ins,
        out_specs=jax.tree.map(lambda _: VMEM, outs),
        scratch_shapes=scratch,
        name=name,
    )


def level_groups():
    return [
        [(8 * face + 2 * x + core) * 16 + fx for x in range(4) for fx in range(16)]
        for face in range(FACES)
        for core in range(2)
    ]


def per_device(state, jacobian, metric_diag, metric_cross, coriolis, nbr_face, nbr_edge):
    axes = ("face", "fy", "fx")
    groups = level_groups()
    along_x, along_y = deriv_operands()
    total = pltpu.VMEM((4 * ROWS, LANES), jnp.float32)
    total_3 = pltpu.VMEM((3 * ROWS, LANES), jnp.float32)

    packed = call(pack_kernel, f32(512, LANES), [VMEM] * 5, name="pack")(
        state.reshape(128, 192), jacobian[0], metric_diag[:, 0], metric_cross[0], coriolis[0]
    )
    own = lax.all_to_all(
        packed.reshape(64, 8, LANES), axes, 0, 0, axis_index_groups=groups, tiled=True
    )
    other = lax.ppermute(own, "fy", [(i, i ^ 1) for i in range(8)])

    def across(send):
        return lax.all_to_all(send.reshape(FACES, 8, LANES), "face", 0, 0, tiled=True).reshape(
            8 * FACES, LANES
        )

    send = f32(8 * FACES, LANES)
    summed, geometry, out = call(
        first_kernel,
        [f32(4 * ROWS, LANES), f32(4 * ROWS, LANES), send],
        [SMEM] + [VMEM] * 4,
        name="first",
    )(nbr_face, own.reshape(512, LANES), other.reshape(512, LANES), along_x, along_y)
    sectioned, total_mass, summed, out = call(
        second_kernel,
        [f32(3 * ROWS, LANES), f32(ROWS, LANES), f32(3 * ROWS, LANES), send],
        [SMEM] + [VMEM] * 5,
        [total],
        name="second",
    )(nbr_face, across(out), summed, geometry, along_x, along_y)
    summed, out = call(
        third_kernel,
        [f32(3 * ROWS, LANES), send],
        [SMEM] + [VMEM] * 6,
        [total_3],
        name="third",
    )(nbr_face, across(out), summed, total_mass, geometry, along_x, along_y)
    updated = call(
        last_kernel, f32(64, 3 * LANES), [SMEM] + [VMEM] * 4, [total_3], name="last"
    )(nbr_face, across(out), summed, total_mass, sectioned)
    back = lax.all_to_all(
        updated.reshape(64, 1, 3 * LANES), axes, 0, 0, axis_index_groups=groups, tiled=True
    )
    nodes = call(unpack_kernel, f32(128, 192), [VMEM], name="unpack")(
        back.reshape(64, 3 * LANES)
    )
    return nodes.reshape(1, 16, 8, 192)


def solution(mesh):
    return jax.shard_map(
        per_device,
        mesh=mesh,
        in_specs=(
            P("face", "fy", "fx", None),
            P("face", "fy", "fx"),
            P(None, "face", "fy", "fx"),
            P("face", "fy", "fx"),
            P("face", "fy", "fx"),
            P(),
            P(),
        ),
        out_specs=P("face", "fy", "fx", None),
        check_vma=False,
    )
```

```python
import functools

import jax
import jax.numpy as jnp
import numpy as np
from jax import lax
from jax.experimental import pallas as pl
from jax.experimental.pallas import tpu as pltpu
from jax.sharding import PartitionSpec as P

time_step = 0.05
hyper_coeff = 0.0005

FACES = 6
ROWS = 128
LANES = 128
EDGES = 4
RING = (3, 2, 1, 0)
RING_ROWS = 64
SLOT = 64


def deriv_table():
    gll_nodes = np.array([-1.0, -1.0 / np.sqrt(5.0), 1.0 / np.sqrt(5.0), 1.0])
    bary_weights = np.ones(4)
    for j in range(4):
        for m in range(4):
            if m != j:
                bary_weights[j] = bary_weights[j] / (gll_nodes[j] - gll_nodes[m])
    matrix = np.zeros((4, 4))
    for i in range(4):
        for j in range(4):
            if i != j:
                matrix[i, j] = bary_weights[j] / bary_weights[i] / (gll_nodes[i] - gll_nodes[j])
        matrix[i, i] = -np.sum(matrix[i])
    return matrix


def deriv_operands():
    table = deriv_table()
    along_x = np.kron(np.eye(32), table.T)
    along_y = np.kron(np.kron(np.eye(4), table.T), np.eye(8))
    return along_x.astype(np.float32), along_y.astype(np.float32)


def roll(values, shift, axis):
    return pltpu.roll(values, shift % values.shape[axis], axis)


def iota(shape, dim):
    return lax.broadcasted_iota(jnp.int32, shape, dim)


def dot(a, b):
    return jnp.dot(a, b, precision=lax.Precision.HIGHEST, preferred_element_type=jnp.float32)


def dot_t(a, b):
    return lax.dot_general(
        a,
        b,
        (((1,), (1,)), ((), ())),
        precision=lax.Precision.HIGHEST,
        preferred_element_type=jnp.float32,
    )


def stacked(parts, axis=0):
    return jnp.concatenate(parts, axis=axis)


def gll_weight(position):
    return jnp.where((position % 4 == 0) | (position % 4 == 3), 1.0 / 6.0, 5.0 / 6.0)


def mass_weight():
    lane = iota((1, LANES), 1)
    return gll_weight(lane // 8) * gll_weight(lane % 8)


def beside(field):
    return (
        roll(field, 1, 1),
        roll(field, -1, 1),
        roll(roll(field, 1, 0), -7, 1),
        roll(roll(field, -1, 0), 7, 1),
    )


def summed_along_x(field):
    lane = iota(field.shape, 1)
    block = iota(field.shape, 0) % 16
    c = lane % 8
    before, after, before_block, after_block = beside(field)
    summed = field + jnp.where(
        c == 4, before, jnp.where((c == 0) & (block > 0), before_block, 0.0)
    )
    return summed + jnp.where(
        c == 3, after, jnp.where((c == 7) & (block < 15), after_block, 0.0)
    )


def in_face(field):
    summed = summed_along_x(field)
    r = iota(field.shape, 1) // 8
    above = roll(summed, 8, 1)
    below = roll(summed, -8, 1)
    edge_rows = jnp.zeros((16, LANES), jnp.float32)
    above_block = stacked([edge_rows, above[: ROWS - 16]])
    below_block = stacked([below[16:], edge_rows])
    total = summed + jnp.where(r == 0, above_block, jnp.where(r % 4 == 0, above, 0.0))
    return total + jnp.where(r == 15, below_block, jnp.where(r % 4 == 3, below, 0.0))


def in_strips(field):
    summed = summed_along_x(field)
    r = iota(field.shape, 1) // 8
    return (
        summed
        + jnp.where(r == 4, roll(summed, 8, 1), 0.0)
        + jnp.where(r == 3, roll(summed, -8, 1), 0.0)
    )


def between_strips(field):
    block = iota(field.shape, 0) % 16
    c = iota(field.shape, 1) % 8
    _, _, before_block, after_block = beside(field)
    first = (c == 0) & (block == 0)
    last = (c == 7) & (block == 15)
    return jnp.where(first, before_block, jnp.where(last, after_block, 0.0))


def rim_tables(edge, reverse=False):
    lane = iota((LANES, LANES), 0)
    k = iota((LANES, LANES), 1)
    count = 16 if edge in (0, 2) else 8
    block = iota((count, LANES), 0)
    at = iota((count, LANES), 1)
    if reverse:
        k, at = 127 - k, 127 - at
    if edge == 0:
        hit, mask = lane == k % 8, block == at // 8
    elif edge == 1:
        hit, mask = lane == 8 * (k % 16) + 7, block == at // 16
    elif edge == 2:
        hit, mask = lane == 127 - k % 8, block == 15 - at // 8
    else:
        hit, mask = lane == 8 * (15 - k % 16), block == 7 - at // 16
    return jnp.where(hit, 1.0, 0.0), jnp.where(mask, 1.0, 0.0)


def rim_rows(edge, base=0):
    if edge == 0:
        return pl.ds(base, 16)
    if edge == 1:
        return pl.ds(base + 15, 8, 16)
    if edge == 2:
        return pl.ds(base + 112, 16)
    return pl.ds(base, 8, 16)


def turned(u, v, quarter):
    quarter = quarter % 4
    if quarter == 0:
        return u, v
    if quarter == 1:
        return -v, u
    if quarter == 2:
        return -u, -v
    return v, -u


def block_sums(values, mask):
    count = mask.shape[0]
    return [
        jnp.sum(values[n : n + count] * mask, axis=0, keepdims=True)
        for n in range(0, values.shape[0], count)
    ]


def join(face_ref, ring, channels):
    south, south_mask = rim_tables(0)
    spread, mask = rim_tables(0, reverse=True)
    up = block_sums(dot(stacked(ring), spread), mask)
    down = []
    for edge in range(EDGES):
        spread, mask = rim_tables(edge, reverse=True)
        rows = stacked([face_ref[rim_rows(edge, ROWS * ch), :] for ch in range(channels)])
        line = block_sums(dot(rows, spread), mask)
        down.append([*turned(line[0], line[1], 2 - edge), *line[2:]])
    down_rows = [down[edge][ch] * south_mask for ch in range(channels) for edge in RING]
    placed = dot_t(stacked(down_rows), south)
    ring_total = [
        ring[ch] + between_strips(ring[ch]) + placed[RING_ROWS * ch : RING_ROWS * ch + RING_ROWS]
        for ch in range(channels)
    ]
    for n, edge in enumerate(RING):
        line = [up[EDGES * ch + n] for ch in range(channels)]
        line = [*turned(line[0], line[1], edge + 2), *line[2:]]
        spread, mask = rim_tables(edge)
        count = mask.shape[0]
        placed = dot_t(stacked([part * mask for part in line]), spread)
        for ch in range(channels):
            rows = rim_rows(edge, ROWS * ch)
            face_ref[rows, :] = face_ref[rows, :] + placed[ch * count : (ch + 1) * count]
    return ring_total


def pack_kernel(state_ref, jac_ref, diag_ref, cross_ref, cor_ref, out_ref):
    turned_state = jnp.transpose(state_ref[...])
    for part in range(3):
        out_ref[pl.ds(part, 64, 8), :] = turned_state[64 * part : 64 * part + 64]
    spread = jnp.where(iota((16, LANES), 1) // 8 == iota((16, LANES), 0), 1.0, 0.0)
    mask = jnp.where(iota((8, LANES), 1) % 8 == iota((8, LANES), 0), 1.0, 0.0)
    fields = [jac_ref[...], diag_ref[0], diag_ref[1], cross_ref[...], cor_ref[...]]
    for k, line in enumerate(block_sums(dot(stacked(fields), spread), mask)):
        out_ref[pl.ds(3 + k, 64, 8), :] = jnp.broadcast_to(line, (64, LANES))


def strip_of(edge, fields_ref):
    rows = stacked([fields_ref[rim_rows(edge, ROWS * k), :] for k in range(8)])
    if edge == 0:
        return rows
    lane = iota((LANES, LANES), 0)
    m = iota((LANES, LANES), 1)
    if edge == 2:
        nodes = dot(rows, jnp.where(lane == 127 - m, 1.0, 0.0))
        return dot(jnp.where((lane // 16 == m // 16) & (lane % 16 == 15 - m % 16), 1.0, 0.0), nodes)
    near = m < 64
    if edge == 1:
        source = 8 * (m % 8) + 7 - m // 8
    else:
        source = 8 * (7 - m % 8) + m // 8
    halves = [
        dot(rows, jnp.where(near & (lane == source + 64 * half), 1.0, 0.0)) for half in range(2)
    ]
    j = lane % 16 if edge == 1 else 15 - lane % 16
    wanted = 64 * (j % 2) + 8 * (lane // 16) + j // 2
    return dot(jnp.where(m == wanted, 1.0, 0.0), stacked(halves))


def put_strips(fields_ref, nbr_ref, face, send_ref):
    near = iota((16, LANES), 1) < 64
    for edge in range(EDGES):
        rows = strip_of(edge, fields_ref)
        u, v, t, mass, volume, m_xx, m_yy, m_xy = [rows[16 * k : 16 * k + 16] for k in range(8)]
        u, v = turned(u, v, -edge)
        if edge % 2:
            m_xx, m_yy, m_xy = m_yy, m_xx, -m_xy
        slot = [
            jnp.where(near, low, roll(high, 64, 1))
            for low, high in ((u, v), (t, mass), (volume, m_xx), (m_yy, m_xy))
        ]
        start = pl.multiple_of(SLOT * nbr_ref[face, edge], SLOT)
        send_ref[pl.ds(start, SLOT), :] = stacked(slot)


def got_strips(nbr_ref, face, got_ref):
    near = iota((RING_ROWS, LANES), 1) < 64
    pairs = [[] for _ in range(4)]
    for edge in RING:
        start = pl.multiple_of(SLOT * nbr_ref[face, edge], SLOT)
        slot = got_ref[pl.ds(start, SLOT), :]
        for n in range(4):
            pairs[n].append(slot[16 * n : 16 * n + 16])
    fields = []
    for pair in pairs:
        rows = stacked(pair)
        fields += [jnp.where(near, rows, 0.0), jnp.where(near, roll(rows, 64, 1), 0.0)]
    fields[3] = jnp.where(near, fields[3], 1.0)
    fields[4] = jnp.where(near, fields[4], 1.0)
    return fields


def first_kernel(nbr_ref, own_ref, other_ref, dx_ref, dy_ref, fields_ref, send_ref):
    core = lax.axis_index("fy") % 2
    face = lax.axis_index("face")
    fields = []
    for k in range(8):
        own = own_ref[pl.ds(k, 64, 8), :]
        other = other_ref[pl.ds(k, 64, 8), :]
        even = jnp.where(core == 0, own, other)
        odd = jnp.where(core == 0, other, own)
        pieces = []
        for x in range(4):
            pieces += [even[16 * x : 16 * x + 16], odd[16 * x : 16 * x + 16]]
        fields.append(stacked(pieces))
    u, v, t, volume, m_xx, m_yy, m_xy, planet = fields
    contra_u = m_xx * u + m_xy * v
    contra_v = m_xy * u + m_yy * v
    energy = 0.5 * (u * contra_u + v * contra_v) + t
    x_derivs = dot(stacked([v, t, energy]), dx_ref[...])
    y_derivs = dot(stacked([u, t, energy]), dy_ref[...])
    dx_v, dx_t, dx_e = x_derivs[:ROWS], x_derivs[ROWS : 2 * ROWS], x_derivs[2 * ROWS :]
    dy_u, dy_t, dy_e = y_derivs[:ROWS], y_derivs[ROWS : 2 * ROWS], y_derivs[2 * ROWS :]
    absolute = (dx_v - dy_u) / volume + planet
    mass = mass_weight() * volume
    raw_u = u + time_step * (absolute * volume * contra_v - dx_e)
    raw_v = v + time_step * (-absolute * volume * contra_u - dy_e)
    raw_t = t - time_step * (contra_u * dx_t + contra_v * dy_t)
    sums = [in_face(field) for field in (mass * raw_u, mass * raw_v, mass * raw_t, mass)]
    for k, field in enumerate([*sums, volume, m_xx, m_yy, m_xy]):
        fields_ref[ROWS * k : ROWS * k + ROWS, :] = field
    put_strips(fields_ref, nbr_ref, face, send_ref)


def laplace(fields, geometry, along_x, along_y):
    volume, m_xx, m_yy, m_xy = geometry
    count = volume.shape[0]
    values = stacked(fields)
    grad_x, grad_y = dot(values, along_x), dot(values, along_y)
    flux_x, flux_y = [], []
    for ch in range(3):
        part = slice(count * ch, count * ch + count)
        flux_x.append(volume * (m_xx * grad_x[part] + m_xy * grad_y[part]))
        flux_y.append(volume * (m_xy * grad_x[part] + m_yy * grad_y[part]))
    spread = dot(stacked(flux_x), along_x) + dot(stacked(flux_y), along_y)
    mass = mass_weight() * volume
    return [mass * (spread[count * ch : count * ch + count] / volume) for ch in range(3)]


def second_kernel(nbr_ref, got_ref, fields_ref, dx_ref, dy_ref, out_ref, total_ref):
    face = lax.axis_index("face")
    core = lax.axis_index("fy") % 2
    along_x, along_y = dx_ref[...], dy_ref[...]
    ring_fields = got_strips(nbr_ref, face, got_ref)
    geometry = [
        stacked([fields_ref[ROWS * k : ROWS * k + ROWS, :], ring_fields[k]]) for k in range(4, 8)
    ]

    total_ref[...] = fields_ref[: 4 * ROWS, :]
    ring = join(total_ref, ring_fields[:4], 4)
    face_mass = total_ref[3 * ROWS : 4 * ROWS, :]
    total_mass = stacked([face_mass, ring[3]])
    sectioned = [total_ref[ROWS * ch : ROWS * ch + ROWS, :] / face_mass for ch in range(3)]
    fields = [stacked([sectioned[ch], ring[ch] / ring[3]]) for ch in range(3)]
    for step in range(2):
        lapped = laplace(fields, geometry, along_x, along_y)
        for ch in range(3):
            total_ref[ROWS * ch : ROWS * ch + ROWS, :] = in_face(lapped[ch][:ROWS])
        ring = join(total_ref, [in_strips(field[ROWS:]) for field in lapped], 3)
        if step == 0:
            fields = [
                stacked([total_ref[ROWS * ch : ROWS * ch + ROWS, :], ring[ch]]) / total_mass
                for ch in range(3)
            ]
    for ch in range(3):
        part = slice(ROWS * ch, ROWS * ch + ROWS)
        total_ref[part, :] = sectioned[ch] - hyper_coeff * (total_ref[part, :] / face_mass)
    for x in range(4):
        for ch in range(3):
            start = pl.multiple_of(ROWS * ch + 32 * x + 16 * core, 16)
            out_ref[16 * x : 16 * x + 16, LANES * ch : LANES * ch + LANES] = total_ref[
                pl.ds(start, 16), :
            ]


def unpack_kernel(got_ref, out_ref):
    levels = got_ref[...]
    columns = stacked([levels[:, LANES * ch : LANES * ch + LANES] for ch in range(3)])
    out_ref[...] = jnp.transpose(columns)


def f32(*shape):
    return jax.ShapeDtypeStruct(shape, jnp.float32)


VMEM = pl.BlockSpec(memory_space=pltpu.VMEM)
SMEM = pl.BlockSpec(memory_space=pltpu.SMEM)


def call(kernel, outs, ins, scratch=(), name=None):
    return pl.pallas_call(
        kernel,
        out_shape=outs,
        in_specs=ins,
        out_specs=jax.tree.map(lambda _: VMEM, outs),
        scratch_shapes=scratch,
        name=name,
    )


def level_groups():
    return [
        [(8 * face + 2 * x + core) * 16 + fx for x in range(4) for fx in range(16)]
        for face in range(FACES)
        for core in range(2)
    ]


def per_device(state, jacobian, metric_diag, metric_cross, coriolis, nbr_face, nbr_edge):
    axes = ("face", "fy", "fx")
    groups = level_groups()
    along_x, along_y = deriv_operands()

    packed = call(pack_kernel, f32(512, LANES), [VMEM] * 5, name="pack")(
        state.reshape(128, 192),
        jacobian[0].T,
        metric_diag[:, 0].transpose(0, 2, 1),
        metric_cross[0].T,
        coriolis[0].T,
    )
    own = lax.all_to_all(
        packed.reshape(64, 8, LANES), axes, 0, 0, axis_index_groups=groups, tiled=True
    )
    other = lax.ppermute(own, "fy", [(i, i ^ 1) for i in range(8)])
    fields, send = call(
        first_kernel,
        [f32(8 * ROWS, LANES), f32(SLOT * FACES, LANES)],
        [SMEM] + [VMEM] * 4,
        name="first",
    )(nbr_face, own.reshape(512, LANES), other.reshape(512, LANES), along_x, along_y)
    got = lax.all_to_all(send.reshape(FACES, SLOT, LANES), "face", 0, 0, tiled=True)
    updated = call(
        second_kernel,
        f32(64, 3 * LANES),
        [SMEM] + [VMEM] * 4,
        [pltpu.VMEM((4 * ROWS, LANES), jnp.float32)],
        name="second",
    )(nbr_face, got.reshape(SLOT * FACES, LANES), fields, along_x, along_y)
    back = lax.all_to_all(
        updated.reshape(64, 1, 3 * LANES), axes, 0, 0, axis_index_groups=groups, tiled=True
    )
    nodes = call(unpack_kernel, f32(128, 192), [VMEM], name="unpack")(
        back.reshape(64, 3 * LANES)
    )
    return nodes.reshape(1, 16, 8, 192)


def solution(mesh):
    return jax.shard_map(
        per_device,
        mesh=mesh,
        in_specs=(
            P("face", "fy", "fx", None),
            P("face", "fy", "fx"),
            P(None, "face", "fy", "fx"),
            P("face", "fy", "fx"),
            P("face", "fy", "fx"),
            P(),
            P(),
        ),
        out_specs=P("face", "fy", "fx", None),
        check_vma=False,
    )
```

```python
import functools

import jax
import jax.numpy as jnp
import numpy as np
from jax import lax
from jax.experimental import pallas as pl
from jax.experimental.pallas import tpu as pltpu
from jax.sharding import PartitionSpec as P

time_step = 0.05
hyper_coeff = 0.0005

FACES = 6
ROWS = 128
LANES = 128
EDGES = 4
RING = (3, 2, 1, 0)
RING_ROWS = 64
SLOT = 64


def deriv_table():
    gll_nodes = np.array([-1.0, -1.0 / np.sqrt(5.0), 1.0 / np.sqrt(5.0), 1.0])
    bary_weights = np.ones(4)
    for j in range(4):
        for m in range(4):
            if m != j:
                bary_weights[j] = bary_weights[j] / (gll_nodes[j] - gll_nodes[m])
    matrix = np.zeros((4, 4))
    for i in range(4):
        for j in range(4):
            if i != j:
                matrix[i, j] = bary_weights[j] / bary_weights[i] / (gll_nodes[i] - gll_nodes[j])
        matrix[i, i] = -np.sum(matrix[i])
    return matrix


def deriv_operands():
    table = deriv_table()
    along_x = np.kron(np.eye(32), table.T)
    along_y = np.kron(np.kron(np.eye(4), table.T), np.eye(8))
    return along_x.astype(np.float32), along_y.astype(np.float32)


def roll(values, shift, axis):
    return pltpu.roll(values, shift % values.shape[axis], axis)


def iota(shape, dim):
    return lax.broadcasted_iota(jnp.int32, shape, dim)


def dot(a, b):
    return jnp.dot(a, b, precision=lax.Precision.HIGHEST, preferred_element_type=jnp.float32)


def dot_t(a, b):
    return lax.dot_general(
        a,
        b,
        (((1,), (1,)), ((), ())),
        precision=lax.Precision.HIGHEST,
        preferred_element_type=jnp.float32,
    )


def stacked(parts, axis=0):
    return jnp.concatenate(parts, axis=axis)


def gll_weight(position):
    return jnp.where((position % 4 == 0) | (position % 4 == 3), 1.0 / 6.0, 5.0 / 6.0)


def mass_weight():
    lane = iota((1, LANES), 1)
    return gll_weight(lane // 8) * gll_weight(lane % 8)


def beside(field):
    return (
        roll(field, 1, 1),
        roll(field, -1, 1),
        roll(roll(field, 1, 0), -7, 1),
        roll(roll(field, -1, 0), 7, 1),
    )


def summed_along_x(field):
    lane = iota(field.shape, 1)
    block = iota(field.shape, 0) % 16
    c = lane % 8
    before, after, before_block, after_block = beside(field)
    summed = field + jnp.where(
        c == 4, before, jnp.where((c == 0) & (block > 0), before_block, 0.0)
    )
    return summed + jnp.where(
        c == 3, after, jnp.where((c == 7) & (block < 15), after_block, 0.0)
    )


def in_face(field):
    summed = summed_along_x(field)
    r = iota(field.shape, 1) // 8
    above = roll(summed, 8, 1)
    below = roll(summed, -8, 1)
    edge_rows = jnp.zeros((16, LANES), jnp.float32)
    above_block = stacked([edge_rows, above[: ROWS - 16]])
    below_block = stacked([below[16:], edge_rows])
    total = summed + jnp.where(r == 0, above_block, jnp.where(r % 4 == 0, above, 0.0))
    return total + jnp.where(r == 15, below_block, jnp.where(r % 4 == 3, below, 0.0))


def in_strips(field):
    summed = summed_along_x(field)
    r = iota(field.shape, 1) // 8
    return (
        summed
        + jnp.where(r == 4, roll(summed, 8, 1), 0.0)
        + jnp.where(r == 3, roll(summed, -8, 1), 0.0)
    )


def between_strips(field):
    block = iota(field.shape, 0) % 16
    c = iota(field.shape, 1) % 8
    _, _, before_block, after_block = beside(field)
    first = (c == 0) & (block == 0)
    last = (c == 7) & (block == 15)
    return jnp.where(first, before_block, jnp.where(last, after_block, 0.0))


def rim_tables(edge, reverse=False):
    lane = iota((LANES, LANES), 0)
    k = iota((LANES, LANES), 1)
    count = 16 if edge in (0, 2) else 8
    block = iota((count, LANES), 0)
    at = iota((count, LANES), 1)
    if reverse:
        k, at = 127 - k, 127 - at
    if edge == 0:
        hit, mask = lane == k % 8, block == at // 8
    elif edge == 1:
        hit, mask = lane == 8 * (k % 16) + 7, block == at // 16
    elif edge == 2:
        hit, mask = lane == 127 - k % 8, block == 15 - at // 8
    else:
        hit, mask = lane == 8 * (15 - k % 16), block == 7 - at // 16
    return jnp.where(hit, 1.0, 0.0), jnp.where(mask, 1.0, 0.0)


def rim_rows(edge, base=0):
    if edge == 0:
        return pl.ds(base, 16)
    if edge == 1:
        return pl.ds(base + 15, 8, 16)
    if edge == 2:
        return pl.ds(base + 112, 16)
    return pl.ds(base, 8, 16)


def turned(u, v, quarter):
    quarter = quarter % 4
    if quarter == 0:
        return u, v
    if quarter == 1:
        return -v, u
    if quarter == 2:
        return -u, -v
    return v, -u


def block_sums(values, mask):
    count = mask.shape[0]
    return [
        jnp.sum(values[n : n + count] * mask, axis=0, keepdims=True)
        for n in range(0, values.shape[0], count)
    ]


def join(face_ref, ring, channels):
    south, south_mask = rim_tables(0)
    spread, mask = rim_tables(0, reverse=True)
    up = block_sums(dot(stacked(ring), spread), mask)
    down = []
    for edge in range(EDGES):
        spread, mask = rim_tables(edge, reverse=True)
        rows = stacked([face_ref[rim_rows(edge, ROWS * ch), :] for ch in range(channels)])
        line = block_sums(dot(rows, spread), mask)
        down.append([*turned(line[0], line[1], 2 - edge), *line[2:]])
    down_rows = [down[edge][ch] * south_mask for ch in range(channels) for edge in RING]
    placed = dot_t(stacked(down_rows), south)
    ring_total = [
        ring[ch] + between_strips(ring[ch]) + placed[RING_ROWS * ch : RING_ROWS * ch + RING_ROWS]
        for ch in range(channels)
    ]
    for n, edge in enumerate(RING):
        line = [up[EDGES * ch + n] for ch in range(channels)]
        line = [*turned(line[0], line[1], edge + 2), *line[2:]]
        spread, mask = rim_tables(edge)
        count = mask.shape[0]
        placed = dot_t(stacked([part * mask for part in line]), spread)
        for ch in range(channels):
            rows = rim_rows(edge, ROWS * ch)
            face_ref[rows, :] = face_ref[rows, :] + placed[ch * count : (ch + 1) * count]
    return ring_total


def pack_kernel(state_ref, jac_ref, diag_ref, cross_ref, cor_ref, out_ref):
    turned_state = jnp.transpose(state_ref[...])
    for part in range(3):
        out_ref[pl.ds(part, 64, 8), :] = turned_state[64 * part : 64 * part + 64]
    spread = jnp.where(iota((16, LANES), 1) // 8 == iota((16, LANES), 0), 1.0, 0.0)
    mask = jnp.where(iota((8, LANES), 1) % 8 == iota((8, LANES), 0), 1.0, 0.0)
    fields = [jac_ref[...], diag_ref[0], diag_ref[1], cross_ref[...], cor_ref[...]]
    for k, line in enumerate(block_sums(dot(stacked(fields), spread), mask)):
        out_ref[pl.ds(3 + k, 64, 8), :] = jnp.broadcast_to(line, (64, LANES))


def strip_of(edge, fields_ref):
    rows = stacked([fields_ref[rim_rows(edge, ROWS * k), :] for k in range(8)])
    if edge == 0:
        return rows
    lane = iota((LANES, LANES), 0)
    m = iota((LANES, LANES), 1)
    if edge == 2:
        nodes = dot(rows, jnp.where(lane == 127 - m, 1.0, 0.0))
        return dot(jnp.where((lane // 16 == m // 16) & (lane % 16 == 15 - m % 16), 1.0, 0.0), nodes)
    near = m < 64
    if edge == 1:
        source = 8 * (m % 8) + 7 - m // 8
    else:
        source = 8 * (7 - m % 8) + m // 8
    halves = [
        dot(rows, jnp.where(near & (lane == source + 64 * half), 1.0, 0.0)) for half in range(2)
    ]
    j = lane % 16 if edge == 1 else 15 - lane % 16
    wanted = 64 * (j % 2) + 8 * (lane // 16) + j // 2
    return dot(jnp.where(m == wanted, 1.0, 0.0), stacked(halves))


def put_strips(fields_ref, nbr_ref, face, send_ref):
    near = iota((16, LANES), 1) < 64
    for edge in range(EDGES):
        rows = strip_of(edge, fields_ref)
        u, v, t, mass, volume, m_xx, m_yy, m_xy = [rows[16 * k : 16 * k + 16] for k in range(8)]
        u, v = turned(u, v, -edge)
        if edge % 2:
            m_xx, m_yy, m_xy = m_yy, m_xx, -m_xy
        slot = [
            jnp.where(near, low, roll(high, 64, 1))
            for low, high in ((u, v), (t, mass), (volume, m_xx), (m_yy, m_xy))
        ]
        start = pl.multiple_of(SLOT * nbr_ref[edge, face], SLOT)
        send_ref[pl.ds(start, SLOT), :] = stacked(slot)


def got_strips(nbr_ref, face, got_ref):
    near = iota((RING_ROWS, LANES), 1) < 64
    pairs = [[] for _ in range(4)]
    for edge in RING:
        start = pl.multiple_of(SLOT * nbr_ref[edge, face], SLOT)
        slot = got_ref[pl.ds(start, SLOT), :]
        for n in range(4):
            pairs[n].append(slot[16 * n : 16 * n + 16])
    fields = []
    for pair in pairs:
        rows = stacked(pair)
        fields += [jnp.where(near, rows, 0.0), jnp.where(near, roll(rows, 64, 1), 0.0)]
    fields[3] = jnp.where(near, fields[3], 1.0)
    fields[4] = jnp.where(near, fields[4], 1.0)
    return fields


def first_kernel(nbr_ref, own_ref, other_ref, dx_ref, dy_ref, fields_ref, send_ref):
    core = lax.axis_index("fy") % 2
    face = lax.axis_index("face")
    fields = []
    for k in range(8):
        own = own_ref[pl.ds(k, 64, 8), :]
        other = other_ref[pl.ds(k, 64, 8), :]
        even = jnp.where(core == 0, own, other)
        odd = jnp.where(core == 0, other, own)
        pieces = []
        for x in range(4):
            pieces += [even[16 * x : 16 * x + 16], odd[16 * x : 16 * x + 16]]
        fields.append(stacked(pieces))
    u, v, t, volume, m_xx, m_yy, m_xy, planet = fields
    contra_u = m_xx * u + m_xy * v
    contra_v = m_xy * u + m_yy * v
    energy = 0.5 * (u * contra_u + v * contra_v) + t
    x_derivs = dot(stacked([v, t, energy]), dx_ref[...])
    y_derivs = dot(stacked([u, t, energy]), dy_ref[...])
    dx_v, dx_t, dx_e = x_derivs[:ROWS], x_derivs[ROWS : 2 * ROWS], x_derivs[2 * ROWS :]
    dy_u, dy_t, dy_e = y_derivs[:ROWS], y_derivs[ROWS : 2 * ROWS], y_derivs[2 * ROWS :]
    absolute = (dx_v - dy_u) / volume + planet
    mass = mass_weight() * volume
    raw_u = u + time_step * (absolute * volume * contra_v - dx_e)
    raw_v = v + time_step * (-absolute * volume * contra_u - dy_e)
    raw_t = t - time_step * (contra_u * dx_t + contra_v * dy_t)
    sums = [in_face(field) for field in (mass * raw_u, mass * raw_v, mass * raw_t, mass)]
    for k, field in enumerate([*sums, volume, m_xx, m_yy, m_xy]):
        fields_ref[ROWS * k : ROWS * k + ROWS, :] = field
    put_strips(fields_ref, nbr_ref, face, send_ref)


def laplace(fields, geometry, along_x, along_y):
    volume, m_xx, m_yy, m_xy = geometry
    count = volume.shape[0]
    values = stacked(fields)
    grad_x, grad_y = dot(values, along_x), dot(values, along_y)
    flux_x, flux_y = [], []
    for ch in range(3):
        part = slice(count * ch, count * ch + count)
        flux_x.append(volume * (m_xx * grad_x[part] + m_xy * grad_y[part]))
        flux_y.append(volume * (m_xy * grad_x[part] + m_yy * grad_y[part]))
    spread = dot(stacked(flux_x), along_x) + dot(stacked(flux_y), along_y)
    mass = mass_weight() * volume
    return [mass * (spread[count * ch : count * ch + count] / volume) for ch in range(3)]


def second_kernel(nbr_ref, got_ref, fields_ref, dx_ref, dy_ref, out_ref, total_ref):
    face = lax.axis_index("face")
    core = lax.axis_index("fy") % 2
    along_x, along_y = dx_ref[...], dy_ref[...]
    ring_fields = got_strips(nbr_ref, face, got_ref)
    geometry = [
        stacked([fields_ref[ROWS * k : ROWS * k + ROWS, :], ring_fields[k]]) for k in range(4, 8)
    ]

    total_ref[...] = fields_ref[: 4 * ROWS, :]
    ring = join(total_ref, ring_fields[:4], 4)
    face_mass = total_ref[3 * ROWS : 4 * ROWS, :]
    total_mass = stacked([face_mass, ring[3]])
    sectioned = [total_ref[ROWS * ch : ROWS * ch + ROWS, :] / face_mass for ch in range(3)]
    fields = [stacked([sectioned[ch], ring[ch] / ring[3]]) for ch in range(3)]
    for step in range(2):
        lapped = laplace(fields, geometry, along_x, along_y)
        for ch in range(3):
            total_ref[ROWS * ch : ROWS * ch + ROWS, :] = in_face(lapped[ch][:ROWS])
        ring = join(total_ref, [in_strips(field[ROWS:]) for field in lapped], 3)
        if step == 0:
            fields = [
                stacked([total_ref[ROWS * ch : ROWS * ch + ROWS, :], ring[ch]]) / total_mass
                for ch in range(3)
            ]
    for ch in range(3):
        part = slice(ROWS * ch, ROWS * ch + ROWS)
        total_ref[part, :] = sectioned[ch] - hyper_coeff * (total_ref[part, :] / face_mass)
    for x in range(4):
        for ch in range(3):
            start = pl.multiple_of(ROWS * ch + 32 * x + 16 * core, 16)
            out_ref[16 * x : 16 * x + 16, 0, LANES * ch : LANES * ch + LANES] = total_ref[
                pl.ds(start, 16), :
            ]


def unpack_kernel(got_ref, out_ref):
    levels = got_ref[...]
    columns = stacked([levels[:, 0, LANES * ch : LANES * ch + LANES] for ch in range(3)])
    out_ref[...] = jnp.transpose(columns)


def f32(*shape):
    return jax.ShapeDtypeStruct(shape, jnp.float32)


def near(*shape):
    return pltpu.VMEM(shape, jnp.float32)


def held(values):
    return pltpu.with_memory_space_constraint(values, pltpu.VMEM)


VMEM = pl.BlockSpec(memory_space=pltpu.VMEM)
SMEM = pl.BlockSpec(memory_space=pltpu.SMEM)


def call(kernel, outs, ins, scratch=(), name=None):
    return pl.pallas_call(
        kernel,
        out_shape=outs,
        in_specs=ins,
        out_specs=jax.tree.map(lambda _: VMEM, outs),
        scratch_shapes=scratch,
        name=name,
    )


def level_groups():
    return [
        [(8 * face + 2 * x + core) * 16 + fx for x in range(4) for fx in range(16)]
        for face in range(FACES)
        for core in range(2)
    ]


def per_device(state, jacobian, metric_diag, metric_cross, coriolis, nbr_face, nbr_edge):
    axes = ("face", "fy", "fx")
    groups = level_groups()
    along_x, along_y = deriv_operands()

    packed = call(pack_kernel, near(512, LANES), [VMEM] * 5, name="pack")(
        state.reshape(128, 192),
        jacobian[0].T,
        metric_diag[:, 0].transpose(0, 2, 1),
        metric_cross[0].T,
        coriolis[0].T,
    )
    own = lax.all_to_all(
        packed.reshape(64, 8, LANES), axes, 0, 0, axis_index_groups=groups, tiled=True
    )
    other = lax.ppermute(own, "fy", [(i, i ^ 1) for i in range(8)])
    fields, send = call(
        first_kernel,
        [near(8 * ROWS, LANES), near(SLOT * FACES, LANES)],
        [SMEM] + [VMEM] * 4,
        name="first",
    )(nbr_face.T, held(own.reshape(512, LANES)), held(other.reshape(512, LANES)), along_x, along_y)
    got = lax.all_to_all(send.reshape(FACES, SLOT, LANES), "face", 0, 0, tiled=True)
    updated = call(
        second_kernel,
        near(64, 1, 3 * LANES),
        [SMEM] + [VMEM] * 4,
        [pltpu.VMEM((4 * ROWS, LANES), jnp.float32)],
        name="second",
    )(nbr_face.T, held(got.reshape(SLOT * FACES, LANES)), held(fields), along_x, along_y)
    back = lax.all_to_all(
        updated, axes, 0, 0, axis_index_groups=groups, tiled=True
    )
    nodes = call(unpack_kernel, f32(128, 192), [VMEM], name="unpack")(
        held(back)
    )
    return nodes.reshape(1, 16, 8, 192)


def solution(mesh):
    return jax.shard_map(
        per_device,
        mesh=mesh,
        in_specs=(
            P("face", "fy", "fx", None),
            P("face", "fy", "fx"),
            P(None, "face", "fy", "fx"),
            P("face", "fy", "fx"),
            P("face", "fy", "fx"),
            P(),
            P(),
        ),
        out_specs=P("face", "fy", "fx", None),
        check_vma=False,
    )
```

```python
import jax
import jax.numpy as jnp
import ml_dtypes
import numpy as np
from jax import lax
from jax.experimental import pallas as pl
from jax.experimental.pallas import tpu as pltpu
from jax.sharding import PartitionSpec as P

time_step = 0.05
hyper_coeff = 0.0005

FACES = 6
ROWS = 128
LANES = 128
EDGES = 4
RING_ROWS = 48
ALL_ROWS = ROWS + RING_ROWS
SLOT = 56
ENDS = ("S0", "S15", "N0", "N15", "E0", "E7", "W0", "W7")
END_ROWS = (0, 15, 16, 31, 32, 39, 40, 47)
MEETS = (6, 4, 7, 5, 1, 3, 0, 2)
TURNS = (1, -1, -1, 1, 1, -1, -1, 1)


def deriv_table():
    gll_nodes = np.array([-1.0, -1.0 / np.sqrt(5.0), 1.0 / np.sqrt(5.0), 1.0])
    bary_weights = np.ones(4)
    for j in range(4):
        for m in range(4):
            if m != j:
                bary_weights[j] = bary_weights[j] / (gll_nodes[j] - gll_nodes[m])
    matrix = np.zeros((4, 4))
    for i in range(4):
        for j in range(4):
            if i != j:
                matrix[i, j] = bary_weights[j] / bary_weights[i] / (gll_nodes[i] - gll_nodes[j])
        matrix[i, i] = -np.sum(matrix[i])
    return matrix


def in_parts(matrix):
    rest = np.asarray(matrix, np.float64)
    parts = []
    for _ in range(3):
        part = rest.astype(ml_dtypes.bfloat16)
        parts.append(part)
        rest = rest - part.astype(np.float64)
    return parts


def face_node(edge, depth, k):
    row, col = ((depth, k), (k, 127 - depth), (127 - depth, 127 - k), (127 - k, depth))[edge]
    return row // 16, col // 8, 8 * (row % 16) + col % 8


def ring_node(edge, depth, k):
    if edge == 1:
        return k // 16, 8 * (k % 16) + depth
    row = 127 - k
    return row // 16, 8 * (row % 16) + 7 - depth


def end_lane(end, depth):
    return {
        "S0": 8 * (15 - depth),
        "S15": 8 * (15 - depth) + 7,
        "N0": 8 * depth,
        "N15": 8 * depth + 7,
        "E0": depth,
        "E7": 120 + depth,
        "W0": 7 - depth,
        "W7": 127 - depth,
    }[end]


def tables():
    deriv = deriv_table()
    along_x = np.kron(np.eye(32), deriv.T)
    along_y = np.kron(np.kron(np.eye(4), deriv.T), np.eye(8))
    lane = np.arange(LANES)
    r, c = lane // 8, lane % 8
    weights = np.array([1.0, 5.0, 5.0, 1.0]) / 6.0
    within = np.eye(LANES)
    across = np.zeros((LANES, LANES))
    for l in range(LANES):
        if c[l] in (3, 4):
            within[l, l + 1 if c[l] == 3 else l - 1] = 1.0
        if c[l] == 7:
            across[l, l - 7] = 1.0
        if c[l] == 0:
            across[l, l + 7] = 1.0
    both = np.concatenate([within, across], 1)
    gradient = in_parts(np.concatenate([along_x, along_y], 1))
    weighted = np.diag(weights[r % 4] * weights[c % 4])
    spread = in_parts(np.concatenate([along_x @ weighted @ both, along_y @ weighted @ both], 0))

    wide = {
        "gradient": np.concatenate([gradient[n] for n in (0, 0, 1, 1, 0, 2)], 0),
        "spread": np.concatenate([spread[n] for n in (0, 0, 0, 1, 1, 2)], 0),
        "both": np.concatenate([both] * 3, 0),
    }
    narrow = {"reverse": np.eye(LANES)[::-1]}
    narrow["reverse_rows"] = np.kron(np.eye(8), np.eye(16)[::-1])
    for edge, name in ((1, "east"), (3, "west")):
        out = np.zeros((2, LANES, LANES))
        out_rows = np.zeros((LANES, LANES))
        into = np.zeros((2, LANES, LANES))
        into_rows = np.zeros((LANES, LANES))
        for k in range(128):
            j, i = k // 8, k % 8
            j2, i2 = (127 - k) // 8, (127 - k) % 8
            for depth in range(8):
                fy, _, at = face_node(edge, depth, k)
                out[j % 2, at, 8 * depth + i] = 1.0
                ring_fy, ring_at = ring_node(edge, depth, k)
                into[j2 % 2, 8 * depth + i2, ring_at] = 1.0
                for field in range(8):
                    out_rows[16 * field + j, 64 * (j % 2) + 8 * field + fy] = 1.0
                    into_rows[64 * (j2 % 2) + 8 * field + ring_fy, 16 * field + j2] = 1.0
        wide[name + "_out"] = np.concatenate([out[0], out[1]], 1)
        narrow[name + "_out_rows"] = out_rows
        narrow[name + "_in_rows"] = into_rows
        narrow[name + "_in"] = np.concatenate([into[0]] * 3 + [into[1]] * 3, 0)
    take = np.zeros((LANES, LANES))
    give = np.zeros((LANES, LANES))
    masks = np.zeros((32, LANES), np.float32)
    for t, end in enumerate(ENDS):
        for depth in range(8):
            take[end_lane(end, depth), 8 * t + depth] = 1.0
            give[8 * t + depth, end_lane(ENDS[MEETS[t]], depth)] = 1.0
            masks[t, end_lane(end, depth)] = 1.0
            masks[8 + t, 8 * t + depth] = 1.0
            masks[16 + t, 8 * MEETS[t] + depth] = 1.0
        masks[24 + t] = TURNS[t]
    narrow["take"] = np.concatenate([take] * 3, 0)
    narrow["give"] = np.concatenate([give] * 3, 0)

    arrays, places = [], {}
    for group in (wide, narrow):
        start = 0
        for name, matrix in group.items():
            places[name] = (start, start + matrix.shape[0])
            start += matrix.shape[0]
        arrays.append(
            np.concatenate([m.astype(ml_dtypes.bfloat16) for m in group.values()], 0)
        )
    return arrays[0], arrays[1], masks, places


WIDE, NARROW, MASKS, PLACES = tables()


def of(ref, name):
    start, end = PLACES[name]
    return ref[start:end, :]


def roll(values, shift, axis):
    return pltpu.roll(values, shift % values.shape[axis], axis)


def iota(shape, dim):
    return lax.broadcasted_iota(jnp.int32, shape, dim)


def dot(a, b):
    return jnp.dot(a, b, preferred_element_type=jnp.float32)


def stacked(parts, axis=0):
    return jnp.concatenate(parts, axis=axis)


def split(values):
    high = values.astype(jnp.bfloat16)
    rest = values - high.astype(jnp.float32)
    mid = rest.astype(jnp.bfloat16)
    return high, mid, (rest - mid.astype(jnp.float32)).astype(jnp.bfloat16)


def gradient(values, wide_ref):
    high, mid, low = split(values)
    both = dot(stacked([high, mid, high, mid, low, high], 1), of(wide_ref, "gradient"))
    return both[:, :LANES], both[:, LANES:]


def mass_weight():
    lane = iota((1, LANES), 1)
    r, c = lane // 8 % 4, lane % 4
    along_y = jnp.where((r == 0) | (r == 3), 1.0 / 6.0, 5.0 / 6.0)
    return along_y * jnp.where((c == 0) | (c == 3), 1.0 / 6.0, 5.0 / 6.0)


def assembled(inner, outer):
    shape = inner.shape
    row = iota(shape, 0)
    lane = iota(shape, 1)
    c = lane % 8
    r = lane // 8
    here = row < ROWS + 32
    from_before = here & (c == 0) & (row % 16 > 0)
    from_after = here & (c == 7) & (row % 16 < 15)
    summed = (
        inner
        + jnp.where(from_before, roll(outer, 1, 0), 0.0)
        + jnp.where(from_after, roll(outer, -1, 0), 0.0)
    )
    above = roll(summed, 8, 1)
    below = roll(summed, -8, 1)
    total = (
        summed
        + jnp.where((r % 4 == 0) & (r > 0), above, 0.0)
        + jnp.where((r % 4 == 3) & (r < 15), below, 0.0)
    )
    edge_rows = jnp.zeros((16, LANES), jnp.float32)
    above_block = [edge_rows, above[: ROWS - 16]]
    below_block = [below[16:ROWS], edge_rows]
    if shape[0] > ROWS:
        sides = slice(ROWS + 32, ROWS + 48)
        fy = iota((16, LANES), 0) % 8
        above_block += [edge_rows] * 2 + [jnp.where(fy > 0, roll(above[sides], 1, 0), 0.0)]
        below_block += [edge_rows] * 2 + [jnp.where(fy < 7, roll(below[sides], -1, 0), 0.0)]
    return (
        total
        + jnp.where(r == 0, stacked(above_block), 0.0)
        + jnp.where(r == 15, stacked(below_block), 0.0)
    )


def rim_rows(edge, base=0):
    if edge == 0:
        return pl.ds(base, 16)
    if edge == 1:
        return pl.ds(base + 15, 8, 16)
    if edge == 2:
        return pl.ds(base + 112, 16)
    return pl.ds(base, 8, 16)


def turned(u, v, quarter):
    quarter = quarter % 4
    if quarter == 0:
        return u, v
    if quarter == 1:
        return -v, u
    if quarter == 2:
        return -u, -v
    return v, -u


def ends_meet(ring, channels, narrow_ref, mask_ref):
    ends = stacked(
        [ring[ch][row : row + 1] for ch in range(channels) for row in END_ROWS]
    )
    own = stacked([mask_ref[0:8, :]] * channels)
    taken = dot(stacked(split(ends * own), 1), of(narrow_ref, "take"))
    lines = []
    for ch in range(channels):
        line = jnp.sum(taken[8 * ch : 8 * ch + 8] * mask_ref[8:16, :], axis=0, keepdims=True)
        lines.append(line * mask_ref[16:24, :])
    given = dot(stacked(split(stacked(lines)), 1), of(narrow_ref, "give"))
    given = [given[8 * ch : 8 * ch + 8] for ch in range(channels)]
    sense = mask_ref[24:32, :]
    return [-sense * given[1], sense * given[0], *given[2:]]


def join(face_ref, ring, channels, narrow_ref, mask_ref, ring_too=True):
    ends = ends_meet(ring, channels, narrow_ref, mask_ref) if ring_too else None
    totals = []
    for ch in range(channels):
        south, north = ring[ch][0:16], ring[ch][16:32]
        east, west = ring[ch][32:40], ring[ch][40:48]
        rows = [rim_rows(edge, ROWS * ch) for edge in range(EDGES)]
        lane = iota((16, LANES), 1)
        lane_8 = iota((8, LANES), 1)
        if ring_too:
            block = iota((16, LANES), 0)
            fy = iota((8, LANES), 0)
            of_end = [ends[ch][t : t + 1] for t in range(8)]

            def at_ends(first, last, position, count):
                return jnp.where(
                    position == 0, first, jnp.where(position == count - 1, last, 0.0)
                )

            totals.append(
                stacked(
                    [
                        south
                        + jnp.where(lane // 8 == 15, roll(face_ref[rows[0], :], -8, 1), 0.0)
                        + at_ends(of_end[0], of_end[1], block, 16),
                        north
                        + jnp.where(lane // 8 == 0, roll(face_ref[rows[2], :], 8, 1), 0.0)
                        + at_ends(of_end[2], of_end[3], block, 16),
                        east
                        + jnp.where(lane_8 % 8 == 0, roll(face_ref[rows[1], :], -7, 1), 0.0)
                        + at_ends(of_end[4], of_end[5], fy, 8),
                        west
                        + jnp.where(lane_8 % 8 == 7, roll(face_ref[rows[3], :], 7, 1), 0.0)
                        + at_ends(of_end[6], of_end[7], fy, 8),
                    ]
                )
            )
        from_south = jnp.where(lane // 8 == 0, roll(south, 8, 1), 0.0)
        from_north = jnp.where(lane // 8 == 15, roll(north, -8, 1), 0.0)
        from_east = jnp.where(lane_8 % 8 == 7, roll(east, 7, 1), 0.0)
        from_west = jnp.where(lane_8 % 8 == 0, roll(west, -7, 1), 0.0)
        for edge, part in enumerate((from_south, from_east, from_north, from_west)):
            face_ref[rows[edge], :] = face_ref[rows[edge], :] + part
    return totals


def pack_kernel(state_ref, jac_ref, diag_ref, cross_ref, cor_ref, out_ref):
    turned_state = jnp.transpose(state_ref[...])
    for part in range(3):
        out_ref[pl.ds(part, 64, 8), :] = turned_state[64 * part : 64 * part + 64]
    spread = jnp.where(iota((16, LANES), 1) // 8 == iota((16, LANES), 0), 1.0, 0.0)
    mask = jnp.where(iota((8, LANES), 1) % 8 == iota((8, LANES), 0), 1.0, 0.0)
    fields = [jac_ref[...], diag_ref[0], diag_ref[1], cross_ref[...], cor_ref[...]]
    lines = jnp.dot(
        stacked(fields),
        spread,
        precision=lax.Precision.HIGHEST,
        preferred_element_type=jnp.float32,
    )
    for k in range(5):
        line = jnp.sum(lines[8 * k : 8 * k + 8] * mask, axis=0, keepdims=True)
        out_ref[pl.ds(3 + k, 64, 8), :] = jnp.broadcast_to(line, (64, LANES))


def reversed_blocks(rows, narrow_ref):
    parts = stacked([part.astype(jnp.float32) for part in split(rows)]).astype(jnp.bfloat16)
    moved = dot(parts, of(narrow_ref, "reverse"))
    count = rows.shape[0]
    moved = stacked([moved[n * count : n * count + count] for n in range(3)], 1)
    moved = dot(of(narrow_ref, "reverse_rows"), moved.astype(jnp.bfloat16))
    return moved[:, :LANES] + moved[:, LANES : 2 * LANES] + moved[:, 2 * LANES :]


def strip_of(edge, fields_ref, wide_ref, narrow_ref):
    rows = [fields_ref[rim_rows(edge, ROWS * k), :] for k in range(7)]
    rows = stacked([*rows, jnp.zeros_like(rows[0])])
    if edge == 0:
        return rows
    if edge == 2:
        return reversed_blocks(rows, narrow_ref)
    name = "east" if edge == 1 else "west"
    moved = dot(stacked(split(rows)), of(wide_ref, name + "_out"))
    halves = stacked([moved[:, :LANES], moved[:, LANES:]], 0)
    moved = stacked(
        [stacked([halves[64 * n : 64 * n + 64], halves[192 + 64 * n : 256 + 64 * n]]) for n in range(3)],
        1,
    )
    moved = dot(of(narrow_ref, name + "_out_rows"), moved.astype(jnp.bfloat16))
    return moved[:, :LANES] + moved[:, LANES : 2 * LANES] + moved[:, 2 * LANES :]


def put_strips(fields_ref, nbr_ref, face, send_ref, wide_ref, narrow_ref):
    near = iota((16, LANES), 1) < 64
    for edge in range(EDGES):
        rows = strip_of(edge, fields_ref, wide_ref, narrow_ref)
        u, v, t, mass, flux_xx, flux_xy, flux_yy = [rows[16 * k : 16 * k + 16] for k in range(7)]
        u, v = turned(u, v, -edge)
        if edge % 2:
            flux_xx, flux_xy, flux_yy = flux_yy, -flux_xy, flux_xx
        slot = [
            jnp.where(near, low, roll(high, 64, 1))
            for low, high in ((u, v), (t, mass), (flux_xx, flux_xy))
        ]
        slot.append(jnp.where(near[:8], flux_yy[:8], roll(flux_yy[8:], 64, 1)))
        start = pl.multiple_of(SLOT * nbr_ref[edge, face], 8)
        send_ref[pl.ds(start, SLOT), :] = stacked(slot)


def ring_of(nbr_ref, face, got_ref, narrow_ref):
    near = iota((16, LANES), 1) < 64
    strips = []
    for edge in range(EDGES):
        start = pl.multiple_of(SLOT * nbr_ref[edge, face], 8)
        slot = got_ref[pl.ds(start, SLOT), :]
        fields = []
        for n in range(3):
            rows = slot[16 * n : 16 * n + 16]
            fields += [jnp.where(near, rows, 0.0), jnp.where(near, roll(rows, 64, 1), 0.0)]
        rows = slot[48:56]
        fields.append(stacked([rows, roll(rows, 64, 1)]))
        fields[6] = jnp.where(near, fields[6], 0.0)
        rows = stacked([*fields, jnp.zeros_like(near, jnp.float32)])
        count = 16
        if edge == 0:
            rows = reversed_blocks(rows, narrow_ref)
        elif edge % 2:
            name = "east" if edge == 1 else "west"
            moved = dot(of(narrow_ref, name + "_in_rows"), stacked(split(rows), 1))
            moved = stacked([moved[:64], moved[64:]], 1)
            rows = dot(moved.astype(jnp.bfloat16), of(narrow_ref, name + "_in"))
            count = 8
        fields = [rows[count * k : count * k + count] for k in range(7)]
        fields[0], fields[1] = turned(fields[0], fields[1], edge + 2)
        if edge % 2:
            fields[4], fields[5], fields[6] = fields[6], -fields[5], fields[4]
        else:
            far = near if edge == 0 else ~near
            fields[3] = jnp.where(far, 1.0, fields[3])
        strips.append(fields)
    return [stacked([strips[edge][k] for edge in (0, 2, 1, 3)]) for k in range(7)]


def first_kernel(nbr_ref, own_ref, other_ref, wide_ref, narrow_ref, fields_ref, send_ref):
    core = lax.axis_index("fy") % 2
    face = lax.axis_index("face")
    fields = []
    for k in range(8):
        own = own_ref[pl.ds(k, 64, 8), :]
        other = other_ref[pl.ds(k, 64, 8), :]
        even = jnp.where(core == 0, own, other)
        odd = jnp.where(core == 0, other, own)
        pieces = []
        for x in range(4):
            pieces += [even[16 * x : 16 * x + 16], odd[16 * x : 16 * x + 16]]
        fields.append(stacked(pieces))
    u, v, t, volume, m_xx, m_yy, m_xy, planet = fields
    contra_u = m_xx * u + m_xy * v
    contra_v = m_xy * u + m_yy * v
    energy = 0.5 * (u * contra_u + v * contra_v) + t
    grad_x, grad_y = gradient(stacked([u, v, t, energy]), wide_ref)
    dy_u, dx_v = grad_y[:ROWS], grad_x[ROWS : 2 * ROWS]
    dx_t, dy_t = grad_x[2 * ROWS : 3 * ROWS], grad_y[2 * ROWS : 3 * ROWS]
    dx_e, dy_e = grad_x[3 * ROWS :], grad_y[3 * ROWS :]
    absolute = dx_v - dy_u + planet * volume
    mass = mass_weight() * volume
    raw_u = u + time_step * (absolute * contra_v - dx_e)
    raw_v = v + time_step * (-absolute * contra_u - dy_e)
    raw_t = t - time_step * (contra_u * dx_t + contra_v * dy_t)
    values = stacked([mass * raw_u, mass * raw_v, mass * raw_t, mass])
    sums = dot(stacked(split(values), 1), of(wide_ref, "both"))
    for ch in range(4):
        part = slice(ROWS * ch, ROWS * ch + ROWS)
        fields_ref[part, :] = assembled(sums[part, :LANES], sums[part, LANES:])
    for k, field in enumerate([m_xx, m_xy, m_yy]):
        fields_ref[ROWS * (4 + k) : ROWS * (5 + k), :] = volume * field
    put_strips(fields_ref, nbr_ref, face, send_ref, wide_ref, narrow_ref)


def laplace(fields, metric, wide_ref):
    flux_xx, flux_xy, flux_yy = metric
    count = flux_xx.shape[0]
    grad_x, grad_y = gradient(stacked(fields), wide_ref)
    flux = []
    for ch in range(3):
        part = slice(count * ch, count * ch + count)
        flux.append(
            stacked(
                [
                    flux_xx * grad_x[part] + flux_xy * grad_y[part],
                    flux_xy * grad_x[part] + flux_yy * grad_y[part],
                ],
                1,
            )
        )
    high, mid, low = split(stacked(flux))
    sums = dot(stacked([high, mid, low, high, mid, high], 1), of(wide_ref, "spread"))
    return [
        assembled(sums[count * ch : count * ch + count, :LANES], sums[count * ch : count * ch + count, LANES:])
        for ch in range(3)
    ]


def second_kernel(nbr_ref, got_ref, fields_ref, wide_ref, narrow_ref, mask_ref, out_ref, total_ref):
    face = lax.axis_index("face")
    core = lax.axis_index("fy") % 2
    ring_fields = ring_of(nbr_ref, face, got_ref, narrow_ref)
    metric = [
        stacked([fields_ref[ROWS * k : ROWS * k + ROWS, :], ring_fields[k]]) for k in range(4, 7)
    ]
    total_ref[...] = fields_ref[: 4 * ROWS, :]
    ring = join(total_ref, ring_fields[:4], 4, narrow_ref, mask_ref)
    share = 1.0 / stacked([total_ref[3 * ROWS : 4 * ROWS, :], ring[3]])
    fields = [
        stacked([total_ref[ROWS * ch : ROWS * ch + ROWS, :], ring[ch]]) * share for ch in range(3)
    ]
    sectioned = [field[:ROWS] for field in fields]
    for step in range(2):
        sums = laplace(fields, metric, wide_ref)
        for ch in range(3):
            total_ref[ROWS * ch : ROWS * ch + ROWS, :] = sums[ch][:ROWS]
        ring = join(
            total_ref, [field[ROWS:] for field in sums], 3, narrow_ref, mask_ref, step == 0
        )
        if step == 0:
            fields = [
                stacked([total_ref[ROWS * ch : ROWS * ch + ROWS, :], ring[ch]]) * share
                for ch in range(3)
            ]
    for ch in range(3):
        part = slice(ROWS * ch, ROWS * ch + ROWS)
        total_ref[part, :] = sectioned[ch] - hyper_coeff * (total_ref[part, :] * share[:ROWS])
    for x in range(4):
        for ch in range(3):
            start = pl.multiple_of(ROWS * ch + 32 * x + 16 * core, 16)
            out_ref[16 * x : 16 * x + 16, 0, LANES * ch : LANES * ch + LANES] = total_ref[
                pl.ds(start, 16), :
            ]


def unpack_kernel(got_ref, out_ref):
    levels = got_ref[...]
    columns = stacked([levels[:, 0, LANES * ch : LANES * ch + LANES] for ch in range(3)])
    out_ref[...] = jnp.transpose(columns)


def f32(*shape):
    return jax.ShapeDtypeStruct(shape, jnp.float32)


def near(*shape):
    return pltpu.VMEM(shape, jnp.float32)


def held(values):
    return pltpu.with_memory_space_constraint(values, pltpu.VMEM)


VMEM = pl.BlockSpec(memory_space=pltpu.VMEM)
SMEM = pl.BlockSpec(memory_space=pltpu.SMEM)


def call(kernel, outs, ins, scratch=(), name=None):
    return pl.pallas_call(
        kernel,
        out_shape=outs,
        in_specs=ins,
        out_specs=jax.tree.map(lambda _: VMEM, outs),
        scratch_shapes=scratch,
        name=name,
    )


def level_groups():
    return [
        [(8 * face + 2 * x + core) * 16 + fx for x in range(4) for fx in range(16)]
        for face in range(FACES)
        for core in range(2)
    ]


def per_device(state, jacobian, metric_diag, metric_cross, coriolis, nbr_face, nbr_edge):
    axes = ("face", "fy", "fx")
    groups = level_groups()
    wide, narrow = held(jnp.asarray(WIDE)), held(jnp.asarray(NARROW))

    packed = call(pack_kernel, near(512, LANES), [VMEM] * 5, name="pack")(
        state.reshape(128, 192),
        jacobian[0].T,
        metric_diag[:, 0].transpose(0, 2, 1),
        metric_cross[0].T,
        coriolis[0].T,
    )
    own = lax.all_to_all(
        packed.reshape(64, 8, LANES), axes, 0, 0, axis_index_groups=groups, tiled=True
    )
    other = lax.ppermute(own, "fy", [(i, i ^ 1) for i in range(8)])
    fields, send = call(
        first_kernel,
        [near(7 * ROWS, LANES), near(SLOT * FACES, LANES)],
        [SMEM] + [VMEM] * 4,
        name="first",
    )(nbr_face.T, held(own.reshape(512, LANES)), held(other.reshape(512, LANES)), wide, narrow)
    got = lax.all_to_all(send.reshape(FACES, SLOT, LANES), "face", 0, 0, tiled=True)
    updated = call(
        second_kernel,
        near(64, 1, 3 * LANES),
        [SMEM] + [VMEM] * 5,
        [pltpu.VMEM((4 * ROWS, LANES), jnp.float32)],
        name="second",
    )(nbr_face.T, held(got.reshape(SLOT * FACES, LANES)), held(fields), wide, narrow, MASKS)
    back = lax.all_to_all(
        updated, axes, 0, 0, axis_index_groups=groups, tiled=True
    )
    nodes = call(unpack_kernel, f32(128, 192), [VMEM], name="unpack")(
        held(back)
    )
    return nodes.reshape(1, 16, 8, 192)


def solution(mesh):
    return jax.shard_map(
        per_device,
        mesh=mesh,
        in_specs=(
            P("face", "fy", "fx", None),
            P("face", "fy", "fx"),
            P(None, "face", "fy", "fx"),
            P("face", "fy", "fx"),
            P("face", "fy", "fx"),
            P(),
            P(),
        ),
        out_specs=P("face", "fy", "fx", None),
        check_vma=False,
    )
```

```python
import jax
import jax.numpy as jnp
import ml_dtypes
import numpy as np
from jax import lax
from jax.experimental import pallas as pl
from jax.experimental.pallas import tpu as pltpu
from jax.sharding import PartitionSpec as P

time_step = 0.05
hyper_coeff = 0.0005

FACES = 6
ROWS = 128
LANES = 128
EDGES = 4
RING_ROWS = 48
ALL_ROWS = ROWS + RING_ROWS
SLOT = 56
ENDS = ("S0", "S15", "N0", "N15", "E0", "E7", "W0", "W7")
END_ROWS = (0, 15, 16, 31, 32, 39, 40, 47)
MEETS = (6, 4, 7, 5, 1, 3, 0, 2)
TURNS = (1, -1, -1, 1, 1, -1, -1, 1)


def deriv_table():
    gll_nodes = np.array([-1.0, -1.0 / np.sqrt(5.0), 1.0 / np.sqrt(5.0), 1.0])
    bary_weights = np.ones(4)
    for j in range(4):
        for m in range(4):
            if m != j:
                bary_weights[j] = bary_weights[j] / (gll_nodes[j] - gll_nodes[m])
    matrix = np.zeros((4, 4))
    for i in range(4):
        for j in range(4):
            if i != j:
                matrix[i, j] = bary_weights[j] / bary_weights[i] / (gll_nodes[i] - gll_nodes[j])
        matrix[i, i] = -np.sum(matrix[i])
    return matrix


def in_parts(matrix):
    rest = np.asarray(matrix, np.float64)
    parts = []
    for _ in range(3):
        part = rest.astype(ml_dtypes.bfloat16)
        parts.append(part)
        rest = rest - part.astype(np.float64)
    return parts


def face_node(edge, depth, k):
    row, col = ((depth, k), (k, 127 - depth), (127 - depth, 127 - k), (127 - k, depth))[edge]
    return row // 16, col // 8, 8 * (row % 16) + col % 8


def ring_node(edge, depth, k):
    if edge == 1:
        return k // 16, 8 * (k % 16) + depth
    row = 127 - k
    return row // 16, 8 * (row % 16) + 7 - depth


def end_lane(end, depth):
    return {
        "S0": 8 * (15 - depth),
        "S15": 8 * (15 - depth) + 7,
        "N0": 8 * depth,
        "N15": 8 * depth + 7,
        "E0": depth,
        "E7": 120 + depth,
        "W0": 7 - depth,
        "W7": 127 - depth,
    }[end]


def tables():
    deriv = deriv_table()
    along_x = np.kron(np.eye(32), deriv.T)
    along_y = np.kron(np.kron(np.eye(4), deriv.T), np.eye(8))
    lane = np.arange(LANES)
    r, c = lane // 8, lane % 8
    weights = np.array([1.0, 5.0, 5.0, 1.0]) / 6.0
    within = np.eye(LANES)
    across = np.zeros((LANES, LANES))
    for l in range(LANES):
        if c[l] in (3, 4):
            within[l, l + 1 if c[l] == 3 else l - 1] = 1.0
        if c[l] == 7:
            across[l, l - 7] = 1.0
        if c[l] == 0:
            across[l, l + 7] = 1.0
    both = np.concatenate([within, across], 1)
    gradient = in_parts(np.concatenate([along_x, along_y], 1))
    weighted = np.diag(weights[r % 4] * weights[c % 4])
    spread = in_parts(np.concatenate([along_x @ weighted @ both, along_y @ weighted @ both], 0))

    out, out_rows, into, into_rows = [], [], [], []
    for edge in (1, 3):
        out.append(np.zeros((2, LANES, LANES)))
        out_rows.append(np.zeros((LANES, LANES)))
        into.append(np.zeros((2, LANES, LANES)))
        into_rows.append(np.zeros((LANES, LANES)))
        for k in range(128):
            j, i = k // 8, k % 8
            j2, i2 = (127 - k) // 8, (127 - k) % 8
            for depth in range(8):
                fy, _, at = face_node(edge, depth, k)
                out[-1][j % 2, at, 8 * depth + i] = 1.0
                ring_fy, ring_at = ring_node(edge, depth, k)
                into[-1][j2 % 2, 8 * depth + i2, ring_at] = 1.0
                for field in range(8):
                    out_rows[-1][16 * field + j, 64 * (j % 2) + 8 * field + fy] = 1.0
                    into_rows[-1][64 * (j2 % 2) + 8 * field + ring_fy, 16 * field + j2] = 1.0
    take = np.zeros((LANES, LANES))
    give = np.zeros((LANES, LANES))
    masks = np.zeros((32, 2 * LANES))
    for t, end in enumerate(ENDS):
        for depth in range(8):
            take[end_lane(end, depth), 8 * t + depth] = 1.0
            give[8 * t + depth, end_lane(ENDS[MEETS[t]], depth)] = 1.0
            masks[t, end_lane(end, depth)] = 1.0
            masks[8 + t, 8 * t + depth] = 1.0
            masks[16 + t, 8 * MEETS[t] + depth] = 1.0
        masks[24 + t] = TURNS[t]

    def pair(left, right):
        return np.concatenate([left, right], 1)

    reverse = pair(np.eye(LANES)[::-1], np.kron(np.eye(8), np.eye(16)[::-1]))
    groups = (
        {
            "gradient": np.concatenate(gradient, 0),
            "both": both,
            "east_out": pair(*out[0]),
            "west_out": pair(*out[1]),
            "out_rows": pair(*out_rows),
            "reverse": reverse,
        },
        {
            "gradient": np.concatenate(gradient, 0),
            "spread": np.concatenate(spread, 0),
            "east_in": pair(*into[0]),
            "west_in": pair(*into[1]),
            "in_rows": pair(*into_rows),
            "reverse": reverse,
            "ends": pair(take, give),
            "masks": masks,
        },
    )
    arrays, places = [], []
    for group in groups:
        start = 0
        places.append({})
        for name, matrix in group.items():
            places[-1][name] = (start, start + matrix.shape[0])
            start += matrix.shape[0]
        arrays.append(np.concatenate([m.astype(ml_dtypes.bfloat16) for m in group.values()], 0))
    return arrays, places


TABLES, PLACES = tables()


class Table:
    def __init__(self, ref, which):
        self.ref, self.places = ref, PLACES[which]

    def whole(self, name):
        start, end = self.places[name]
        return self.ref[start:end, :]

    def left(self, name):
        start, end = self.places[name]
        return self.ref[start:end, :LANES]

    def right(self, name):
        start, end = self.places[name]
        return self.ref[start:end, LANES:]

    def part(self, name, n, rows):
        start = self.places[name][0] + n * rows
        return self.ref[start : start + rows, :]


def roll(values, shift, axis):
    return pltpu.roll(values, shift % values.shape[axis], axis)


def iota(shape, dim):
    return lax.broadcasted_iota(jnp.int32, shape, dim)


def dot(a, b):
    return jnp.dot(a, b, preferred_element_type=jnp.float32)


def stacked(parts, axis=0):
    return jnp.concatenate(parts, axis=axis)


def split(values):
    high = values.astype(jnp.bfloat16)
    rest = values - high.astype(jnp.float32)
    mid = rest.astype(jnp.bfloat16)
    return high, mid, (rest - mid.astype(jnp.float32)).astype(jnp.bfloat16)


def gradient(values, table):
    high, mid, low = split(values)
    parts = [table.part("gradient", n, LANES) for n in (0, 0, 1, 1, 0, 2)]
    both = dot(stacked([high, mid, high, mid, low, high], 1), stacked(parts))
    return both[:, :LANES], both[:, LANES:]


def mass_weight():
    lane = iota((1, LANES), 1)
    r, c = lane // 8 % 4, lane % 4
    along_y = jnp.where((r == 0) | (r == 3), 1.0 / 6.0, 5.0 / 6.0)
    return along_y * jnp.where((c == 0) | (c == 3), 1.0 / 6.0, 5.0 / 6.0)


def assembled(inner, outer):
    shape = inner.shape
    row = iota(shape, 0)
    lane = iota(shape, 1)
    c = lane % 8
    r = lane // 8
    here = row < ROWS + 32
    from_before = here & (c == 0) & (row % 16 > 0)
    from_after = here & (c == 7) & (row % 16 < 15)
    summed = (
        inner
        + jnp.where(from_before, roll(outer, 1, 0), 0.0)
        + jnp.where(from_after, roll(outer, -1, 0), 0.0)
    )
    above = roll(summed, 8, 1)
    below = roll(summed, -8, 1)
    total = (
        summed
        + jnp.where((r % 4 == 0) & (r > 0), above, 0.0)
        + jnp.where((r % 4 == 3) & (r < 15), below, 0.0)
    )
    edge_rows = jnp.zeros((16, LANES), jnp.float32)
    above_block = [edge_rows, above[: ROWS - 16]]
    below_block = [below[16:ROWS], edge_rows]
    if shape[0] > ROWS:
        sides = slice(ROWS + 32, ROWS + 48)
        fy = iota((16, LANES), 0) % 8
        above_block += [edge_rows] * 2 + [jnp.where(fy > 0, roll(above[sides], 1, 0), 0.0)]
        below_block += [edge_rows] * 2 + [jnp.where(fy < 7, roll(below[sides], -1, 0), 0.0)]
    return (
        total
        + jnp.where(r == 0, stacked(above_block), 0.0)
        + jnp.where(r == 15, stacked(below_block), 0.0)
    )


def rim_rows(edge, base=0):
    if edge == 0:
        return pl.ds(base, 16)
    if edge == 1:
        return pl.ds(base + 15, 8, 16)
    if edge == 2:
        return pl.ds(base + 112, 16)
    return pl.ds(base, 8, 16)


def turned(u, v, quarter):
    quarter = quarter % 4
    if quarter == 0:
        return u, v
    if quarter == 1:
        return -v, u
    if quarter == 2:
        return -u, -v
    return v, -u


def ends_meet(ring, channels, table):
    ends = stacked(
        [ring[ch][row : row + 1] for ch in range(channels) for row in END_ROWS]
    )
    masks = table.left("masks").astype(jnp.float32)
    own = stacked([masks[0:8]] * channels)
    taken = dot(stacked(split(ends * own), 1), stacked([table.left("ends")] * 3))
    lines = []
    for ch in range(channels):
        line = jnp.sum(taken[8 * ch : 8 * ch + 8] * masks[8:16], axis=0, keepdims=True)
        lines.append(line * masks[16:24])
    given = dot(stacked(split(stacked(lines)), 1), stacked([table.right("ends")] * 3))
    given = [given[8 * ch : 8 * ch + 8] for ch in range(channels)]
    sense = masks[24:32]
    return [-sense * given[1], sense * given[0], *given[2:]]


def join(face_ref, ring, channels, table, ring_too=True):
    ends = ends_meet(ring, channels, table) if ring_too else None
    totals = []
    for ch in range(channels):
        south, north = ring[ch][0:16], ring[ch][16:32]
        east, west = ring[ch][32:40], ring[ch][40:48]
        rows = [rim_rows(edge, ROWS * ch) for edge in range(EDGES)]
        lane = iota((16, LANES), 1)
        lane_8 = iota((8, LANES), 1)
        if ring_too:
            block = iota((16, LANES), 0)
            fy = iota((8, LANES), 0)
            of_end = [ends[ch][t : t + 1] for t in range(8)]

            def at_ends(first, last, position, count):
                return jnp.where(
                    position == 0, first, jnp.where(position == count - 1, last, 0.0)
                )

            totals.append(
                stacked(
                    [
                        south
                        + jnp.where(lane // 8 == 15, roll(face_ref[rows[0], :], -8, 1), 0.0)
                        + at_ends(of_end[0], of_end[1], block, 16),
                        north
                        + jnp.where(lane // 8 == 0, roll(face_ref[rows[2], :], 8, 1), 0.0)
                        + at_ends(of_end[2], of_end[3], block, 16),
                        east
                        + jnp.where(lane_8 % 8 == 0, roll(face_ref[rows[1], :], -7, 1), 0.0)
                        + at_ends(of_end[4], of_end[5], fy, 8),
                        west
                        + jnp.where(lane_8 % 8 == 7, roll(face_ref[rows[3], :], 7, 1), 0.0)
                        + at_ends(of_end[6], of_end[7], fy, 8),
                    ]
                )
            )
        from_south = jnp.where(lane // 8 == 0, roll(south, 8, 1), 0.0)
        from_north = jnp.where(lane // 8 == 15, roll(north, -8, 1), 0.0)
        from_east = jnp.where(lane_8 % 8 == 7, roll(east, 7, 1), 0.0)
        from_west = jnp.where(lane_8 % 8 == 0, roll(west, -7, 1), 0.0)
        for edge, part in enumerate((from_south, from_east, from_north, from_west)):
            face_ref[rows[edge], :] = face_ref[rows[edge], :] + part
    return totals


def pack_kernel(
    state_ref, jac_ref, diag_ref, cross_ref, cor_ref, later_ref, out_ref, kept_ref, sem
):
    keep = pltpu.make_async_copy(later_ref, kept_ref, sem)
    keep.start()
    turned_state = jnp.transpose(state_ref[...])
    for part in range(3):
        out_ref[pl.ds(part, 64, 8), :] = turned_state[64 * part : 64 * part + 64]
    spread = jnp.where(iota((16, LANES), 1) // 8 == iota((16, LANES), 0), 1.0, 0.0)
    mask = jnp.where(iota((8, LANES), 1) % 8 == iota((8, LANES), 0), 1.0, 0.0)
    fields = [jac_ref[...], diag_ref[0], diag_ref[1], cross_ref[...], cor_ref[...]]
    lines = jnp.dot(
        stacked(fields),
        spread,
        precision=lax.Precision.HIGHEST,
        preferred_element_type=jnp.float32,
    )
    for k in range(5):
        line = jnp.sum(lines[8 * k : 8 * k + 8] * mask, axis=0, keepdims=True)
        out_ref[pl.ds(3 + k, 64, 8), :] = jnp.broadcast_to(line, (64, LANES))
    keep.wait()


def reversed_blocks(rows, table):
    parts = stacked([part.astype(jnp.float32) for part in split(rows)]).astype(jnp.bfloat16)
    moved = dot(parts, table.left("reverse"))
    count = rows.shape[0]
    moved = stacked([moved[n * count : n * count + count] for n in range(3)], 1)
    moved = dot(table.right("reverse"), moved.astype(jnp.bfloat16))
    return moved[:, :LANES] + moved[:, LANES : 2 * LANES] + moved[:, 2 * LANES :]


def strip_of(edge, fields_ref, table):
    rows = [fields_ref[rim_rows(edge, ROWS * k), :] for k in range(7)]
    rows = stacked([*rows, jnp.zeros_like(rows[0])])
    if edge == 0:
        return rows
    if edge == 2:
        return reversed_blocks(rows, table)
    name = "east" if edge == 1 else "west"
    moved = dot(stacked(split(rows)), table.whole(name + "_out"))
    halves = stacked([moved[:, :LANES], moved[:, LANES:]], 0)
    moved = stacked(
        [stacked([halves[64 * n : 64 * n + 64], halves[192 + 64 * n : 256 + 64 * n]]) for n in range(3)],
        1,
    )
    order = table.left("out_rows") if edge == 1 else table.right("out_rows")
    moved = dot(order, moved.astype(jnp.bfloat16))
    return moved[:, :LANES] + moved[:, LANES : 2 * LANES] + moved[:, 2 * LANES :]


def put_strips(fields_ref, nbr_ref, face, send_ref, table):
    near = iota((16, LANES), 1) < 64
    for edge in range(EDGES):
        rows = strip_of(edge, fields_ref, table)
        u, v, t, mass, flux_xx, flux_xy, flux_yy = [rows[16 * k : 16 * k + 16] for k in range(7)]
        u, v = turned(u, v, -edge)
        if edge % 2:
            flux_xx, flux_xy, flux_yy = flux_yy, -flux_xy, flux_xx
        slot = [
            jnp.where(near, low, roll(high, 64, 1))
            for low, high in ((u, v), (t, mass), (flux_xx, flux_xy))
        ]
        slot.append(jnp.where(near[:8], flux_yy[:8], roll(flux_yy[8:], 64, 1)))
        start = pl.multiple_of(SLOT * nbr_ref[edge, face], 8)
        send_ref[pl.ds(start, SLOT), :] = stacked(slot)


def ring_of(nbr_ref, face, got_ref, table):
    near = iota((16, LANES), 1) < 64
    strips = []
    for edge in range(EDGES):
        start = pl.multiple_of(SLOT * nbr_ref[edge, face], 8)
        slot = got_ref[pl.ds(start, SLOT), :]
        fields = []
        for n in range(3):
            rows = slot[16 * n : 16 * n + 16]
            fields += [jnp.where(near, rows, 0.0), jnp.where(near, roll(rows, 64, 1), 0.0)]
        rows = slot[48:56]
        fields.append(stacked([rows, roll(rows, 64, 1)]))
        fields[6] = jnp.where(near, fields[6], 0.0)
        rows = stacked([*fields, jnp.zeros_like(near, jnp.float32)])
        count = 16
        if edge == 0:
            rows = reversed_blocks(rows, table)
        elif edge % 2:
            name = "east" if edge == 1 else "west"
            order = table.left("in_rows") if edge == 1 else table.right("in_rows")
            moved = dot(order, stacked(split(rows), 1))
            moved = stacked([moved[:64], moved[64:]], 1)
            into = [table.left(name + "_in")] * 3 + [table.right(name + "_in")] * 3
            rows = dot(moved.astype(jnp.bfloat16), stacked(into))
            count = 8
        fields = [rows[count * k : count * k + count] for k in range(7)]
        fields[0], fields[1] = turned(fields[0], fields[1], edge + 2)
        if edge % 2:
            fields[4], fields[5], fields[6] = fields[6], -fields[5], fields[4]
        else:
            far = near if edge == 0 else ~near
            fields[3] = jnp.where(far, 1.0, fields[3])
        strips.append(fields)
    return [stacked([strips[edge][k] for edge in (0, 2, 1, 3)]) for k in range(7)]


def first_kernel(
    nbr_ref, own_ref, other_ref, table_ref, later_ref, fields_ref, send_ref, kept_ref, sem
):
    keep = pltpu.make_async_copy(later_ref, kept_ref, sem)
    keep.start()
    table = Table(table_ref, 0)
    core = lax.axis_index("fy") % 2
    face = lax.axis_index("face")
    fields = []
    for k in range(8):
        own = own_ref[pl.ds(k, 64, 8), :]
        other = other_ref[pl.ds(k, 64, 8), :]
        even = jnp.where(core == 0, own, other)
        odd = jnp.where(core == 0, other, own)
        pieces = []
        for x in range(4):
            pieces += [even[16 * x : 16 * x + 16], odd[16 * x : 16 * x + 16]]
        fields.append(stacked(pieces))
    u, v, t, volume, m_xx, m_yy, m_xy, planet = fields
    contra_u = m_xx * u + m_xy * v
    contra_v = m_xy * u + m_yy * v
    energy = 0.5 * (u * contra_u + v * contra_v) + t
    grad_x, grad_y = gradient(stacked([u, v, t, energy]), table)
    dy_u, dx_v = grad_y[:ROWS], grad_x[ROWS : 2 * ROWS]
    dx_t, dy_t = grad_x[2 * ROWS : 3 * ROWS], grad_y[2 * ROWS : 3 * ROWS]
    dx_e, dy_e = grad_x[3 * ROWS :], grad_y[3 * ROWS :]
    absolute = dx_v - dy_u + planet * volume
    mass = mass_weight() * volume
    raw_u = u + time_step * (absolute * contra_v - dx_e)
    raw_v = v + time_step * (-absolute * contra_u - dy_e)
    raw_t = t - time_step * (contra_u * dx_t + contra_v * dy_t)
    values = stacked([mass * raw_u, mass * raw_v, mass * raw_t, mass])
    sums = dot(stacked(split(values), 1), stacked([table.whole("both")] * 3))
    for ch in range(4):
        part = slice(ROWS * ch, ROWS * ch + ROWS)
        fields_ref[part, :] = assembled(sums[part, :LANES], sums[part, LANES:])
    for k, field in enumerate([m_xx, m_xy, m_yy]):
        fields_ref[ROWS * (4 + k) : ROWS * (5 + k), :] = volume * field
    put_strips(fields_ref, nbr_ref, face, send_ref, table)
    keep.wait()


def laplace(fields, metric, table):
    flux_xx, flux_xy, flux_yy = metric
    count = flux_xx.shape[0]
    grad_x, grad_y = gradient(stacked(fields), table)
    flux = []
    for ch in range(3):
        part = slice(count * ch, count * ch + count)
        flux.append(
            stacked(
                [
                    flux_xx * grad_x[part] + flux_xy * grad_y[part],
                    flux_xy * grad_x[part] + flux_yy * grad_y[part],
                ],
                1,
            )
        )
    high, mid, low = split(stacked(flux))
    parts = [table.part("spread", n, 2 * LANES) for n in (0, 0, 0, 1, 1, 2)]
    sums = dot(stacked([high, mid, low, high, mid, high], 1), stacked(parts))
    return [
        assembled(sums[count * ch : count * ch + count, :LANES], sums[count * ch : count * ch + count, LANES:])
        for ch in range(3)
    ]


def second_kernel(nbr_ref, got_ref, fields_ref, table_ref, out_ref, total_ref):
    table = Table(table_ref, 1)
    face = lax.axis_index("face")
    core = lax.axis_index("fy") % 2
    ring_fields = ring_of(nbr_ref, face, got_ref, table)
    metric = [
        stacked([fields_ref[ROWS * k : ROWS * k + ROWS, :], ring_fields[k]]) for k in range(4, 7)
    ]
    total_ref[...] = fields_ref[: 4 * ROWS, :]
    ring = join(total_ref, ring_fields[:4], 4, table)
    share = 1.0 / stacked([total_ref[3 * ROWS : 4 * ROWS, :], ring[3]])
    fields = [
        stacked([total_ref[ROWS * ch : ROWS * ch + ROWS, :], ring[ch]]) * share for ch in range(3)
    ]
    sectioned = [field[:ROWS] for field in fields]
    for step in range(2):
        sums = laplace(fields, metric, table)
        for ch in range(3):
            total_ref[ROWS * ch : ROWS * ch + ROWS, :] = sums[ch][:ROWS]
        ring = join(total_ref, [field[ROWS:] for field in sums], 3, table, step == 0)
        if step == 0:
            fields = [
                stacked([total_ref[ROWS * ch : ROWS * ch + ROWS, :], ring[ch]]) * share
                for ch in range(3)
            ]
    for ch in range(3):
        part = slice(ROWS * ch, ROWS * ch + ROWS)
        total_ref[part, :] = sectioned[ch] - hyper_coeff * (total_ref[part, :] * share[:ROWS])
    for x in range(4):
        for ch in range(3):
            start = pl.multiple_of(ROWS * ch + 32 * x + 16 * core, 16)
            out_ref[16 * x : 16 * x + 16, 0, LANES * ch : LANES * ch + LANES] = total_ref[
                pl.ds(start, 16), :
            ]


def unpack_kernel(got_ref, out_ref):
    levels = got_ref[...]
    columns = stacked([levels[:, 0, LANES * ch : LANES * ch + LANES] for ch in range(3)])
    out_ref[...] = jnp.transpose(columns)


def f32(*shape):
    return jax.ShapeDtypeStruct(shape, jnp.float32)


def near(*shape):
    return pltpu.VMEM(shape, jnp.float32)


def kept(table):
    return pltpu.VMEM(table.shape, jnp.bfloat16)


def held(values):
    return pltpu.with_memory_space_constraint(values, pltpu.VMEM)


VMEM = pl.BlockSpec(memory_space=pltpu.VMEM)
SMEM = pl.BlockSpec(memory_space=pltpu.SMEM)
ANY = pl.BlockSpec(memory_space=pl.ANY)


def call(kernel, outs, ins, scratch=(), name=None):
    return pl.pallas_call(
        kernel,
        out_shape=outs,
        in_specs=ins,
        out_specs=jax.tree.map(lambda _: VMEM, outs),
        scratch_shapes=scratch,
        name=name,
    )


def level_groups():
    return [
        [(8 * face + 2 * x + core) * 16 + fx for x in range(4) for fx in range(16)]
        for face in range(FACES)
        for core in range(2)
    ]


def per_device(state, jacobian, metric_diag, metric_cross, coriolis, nbr_face, nbr_edge):
    axes = ("face", "fy", "fx")
    groups = level_groups()
    tables = [jnp.asarray(table) for table in TABLES]
    packed, table = call(
        pack_kernel,
        [near(512, LANES), kept(TABLES[0])],
        [VMEM] * 5 + [ANY],
        [pltpu.SemaphoreType.DMA],
        name="pack",
    )(
        state.reshape(128, 192),
        jacobian[0].T,
        metric_diag[:, 0].transpose(0, 2, 1),
        metric_cross[0].T,
        coriolis[0].T,
        tables[0],
    )
    own = lax.all_to_all(
        packed.reshape(64, 8, LANES), axes, 0, 0, axis_index_groups=groups, tiled=True
    )
    other = lax.ppermute(own, "fy", [(i, i ^ 1) for i in range(8)])
    fields, send, table = call(
        first_kernel,
        [near(7 * ROWS, LANES), near(SLOT * FACES, LANES), kept(TABLES[1])],
        [SMEM] + [VMEM] * 3 + [ANY],
        [pltpu.SemaphoreType.DMA],
        name="first",
    )(
        nbr_face.T,
        held(own.reshape(512, LANES)),
        held(other.reshape(512, LANES)),
        held(table),
        tables[1],
    )
    got = lax.all_to_all(send.reshape(FACES, SLOT, LANES), "face", 0, 0, tiled=True)
    updated = call(
        second_kernel,
        near(64, 1, 3 * LANES),
        [SMEM] + [VMEM] * 3,
        [pltpu.VMEM((4 * ROWS, LANES), jnp.float32)],
        name="second",
    )(nbr_face.T, held(got.reshape(SLOT * FACES, LANES)), held(fields), held(table))
    back = lax.all_to_all(
        updated, axes, 0, 0, axis_index_groups=groups, tiled=True
    )
    nodes = call(unpack_kernel, f32(128, 192), [VMEM], name="unpack")(
        held(back)
    )
    return nodes.reshape(1, 16, 8, 192)


def solution(mesh):
    return jax.shard_map(
        per_device,
        mesh=mesh,
        in_specs=(
            P("face", "fy", "fx", None),
            P("face", "fy", "fx"),
            P(None, "face", "fy", "fx"),
            P("face", "fy", "fx"),
            P("face", "fy", "fx"),
            P(),
            P(),
        ),
        out_specs=P("face", "fy", "fx", None),
        check_vma=False,
    )
```

```python
import jax
import jax.numpy as jnp
import ml_dtypes
import numpy as np
from jax import lax
from jax.experimental import pallas as pl
from jax.experimental.pallas import tpu as pltpu
from jax.sharding import PartitionSpec as P

time_step = 0.05
hyper_coeff = 0.0005

FACES = 6
ROWS = 128
LANES = 128
EDGES = 4
RING_ROWS = 48
ALL_ROWS = ROWS + RING_ROWS
SLOT = 56
ENDS = ("S0", "S15", "N0", "N15", "E0", "E7", "W0", "W7")
END_ROWS = (0, 15, 16, 31, 32, 39, 40, 47)
MEETS = (6, 4, 7, 5, 1, 3, 0, 2)
TURNS = (1, -1, -1, 1, 1, -1, -1, 1)


def deriv_table():
    gll_nodes = np.array([-1.0, -1.0 / np.sqrt(5.0), 1.0 / np.sqrt(5.0), 1.0])
    bary_weights = np.ones(4)
    for j in range(4):
        for m in range(4):
            if m != j:
                bary_weights[j] = bary_weights[j] / (gll_nodes[j] - gll_nodes[m])
    matrix = np.zeros((4, 4))
    for i in range(4):
        for j in range(4):
            if i != j:
                matrix[i, j] = bary_weights[j] / bary_weights[i] / (gll_nodes[i] - gll_nodes[j])
        matrix[i, i] = -np.sum(matrix[i])
    return matrix


def in_parts(matrix):
    rest = np.asarray(matrix, np.float64)
    parts = []
    for _ in range(3):
        part = rest.astype(ml_dtypes.bfloat16)
        parts.append(part)
        rest = rest - part.astype(np.float64)
    return parts


def face_node(edge, depth, k):
    row, col = ((depth, k), (k, 127 - depth), (127 - depth, 127 - k), (127 - k, depth))[edge]
    return row // 16, col // 8, 8 * (row % 16) + col % 8


def ring_node(edge, depth, k):
    if edge == 1:
        return k // 16, 8 * (k % 16) + depth
    row = 127 - k
    return row // 16, 8 * (row % 16) + 7 - depth


def end_lane(end, depth):
    return {
        "S0": 8 * (15 - depth),
        "S15": 8 * (15 - depth) + 7,
        "N0": 8 * depth,
        "N15": 8 * depth + 7,
        "E0": depth,
        "E7": 120 + depth,
        "W0": 7 - depth,
        "W7": 127 - depth,
    }[end]


def tables():
    deriv = deriv_table()
    along_x = np.kron(np.eye(32), deriv.T)
    along_y = np.kron(np.kron(np.eye(4), deriv.T), np.eye(8))
    lane = np.arange(LANES)
    r, c = lane // 8, lane % 8
    weights = np.array([1.0, 5.0, 5.0, 1.0]) / 6.0
    within = np.eye(LANES)
    across = np.zeros((LANES, LANES))
    for l in range(LANES):
        if c[l] in (3, 4):
            within[l, l + 1 if c[l] == 3 else l - 1] = 1.0
        if c[l] == 7:
            across[l, l - 7] = 1.0
        if c[l] == 0:
            across[l, l + 7] = 1.0
    both = np.concatenate([within, across], 1)
    gradient = in_parts(np.concatenate([along_x, along_y], 1))
    weighted = np.diag(weights[r % 4] * weights[c % 4])
    spread = in_parts(np.concatenate([along_x @ weighted @ both, along_y @ weighted @ both], 0))

    out, out_rows, into, into_rows = [], [], [], []
    for edge in (1, 3):
        out.append(np.zeros((2, LANES, LANES)))
        out_rows.append(np.zeros((LANES, LANES)))
        into.append(np.zeros((2, LANES, LANES)))
        into_rows.append(np.zeros((LANES, LANES)))
        for k in range(128):
            j, i = k // 8, k % 8
            j2, i2 = (127 - k) // 8, (127 - k) % 8
            for depth in range(8):
                fy, _, at = face_node(edge, depth, k)
                out[-1][j % 2, at, 8 * depth + i] = 1.0
                ring_fy, ring_at = ring_node(edge, depth, k)
                into[-1][j2 % 2, 8 * depth + i2, ring_at] = 1.0
                for field in range(8):
                    out_rows[-1][16 * field + j, 64 * (j % 2) + 8 * field + fy] = 1.0
                    into_rows[-1][64 * (j2 % 2) + 8 * field + ring_fy, 16 * field + j2] = 1.0
    take = np.zeros((LANES, LANES))
    give = np.zeros((LANES, LANES))
    masks = np.zeros((32, 2 * LANES))
    for t, end in enumerate(ENDS):
        for depth in range(8):
            take[end_lane(end, depth), 8 * t + depth] = 1.0
            give[8 * t + depth, end_lane(ENDS[MEETS[t]], depth)] = 1.0
            masks[t, end_lane(end, depth)] = 1.0
            masks[8 + t, 8 * t + depth] = 1.0
            masks[16 + t, 8 * MEETS[t] + depth] = 1.0
        masks[24 + t] = TURNS[t]

    def pair(left, right):
        return np.concatenate([left, right], 1)

    reverse = pair(np.eye(LANES)[::-1], np.kron(np.eye(8), np.eye(16)[::-1]))
    groups = (
        {
            "gradient": np.concatenate(gradient, 0),
            "both": both,
            "east_out": pair(*out[0]),
            "west_out": pair(*out[1]),
            "out_rows": pair(*out_rows),
            "reverse": reverse,
        },
        {
            "gradient": np.concatenate(gradient, 0),
            "spread": np.concatenate(spread, 0),
            "east_in": pair(*into[0]),
            "west_in": pair(*into[1]),
            "in_rows": pair(*into_rows),
            "reverse": reverse,
            "ends": pair(take, give),
            "masks": masks,
        },
    )
    arrays, places = [], []
    for group in groups:
        start = 0
        places.append({})
        for name, matrix in group.items():
            places[-1][name] = (start, start + matrix.shape[0])
            start += matrix.shape[0]
        arrays.append(np.concatenate([m.astype(ml_dtypes.bfloat16) for m in group.values()], 0))
    return arrays, places


TABLES, PLACES = tables()


class Table:
    def __init__(self, ref, which):
        self.ref, self.places = ref, PLACES[which]

    def whole(self, name):
        start, end = self.places[name]
        return self.ref[start:end, :]

    def left(self, name):
        start, end = self.places[name]
        return self.ref[start:end, :LANES]

    def right(self, name):
        start, end = self.places[name]
        return self.ref[start:end, LANES:]

    def part(self, name, n, rows):
        start = self.places[name][0] + n * rows
        return self.ref[start : start + rows, :]


def roll(values, shift, axis):
    return pltpu.roll(values, shift % values.shape[axis], axis)


def iota(shape, dim):
    return lax.broadcasted_iota(jnp.int32, shape, dim)


def dot(a, b):
    return jnp.dot(a, b, preferred_element_type=jnp.float32)


def dot_halves(a, b):
    half = a.shape[0] // 32 * 16
    return jnp.concatenate([dot(a[:half], b), dot(a[half:], b)], axis=0)


def stacked(parts, axis=0):
    return jnp.concatenate(parts, axis=axis)


def split(values):
    high = values.astype(jnp.bfloat16)
    rest = values - high.astype(jnp.float32)
    mid = rest.astype(jnp.bfloat16)
    return high, mid, (rest - mid.astype(jnp.float32)).astype(jnp.bfloat16)


def gradient(values, table):
    high, mid, low = split(values)
    parts = [table.part("gradient", n, LANES) for n in (0, 0, 1, 1, 0, 2)]
    both = dot_halves(stacked([high, mid, high, mid, low, high], 1), stacked(parts))
    return both[:, :LANES], both[:, LANES:]


def mass_weight():
    lane = iota((1, LANES), 1)
    r, c = lane // 8 % 4, lane % 4
    along_y = jnp.where((r == 0) | (r == 3), 1.0 / 6.0, 5.0 / 6.0)
    return along_y * jnp.where((c == 0) | (c == 3), 1.0 / 6.0, 5.0 / 6.0)


def assembled(inner, outer):
    shape = inner.shape
    row = iota(shape, 0)
    lane = iota(shape, 1)
    c = lane % 8
    r = lane // 8
    here = row < ROWS + 32
    from_before = here & (c == 0) & (row % 16 > 0)
    from_after = here & (c == 7) & (row % 16 < 15)
    summed = (
        inner
        + jnp.where(from_before, roll(outer, 1, 0), 0.0)
        + jnp.where(from_after, roll(outer, -1, 0), 0.0)
    )
    above = roll(summed, 8, 1)
    below = roll(summed, -8, 1)
    total = (
        summed
        + jnp.where((r % 4 == 0) & (r > 0), above, 0.0)
        + jnp.where((r % 4 == 3) & (r < 15), below, 0.0)
    )
    edge_rows = jnp.zeros((16, LANES), jnp.float32)
    above_block = [edge_rows, above[: ROWS - 16]]
    below_block = [below[16:ROWS], edge_rows]
    if shape[0] > ROWS:
        sides = slice(ROWS + 32, ROWS + 48)
        fy = iota((16, LANES), 0) % 8
        above_block += [edge_rows] * 2 + [jnp.where(fy > 0, roll(above[sides], 1, 0), 0.0)]
        below_block += [edge_rows] * 2 + [jnp.where(fy < 7, roll(below[sides], -1, 0), 0.0)]
    return (
        total
        + jnp.where(r == 0, stacked(above_block), 0.0)
        + jnp.where(r == 15, stacked(below_block), 0.0)
    )


def rim_rows(edge, base=0):
    if edge == 0:
        return pl.ds(base, 16)
    if edge == 1:
        return pl.ds(base + 15, 8, 16)
    if edge == 2:
        return pl.ds(base + 112, 16)
    return pl.ds(base, 8, 16)


def turned(u, v, quarter):
    quarter = quarter % 4
    if quarter == 0:
        return u, v
    if quarter == 1:
        return -v, u
    if quarter == 2:
        return -u, -v
    return v, -u


def ends_meet(ring, channels, table):
    ends = stacked(
        [ring[ch][row : row + 1] for ch in range(channels) for row in END_ROWS]
    )
    masks = table.left("masks").astype(jnp.float32)
    own = stacked([masks[0:8]] * channels)
    taken = dot(stacked(split(ends * own), 1), stacked([table.left("ends")] * 3))
    lines = []
    for ch in range(channels):
        line = jnp.sum(taken[8 * ch : 8 * ch + 8] * masks[8:16], axis=0, keepdims=True)
        lines.append(line * masks[16:24])
    given = dot(stacked(split(stacked(lines)), 1), stacked([table.right("ends")] * 3))
    given = [given[8 * ch : 8 * ch + 8] for ch in range(channels)]
    sense = masks[24:32]
    return [-sense * given[1], sense * given[0], *given[2:]]


def join(face_ref, ring, channels, table, ring_too=True):
    ends = ends_meet(ring, channels, table) if ring_too else None
    totals = []
    for ch in range(channels):
        south, north = ring[ch][0:16], ring[ch][16:32]
        east, west = ring[ch][32:40], ring[ch][40:48]
        rows = [rim_rows(edge, ROWS * ch) for edge in range(EDGES)]
        lane = iota((16, LANES), 1)
        lane_8 = iota((8, LANES), 1)
        if ring_too:
            block = iota((16, LANES), 0)
            fy = iota((8, LANES), 0)
            of_end = [ends[ch][t : t + 1] for t in range(8)]

            def at_ends(first, last, position, count):
                return jnp.where(
                    position == 0, first, jnp.where(position == count - 1, last, 0.0)
                )

            totals.append(
                stacked(
                    [
                        south
                        + jnp.where(lane // 8 == 15, roll(face_ref[rows[0], :], -8, 1), 0.0)
                        + at_ends(of_end[0], of_end[1], block, 16),
                        north
                        + jnp.where(lane // 8 == 0, roll(face_ref[rows[2], :], 8, 1), 0.0)
                        + at_ends(of_end[2], of_end[3], block, 16),
                        east
                        + jnp.where(lane_8 % 8 == 0, roll(face_ref[rows[1], :], -7, 1), 0.0)
                        + at_ends(of_end[4], of_end[5], fy, 8),
                        west
                        + jnp.where(lane_8 % 8 == 7, roll(face_ref[rows[3], :], 7, 1), 0.0)
                        + at_ends(of_end[6], of_end[7], fy, 8),
                    ]
                )
            )
        from_south = jnp.where(lane // 8 == 0, roll(south, 8, 1), 0.0)
        from_north = jnp.where(lane // 8 == 15, roll(north, -8, 1), 0.0)
        from_east = jnp.where(lane_8 % 8 == 7, roll(east, 7, 1), 0.0)
        from_west = jnp.where(lane_8 % 8 == 0, roll(west, -7, 1), 0.0)
        for edge, part in enumerate((from_south, from_east, from_north, from_west)):
            face_ref[rows[edge], :] = face_ref[rows[edge], :] + part
    return totals


def pack_kernel(state_ref, jac_ref, diag_ref, cross_ref, cor_ref, out_ref):
    turned_state = jnp.transpose(state_ref[...])
    for part in range(3):
        out_ref[pl.ds(part, 64, 8), :] = turned_state[64 * part : 64 * part + 64]
    spread = jnp.where(iota((16, LANES), 1) // 8 == iota((16, LANES), 0), 1.0, 0.0)
    mask = jnp.where(iota((8, LANES), 1) % 8 == iota((8, LANES), 0), 1.0, 0.0)
    fields = [jac_ref[...], diag_ref[0], diag_ref[1], cross_ref[...], cor_ref[...]]
    lines = jnp.dot(
        stacked(fields),
        spread,
        precision=lax.Precision.HIGHEST,
        preferred_element_type=jnp.float32,
    )
    for k in range(5):
        line = jnp.sum(lines[8 * k : 8 * k + 8] * mask, axis=0, keepdims=True)
        out_ref[pl.ds(3 + k, 64, 8), :] = jnp.broadcast_to(line, (64, LANES))


def keep_kernel(after_ref, table_ref, kept_ref, sem):
    del after_ref
    keep = pltpu.make_async_copy(table_ref, kept_ref, sem)
    keep.start()
    keep.wait()


def reversed_blocks(rows, table):
    parts = stacked([part.astype(jnp.float32) for part in split(rows)]).astype(jnp.bfloat16)
    moved = dot(parts, table.left("reverse"))
    count = rows.shape[0]
    moved = stacked([moved[n * count : n * count + count] for n in range(3)], 1)
    moved = dot(table.right("reverse"), moved.astype(jnp.bfloat16))
    return moved[:, :LANES] + moved[:, LANES : 2 * LANES] + moved[:, 2 * LANES :]


def strip_of(edge, fields_ref, table):
    rows = [fields_ref[rim_rows(edge, ROWS * k), :] for k in range(7)]
    rows = stacked([*rows, jnp.zeros_like(rows[0])])
    if edge == 0:
        return rows
    if edge == 2:
        return reversed_blocks(rows, table)
    name = "east" if edge == 1 else "west"
    moved = dot(stacked(split(rows)), table.whole(name + "_out"))
    halves = stacked([moved[:, :LANES], moved[:, LANES:]], 0)
    moved = stacked(
        [stacked([halves[64 * n : 64 * n + 64], halves[192 + 64 * n : 256 + 64 * n]]) for n in range(3)],
        1,
    )
    order = table.left("out_rows") if edge == 1 else table.right("out_rows")
    moved = dot(order, moved.astype(jnp.bfloat16))
    return moved[:, :LANES] + moved[:, LANES : 2 * LANES] + moved[:, 2 * LANES :]


def put_strips(fields_ref, nbr_ref, face, send_ref, table):
    near = iota((16, LANES), 1) < 64
    strips = [strip_of(edge, fields_ref, table) for edge in range(EDGES)]
    for edge, rows in enumerate(strips):
        u, v, t, mass, flux_xx, flux_xy, flux_yy = [rows[16 * k : 16 * k + 16] for k in range(7)]
        u, v = turned(u, v, -edge)
        if edge % 2:
            flux_xx, flux_xy, flux_yy = flux_yy, -flux_xy, flux_xx
        slot = [
            jnp.where(near, low, roll(high, 64, 1))
            for low, high in ((u, v), (t, mass), (flux_xx, flux_xy))
        ]
        slot.append(jnp.where(near[:8], flux_yy[:8], roll(flux_yy[8:], 64, 1)))
        start = pl.multiple_of(SLOT * nbr_ref[edge, face], 8)
        send_ref[pl.ds(start, SLOT), :] = stacked(slot)


def ring_of(which_ref, got_ref, table):
    near = iota((16, LANES), 1) < 64
    strips = []
    for edge in range(EDGES):
        slot = got_ref[:SLOT, :]
        which = jnp.broadcast_to(which_ref[edge : edge + 1, :], (SLOT, LANES))
        for other in range(1, FACES):
            slot = jnp.where(which == other, got_ref[SLOT * other : SLOT * other + SLOT, :], slot)
        fields = []
        for n in range(3):
            rows = slot[16 * n : 16 * n + 16]
            fields += [jnp.where(near, rows, 0.0), jnp.where(near, roll(rows, 64, 1), 0.0)]
        rows = slot[48:56]
        fields.append(stacked([rows, roll(rows, 64, 1)]))
        fields[6] = jnp.where(near, fields[6], 0.0)
        rows = stacked([*fields, jnp.zeros_like(near, jnp.float32)])
        count = 16
        if edge == 0:
            rows = reversed_blocks(rows, table)
        elif edge % 2:
            name = "east" if edge == 1 else "west"
            order = table.left("in_rows") if edge == 1 else table.right("in_rows")
            moved = dot(order, stacked(split(rows), 1))
            moved = stacked([moved[:64], moved[64:]], 1)
            into = [table.left(name + "_in")] * 3 + [table.right(name + "_in")] * 3
            rows = dot(moved.astype(jnp.bfloat16), stacked(into))
            count = 8
        fields = [rows[count * k : count * k + count] for k in range(7)]
        fields[0], fields[1] = turned(fields[0], fields[1], edge + 2)
        if edge % 2:
            fields[4], fields[5], fields[6] = fields[6], -fields[5], fields[4]
        else:
            far = near if edge == 0 else ~near
            fields[3] = jnp.where(far, 1.0, fields[3])
        strips.append(fields)
    return [stacked([strips[edge][k] for edge in (0, 2, 1, 3)]) for k in range(7)]


def first_kernel(
    nbr_from, own_ref, other_ref, table_ref, later_ref,
    fields_ref, send_ref, which_ref, kept_ref, nbr_ref, nbr_sem, sem,
):
    fetch = pltpu.make_async_copy(nbr_from, nbr_ref, nbr_sem)
    fetch.start()
    keep = pltpu.make_async_copy(later_ref, kept_ref, sem)
    keep.start()
    table = Table(table_ref, 0)
    core = lax.axis_index("fy") % 2
    face = lax.axis_index("face")
    fields = []
    for k in range(8):
        own = own_ref[pl.ds(k, 64, 8), :]
        other = other_ref[pl.ds(k, 64, 8), :]
        even = jnp.where(core == 0, own, other)
        odd = jnp.where(core == 0, other, own)
        pieces = []
        for x in range(4):
            pieces += [even[16 * x : 16 * x + 16], odd[16 * x : 16 * x + 16]]
        fields.append(stacked(pieces))
    u, v, t, volume, m_xx, m_yy, m_xy, planet = fields
    contra_u = m_xx * u + m_xy * v
    contra_v = m_xy * u + m_yy * v
    energy = 0.5 * (u * contra_u + v * contra_v) + t
    grad_x, grad_y = gradient(stacked([u, v, t, energy]), table)
    dy_u, dx_v = grad_y[:ROWS], grad_x[ROWS : 2 * ROWS]
    dx_t, dy_t = grad_x[2 * ROWS : 3 * ROWS], grad_y[2 * ROWS : 3 * ROWS]
    dx_e, dy_e = grad_x[3 * ROWS :], grad_y[3 * ROWS :]
    absolute = dx_v - dy_u + planet * volume
    mass = mass_weight() * volume
    raw_u = u + time_step * (absolute * contra_v - dx_e)
    raw_v = v + time_step * (-absolute * contra_u - dy_e)
    raw_t = t - time_step * (contra_u * dx_t + contra_v * dy_t)
    values = stacked([mass * raw_u, mass * raw_v, mass * raw_t, mass])
    sums = dot_halves(stacked(split(values), 1), stacked([table.whole("both")] * 3))
    for ch in range(4):
        part = slice(ROWS * ch, ROWS * ch + ROWS)
        fields_ref[part, :] = assembled(sums[part, :LANES], sums[part, LANES:])
    for k, field in enumerate([m_xx, m_xy, m_yy]):
        fields_ref[ROWS * (4 + k) : ROWS * (5 + k), :] = volume * field
    fetch.wait()
    for edge in range(8):
        which_ref[edge : edge + 1, :] = jnp.full((1, LANES), nbr_ref[edge % EDGES, face], jnp.int32)
    put_strips(fields_ref, nbr_ref, face, send_ref, table)
    keep.wait()


def laplace(fields, metric, table):
    flux_xx, flux_xy, flux_yy = metric
    count = flux_xx.shape[0]
    grad_x, grad_y = gradient(stacked(fields), table)
    flux = []
    for ch in range(3):
        part = slice(count * ch, count * ch + count)
        flux.append(
            stacked(
                [
                    flux_xx * grad_x[part] + flux_xy * grad_y[part],
                    flux_xy * grad_x[part] + flux_yy * grad_y[part],
                ],
                1,
            )
        )
    high, mid, low = split(stacked(flux))
    parts = [table.part("spread", n, 2 * LANES) for n in (0, 0, 0, 1, 1, 2)]
    sums = dot_halves(stacked([high, mid, low, high, mid, high], 1), stacked(parts))
    return [
        assembled(sums[count * ch : count * ch + count, :LANES], sums[count * ch : count * ch + count, LANES:])
        for ch in range(3)
    ]


def second_kernel(which_ref, got_ref, fields_ref, table_ref, out_ref, total_ref):
    table = Table(table_ref, 1)
    core = lax.axis_index("fy") % 2
    ring_fields = ring_of(which_ref, got_ref, table)
    metric = [
        stacked([fields_ref[ROWS * k : ROWS * k + ROWS, :], ring_fields[k]]) for k in range(4, 7)
    ]
    total_ref[...] = fields_ref[: 4 * ROWS, :]
    ring = join(total_ref, ring_fields[:4], 4, table)
    share = 1.0 / stacked([total_ref[3 * ROWS : 4 * ROWS, :], ring[3]])
    fields = [
        stacked([total_ref[ROWS * ch : ROWS * ch + ROWS, :], ring[ch]]) * share for ch in range(3)
    ]
    sectioned = [field[:ROWS] for field in fields]
    for step in range(2):
        sums = laplace(fields, metric, table)
        for ch in range(3):
            total_ref[ROWS * ch : ROWS * ch + ROWS, :] = sums[ch][:ROWS]
        ring = join(total_ref, [field[ROWS:] for field in sums], 3, table, step == 0)
        if step == 0:
            fields = [
                stacked([total_ref[ROWS * ch : ROWS * ch + ROWS, :], ring[ch]]) * share
                for ch in range(3)
            ]
    for ch in range(3):
        part = slice(ROWS * ch, ROWS * ch + ROWS)
        total_ref[part, :] = sectioned[ch] - hyper_coeff * (total_ref[part, :] * share[:ROWS])
    for x in range(4):
        for ch in range(3):
            start = pl.multiple_of(ROWS * ch + 32 * x + 16 * core, 16)
            out_ref[16 * x : 16 * x + 16, 0, LANES * ch : LANES * ch + LANES] = total_ref[
                pl.ds(start, 16), :
            ]


def unpack_kernel(got_ref, out_ref):
    levels = got_ref[...]
    columns = stacked([levels[:, 0, LANES * ch : LANES * ch + LANES] for ch in range(3)])
    out_ref[...] = jnp.transpose(columns)


def f32(*shape):
    return jax.ShapeDtypeStruct(shape, jnp.float32)


def near(*shape):
    return pltpu.VMEM(shape, jnp.float32)


def kept(table):
    return pltpu.VMEM(table.shape, jnp.bfloat16)


def held(values):
    return pltpu.with_memory_space_constraint(values, pltpu.VMEM)


VMEM = pl.BlockSpec(memory_space=pltpu.VMEM)
ANY = pl.BlockSpec(memory_space=pl.ANY)


def call(kernel, outs, ins, scratch=(), name=None):
    return pl.pallas_call(
        kernel,
        out_shape=outs,
        in_specs=ins,
        out_specs=jax.tree.map(lambda _: VMEM, outs),
        scratch_shapes=scratch,
        name=name,
    )


def level_groups():
    return [
        [(8 * face + 2 * x + core) * 16 + fx for x in range(4) for fx in range(16)]
        for face in range(FACES)
        for core in range(2)
    ]


def per_device(state, jacobian, metric_diag, metric_cross, coriolis, nbr_face, nbr_edge):
    axes = ("face", "fy", "fx")
    groups = level_groups()
    tables = [jnp.asarray(table) for table in TABLES]
    packed = call(pack_kernel, near(512, LANES), [VMEM] * 5, name="pack")(
        state.reshape(128, 192),
        jacobian[0].T,
        metric_diag[:, 0].transpose(0, 2, 1),
        metric_cross[0].T,
        coriolis[0].T,
    )
    own = lax.all_to_all(
        packed.reshape(64, 8, LANES), axes, 0, 0, axis_index_groups=groups, tiled=True
    )
    other = lax.ppermute(own, "fy", [(i, i ^ 1) for i in range(8)])
    table = call(
        keep_kernel,
        kept(TABLES[0]),
        [VMEM, ANY],
        [pltpu.SemaphoreType.DMA],
        name="keep",
    )(held(own.reshape(512, LANES)), tables[0])
    fields, send, which, table = call(
        first_kernel,
        [
            near(7 * ROWS, LANES),
            near(SLOT * FACES, LANES),
            pltpu.VMEM((8, LANES), jnp.int32),
            kept(TABLES[1]),
        ],
        [ANY] + [VMEM] * 3 + [ANY],
        [
            pltpu.SMEM((EDGES, FACES), jnp.int32),
            pltpu.SemaphoreType.DMA,
            pltpu.SemaphoreType.DMA,
        ],
        name="first",
    )(
        nbr_face.T,
        held(own.reshape(512, LANES)),
        held(other.reshape(512, LANES)),
        held(table),
        tables[1],
    )
    got = lax.all_to_all(send.reshape(FACES, SLOT, LANES), "face", 0, 0, tiled=True)
    updated = call(
        second_kernel,
        near(64, 1, 3 * LANES),
        [VMEM] * 4,
        [pltpu.VMEM((4 * ROWS, LANES), jnp.float32)],
        name="second",
    )(held(which), held(got.reshape(SLOT * FACES, LANES)), held(fields), held(table))
    back = lax.all_to_all(
        updated, axes, 0, 0, axis_index_groups=groups, tiled=True
    )
    nodes = call(unpack_kernel, f32(128, 192), [VMEM], name="unpack")(
        held(back)
    )
    return nodes.reshape(1, 16, 8, 192)


def solution(mesh):
    return jax.shard_map(
        per_device,
        mesh=mesh,
        in_specs=(
            P("face", "fy", "fx", None),
            P("face", "fy", "fx"),
            P(None, "face", "fy", "fx"),
            P("face", "fy", "fx"),
            P("face", "fy", "fx"),
            P(),
            P(),
        ),
        out_specs=P("face", "fy", "fx", None),
        check_vma=False,
    )
```

```python
import jax
import jax.numpy as jnp
import ml_dtypes
import numpy as np
from jax import lax
from jax.experimental import pallas as pl
from jax.experimental.pallas import tpu as pltpu
from jax.sharding import PartitionSpec as P

time_step = 0.05
hyper_coeff = 0.0005

FACES = 6
ROWS = 128
LANES = 128
EDGES = 4
RING_ROWS = 48
ALL_ROWS = ROWS + RING_ROWS
SLOT = 56
ENDS = ("S0", "S15", "N0", "N15", "E0", "E7", "W0", "W7")
END_ROWS = (0, 15, 16, 31, 32, 39, 40, 47)
MEETS = (6, 4, 7, 5, 1, 3, 0, 2)
TURNS = (1, -1, -1, 1, 1, -1, -1, 1)


def deriv_table():
    gll_nodes = np.array([-1.0, -1.0 / np.sqrt(5.0), 1.0 / np.sqrt(5.0), 1.0])
    bary_weights = np.ones(4)
    for j in range(4):
        for m in range(4):
            if m != j:
                bary_weights[j] = bary_weights[j] / (gll_nodes[j] - gll_nodes[m])
    matrix = np.zeros((4, 4))
    for i in range(4):
        for j in range(4):
            if i != j:
                matrix[i, j] = bary_weights[j] / bary_weights[i] / (gll_nodes[i] - gll_nodes[j])
        matrix[i, i] = -np.sum(matrix[i])
    return matrix


def in_parts(matrix):
    rest = np.asarray(matrix, np.float64)
    parts = []
    for _ in range(3):
        part = rest.astype(ml_dtypes.bfloat16)
        parts.append(part)
        rest = rest - part.astype(np.float64)
    return parts


def face_node(edge, depth, k):
    row, col = ((depth, k), (k, 127 - depth), (127 - depth, 127 - k), (127 - k, depth))[edge]
    return row // 16, col // 8, 8 * (row % 16) + col % 8


def ring_node(edge, depth, k):
    if edge == 1:
        return k // 16, 8 * (k % 16) + depth
    row = 127 - k
    return row // 16, 8 * (row % 16) + 7 - depth


def end_lane(end, depth):
    return {
        "S0": 8 * (15 - depth),
        "S15": 8 * (15 - depth) + 7,
        "N0": 8 * depth,
        "N15": 8 * depth + 7,
        "E0": depth,
        "E7": 120 + depth,
        "W0": 7 - depth,
        "W7": 127 - depth,
    }[end]


def tables():
    deriv = deriv_table()
    along_x = np.kron(np.eye(32), deriv.T)
    along_y = np.kron(np.kron(np.eye(4), deriv.T), np.eye(8))
    lane = np.arange(LANES)
    r, c = lane // 8, lane % 8
    weights = np.array([1.0, 5.0, 5.0, 1.0]) / 6.0
    within = np.eye(LANES)
    across = np.zeros((LANES, LANES))
    for l in range(LANES):
        if c[l] in (3, 4):
            within[l, l + 1 if c[l] == 3 else l - 1] = 1.0
        if c[l] == 7:
            across[l, l - 7] = 1.0
        if c[l] == 0:
            across[l, l + 7] = 1.0
    both = np.concatenate([within, across], 1)
    gradient = in_parts(np.concatenate([along_x, along_y], 1))
    weighted = np.diag(weights[r % 4] * weights[c % 4])
    spread = in_parts(np.concatenate([along_x @ weighted @ both, along_y @ weighted @ both], 0))

    out, out_rows, into, into_rows = [], [], [], []
    for edge in (1, 3):
        out.append(np.zeros((2, LANES, LANES)))
        out_rows.append(np.zeros((LANES, LANES)))
        into.append(np.zeros((2, LANES, LANES)))
        into_rows.append(np.zeros((LANES, LANES)))
        for k in range(128):
            j, i = k // 8, k % 8
            j2, i2 = (127 - k) // 8, (127 - k) % 8
            for depth in range(8):
                fy, _, at = face_node(edge, depth, k)
                out[-1][j % 2, at, 8 * depth + i] = 1.0
                ring_fy, ring_at = ring_node(edge, depth, k)
                into[-1][j2 % 2, 8 * depth + i2, ring_at] = 1.0
                for field in range(8):
                    out_rows[-1][16 * field + j, 64 * (j % 2) + 8 * field + fy] = 1.0
                    into_rows[-1][64 * (j2 % 2) + 8 * field + ring_fy, 16 * field + j2] = 1.0
    take = np.zeros((LANES, LANES))
    give = np.zeros((LANES, LANES))
    masks = np.zeros((32, 2 * LANES))
    for t, end in enumerate(ENDS):
        for depth in range(8):
            take[end_lane(end, depth), 8 * t + depth] = 1.0
            give[8 * t + depth, end_lane(ENDS[MEETS[t]], depth)] = 1.0
            masks[t, end_lane(end, depth)] = 1.0
            masks[8 + t, 8 * t + depth] = 1.0
            masks[16 + t, 8 * MEETS[t] + depth] = 1.0
        masks[24 + t] = TURNS[t]

    def pair(left, right):
        return np.concatenate([left, right], 1)

    reverse = pair(np.eye(LANES)[::-1], np.kron(np.eye(8), np.eye(16)[::-1]))
    groups = (
        {
            "gradient": np.concatenate(gradient, 0),
            "both": both,
            "east_out": pair(*out[0]),
            "west_out": pair(*out[1]),
            "out_rows": pair(*out_rows),
            "reverse": reverse,
        },
        {
            "gradient": np.concatenate(gradient, 0),
            "spread": np.concatenate(spread, 0),
            "east_in": pair(*into[0]),
            "west_in": pair(*into[1]),
            "in_rows": pair(*into_rows),
            "reverse": reverse,
            "ends": pair(take, give),
            "masks": masks,
        },
    )
    arrays, places = [], []
    for group in groups:
        start = 0
        places.append({})
        for name, matrix in group.items():
            places[-1][name] = (start, start + matrix.shape[0])
            start += matrix.shape[0]
        arrays.append(np.concatenate([m.astype(ml_dtypes.bfloat16) for m in group.values()], 0))
    return arrays, places


TABLES, PLACES = tables()


class Table:
    def __init__(self, ref, which):
        self.ref, self.places = ref, PLACES[which]

    def whole(self, name):
        start, end = self.places[name]
        return self.ref[start:end, :]

    def left(self, name):
        start, end = self.places[name]
        return self.ref[start:end, :LANES]

    def right(self, name):
        start, end = self.places[name]
        return self.ref[start:end, LANES:]

    def part(self, name, n, rows):
        start = self.places[name][0] + n * rows
        return self.ref[start : start + rows, :]


def roll(values, shift, axis):
    return pltpu.roll(values, shift % values.shape[axis], axis)


def iota(shape, dim):
    return lax.broadcasted_iota(jnp.int32, shape, dim)


def dot(a, b):
    return jnp.dot(a, b, preferred_element_type=jnp.float32)


def dot_halves(a, b):
    half = a.shape[0] // 32 * 16
    return jnp.concatenate([dot(a[:half], b), dot(a[half:], b)], axis=0)


def stacked(parts, axis=0):
    return jnp.concatenate(parts, axis=axis)


def split(values):
    high = values.astype(jnp.bfloat16)
    rest = values - high.astype(jnp.float32)
    mid = rest.astype(jnp.bfloat16)
    return high, mid, (rest - mid.astype(jnp.float32)).astype(jnp.bfloat16)


def gradient(values, table, parts=3):
    high, mid, low = split(values)
    left = [high, mid, high, mid, low, high][: 2 * parts]
    right = [table.part("gradient", n, LANES) for n in (0, 0, 1, 1, 0, 2)[: 2 * parts]]
    both = dot_halves(stacked(left, 1), stacked(right))
    return both[:, :LANES], both[:, LANES:]


def mass_weight():
    lane = iota((1, LANES), 1)
    r, c = lane // 8 % 4, lane % 4
    along_y = jnp.where((r == 0) | (r == 3), 1.0 / 6.0, 5.0 / 6.0)
    return along_y * jnp.where((c == 0) | (c == 3), 1.0 / 6.0, 5.0 / 6.0)


def assembled(inner, outer):
    shape = inner.shape
    row = iota(shape, 0)
    lane = iota(shape, 1)
    c = lane % 8
    r = lane // 8
    here = row < ROWS + 32
    from_before = here & (c == 0) & (row % 16 > 0)
    from_after = here & (c == 7) & (row % 16 < 15)
    summed = (
        inner
        + jnp.where(from_before, roll(outer, 1, 0), 0.0)
        + jnp.where(from_after, roll(outer, -1, 0), 0.0)
    )
    above = roll(summed, 8, 1)
    below = roll(summed, -8, 1)
    total = (
        summed
        + jnp.where((r % 4 == 0) & (r > 0), above, 0.0)
        + jnp.where((r % 4 == 3) & (r < 15), below, 0.0)
    )
    edge_rows = jnp.zeros((16, LANES), jnp.float32)
    above_block = [edge_rows, above[: ROWS - 16]]
    below_block = [below[16:ROWS], edge_rows]
    if shape[0] > ROWS:
        sides = slice(ROWS + 32, ROWS + 48)
        fy = iota((16, LANES), 0) % 8
        above_block += [edge_rows] * 2 + [jnp.where(fy > 0, roll(above[sides], 1, 0), 0.0)]
        below_block += [edge_rows] * 2 + [jnp.where(fy < 7, roll(below[sides], -1, 0), 0.0)]
    return (
        total
        + jnp.where(r == 0, stacked(above_block), 0.0)
        + jnp.where(r == 15, stacked(below_block), 0.0)
    )


def rim_rows(edge, base=0):
    if edge == 0:
        return pl.ds(base, 16)
    if edge == 1:
        return pl.ds(base + 15, 8, 16)
    if edge == 2:
        return pl.ds(base + 112, 16)
    return pl.ds(base, 8, 16)


def turned(u, v, quarter):
    quarter = quarter % 4
    if quarter == 0:
        return u, v
    if quarter == 1:
        return -v, u
    if quarter == 2:
        return -u, -v
    return v, -u


def ends_meet(ring, channels, table):
    ends = stacked(
        [ring[ch][row : row + 1] for ch in range(channels) for row in END_ROWS]
    )
    masks = table.left("masks").astype(jnp.float32)
    own = stacked([masks[0:8]] * channels)
    taken = dot(stacked(split(ends * own), 1), stacked([table.left("ends")] * 3))
    lines = []
    for ch in range(channels):
        line = jnp.sum(taken[8 * ch : 8 * ch + 8] * masks[8:16], axis=0, keepdims=True)
        lines.append(line * masks[16:24])
    given = dot(stacked(split(stacked(lines)), 1), stacked([table.right("ends")] * 3))
    given = [given[8 * ch : 8 * ch + 8] for ch in range(channels)]
    sense = masks[24:32]
    return [-sense * given[1], sense * given[0], *given[2:]]


def placed_ends(ends):
    block, fy = iota((16, LANES), 0), iota((8, LANES), 0)
    parts = []
    for side, position, count in ((0, block, 16), (1, block, 16), (2, fy, 8), (3, fy, 8)):
        first, last = ends[2 * side : 2 * side + 1], ends[2 * side + 1 : 2 * side + 2]
        parts.append(
            jnp.where(position == 0, first, jnp.where(position == count - 1, last, 0.0))
        )
    return stacked(parts)


def join(face_ref, ring, channels, ends=None):
    totals = []
    lane = iota((16, LANES), 1)
    lane_8 = iota((8, LANES), 1)
    for ch in range(channels):
        south, north = ring[ch][0:16], ring[ch][16:32]
        east, west = ring[ch][32:40], ring[ch][40:48]
        rows = [rim_rows(edge, ROWS * ch) for edge in range(EDGES)]
        if ends is not None:
            rims = [
                jnp.where(lane // 8 == 15, roll(face_ref[rows[0], :], -8, 1), 0.0),
                jnp.where(lane // 8 == 0, roll(face_ref[rows[2], :], 8, 1), 0.0),
                jnp.where(lane_8 % 8 == 0, roll(face_ref[rows[1], :], -7, 1), 0.0),
                jnp.where(lane_8 % 8 == 7, roll(face_ref[rows[3], :], 7, 1), 0.0),
            ]
            totals.append(ring[ch] + ends[ch] + stacked(rims))
        from_south = jnp.where(lane // 8 == 0, roll(south, 8, 1), 0.0)
        from_north = jnp.where(lane // 8 == 15, roll(north, -8, 1), 0.0)
        from_east = jnp.where(lane_8 % 8 == 7, roll(east, 7, 1), 0.0)
        from_west = jnp.where(lane_8 % 8 == 0, roll(west, -7, 1), 0.0)
        for edge, part in enumerate((from_south, from_east, from_north, from_west)):
            face_ref[rows[edge], :] = face_ref[rows[edge], :] + part
    return totals


def pack_kernel(state_ref, jac_ref, diag_ref, cross_ref, cor_ref, out_ref):
    turned_state = jnp.transpose(state_ref[...])
    for part in range(3):
        out_ref[pl.ds(part, 64, 8), :] = turned_state[64 * part : 64 * part + 64]
    spread = jnp.where(iota((16, LANES), 1) // 8 == iota((16, LANES), 0), 1.0, 0.0)
    mask = jnp.where(iota((8, LANES), 1) % 8 == iota((8, LANES), 0), 1.0, 0.0)
    fields = [jac_ref[...], diag_ref[0], diag_ref[1], cross_ref[...], cor_ref[...]]
    lines = jnp.dot(
        stacked(fields),
        spread,
        precision=lax.Precision.HIGHEST,
        preferred_element_type=jnp.float32,
    )
    for k in range(5):
        line = jnp.sum(lines[8 * k : 8 * k + 8] * mask, axis=0, keepdims=True)
        out_ref[pl.ds(3 + k, 64, 8), :] = jnp.broadcast_to(line, (64, LANES))


def keep_kernel(after_ref, table_ref, kept_ref, sem):
    del after_ref
    keep = pltpu.make_async_copy(table_ref, kept_ref, sem)
    keep.start()
    keep.wait()


def reversed_blocks(rows, table):
    parts = stacked([part.astype(jnp.float32) for part in split(rows)]).astype(jnp.bfloat16)
    moved = dot(parts, table.left("reverse"))
    count = rows.shape[0]
    moved = stacked([moved[n * count : n * count + count] for n in range(3)], 1)
    moved = dot(table.right("reverse"), moved.astype(jnp.bfloat16))
    return moved[:, :LANES] + moved[:, LANES : 2 * LANES] + moved[:, 2 * LANES :]


def strip_of(edge, fields_ref, table):
    rows = [fields_ref[rim_rows(edge, ROWS * k), :] for k in range(7)]
    rows = stacked([*rows, jnp.zeros_like(rows[0])])
    if edge == 0:
        return rows
    if edge == 2:
        return reversed_blocks(rows, table)
    name = "east" if edge == 1 else "west"
    moved = dot(stacked(split(rows)), table.whole(name + "_out"))
    halves = stacked([moved[:, :LANES], moved[:, LANES:]], 0)
    moved = stacked(
        [stacked([halves[64 * n : 64 * n + 64], halves[192 + 64 * n : 256 + 64 * n]]) for n in range(3)],
        1,
    )
    order = table.left("out_rows") if edge == 1 else table.right("out_rows")
    moved = dot(order, moved.astype(jnp.bfloat16))
    return moved[:, :LANES] + moved[:, LANES : 2 * LANES] + moved[:, 2 * LANES :]


def put_strips(fields_ref, nbr_ref, face, send_ref, table):
    near = iota((16, LANES), 1) < 64
    strips = [strip_of(edge, fields_ref, table) for edge in range(EDGES)]
    for edge, rows in enumerate(strips):
        u, v, t, mass, flux_xx, flux_xy, flux_yy = [rows[16 * k : 16 * k + 16] for k in range(7)]
        u, v = turned(u, v, -edge)
        if edge % 2:
            flux_xx, flux_xy, flux_yy = flux_yy, -flux_xy, flux_xx
        slot = [
            jnp.where(near, low, roll(high, 64, 1))
            for low, high in ((u, v), (t, mass), (flux_xx, flux_xy))
        ]
        slot.append(jnp.where(near[:8], flux_yy[:8], roll(flux_yy[8:], 64, 1)))
        start = pl.multiple_of(SLOT * nbr_ref[edge, face], 8)
        send_ref[pl.ds(start, SLOT), :] = stacked(slot)


def ring_of(which_ref, got_ref, table):
    lane = iota((16, LANES), 1)
    block = iota((16, LANES), 0)
    near = lane < 64
    first = (block == 0) & (lane % 8 == 0) & (lane >= 8)
    last = (block == 15) & (lane % 8 == 7) & (lane >= 8)
    got, strips, seams = [], [], []
    for edge in range(EDGES):
        slot = got_ref[:SLOT, :]
        which = jnp.broadcast_to(which_ref[edge : edge + 1, :], (SLOT, LANES))
        for other in range(1, FACES):
            slot = jnp.where(which == other, got_ref[SLOT * other : SLOT * other + SLOT, :], slot)
        fields = []
        for n in range(3):
            rows = slot[16 * n : 16 * n + 16]
            fields += [jnp.where(near, rows, 0.0), jnp.where(near, roll(rows, 64, 1), 0.0)]
        rows = slot[48:56]
        fields.append(stacked([rows, roll(rows, 64, 1)]))
        fields[6] = jnp.where(near, fields[6], 0.0)
        got.append(fields)
    for edge in range(EDGES):
        fields = list(got[edge])
        corner = jnp.zeros((16, LANES), jnp.float32)
        for ch in range(4):
            after, before = got[(edge + 1) % EDGES][ch], got[(edge - 1) % EDGES][ch]
            at_first = (block == 0) & (lane == 8 * ch)
            at_last = (block == 15) & (lane == 8 * ch + 7)
            corner = jnp.where(at_first, roll(after[15:16], 8 * ch - 7, 1), corner)
            corner = jnp.where(at_last, roll(before[0:1], 8 * ch + 7, 1), corner)
            fields[ch] = (
                fields[ch]
                + jnp.where(first, roll(after[15:16], -7, 1), 0.0)
                + jnp.where(last, roll(before[0:1], 7, 1), 0.0)
            )
        rows = stacked([*fields, corner])
        count = 16
        if edge == 0:
            rows = reversed_blocks(rows, table)
        elif edge % 2:
            name = "east" if edge == 1 else "west"
            order = table.left("in_rows") if edge == 1 else table.right("in_rows")
            moved = dot(order, stacked(split(rows), 1))
            moved = stacked([moved[:64], moved[64:]], 1)
            into = [table.left(name + "_in")] * 3 + [table.right(name + "_in")] * 3
            rows = dot(moved.astype(jnp.bfloat16), stacked(into))
            count = 8
        fields = [rows[count * k : count * k + count] for k in range(7)]
        corner = rows[7 * count : 8 * count]
        low, high = ((120, 127), (0, 120), (0, 7), (7, 127))[edge]
        position, at = iota((count, LANES), 0), iota((count, LANES), 1)
        here = ((position == 0) & (at == low)) | ((position == count - 1) & (at == high))
        step = (8, -1, -8, 1)[edge]
        seam = [jnp.where(here, roll(corner, step * ch, 1), 0.0) for ch in range(4)]
        seams.append([*turned(seam[0], seam[1], edge + 2), *seam[2:]])
        fields[0], fields[1] = turned(fields[0], fields[1], edge + 2)
        if edge % 2:
            fields[4], fields[5], fields[6] = fields[6], -fields[5], fields[4]
        else:
            far = near if edge == 0 else ~near
            fields[3] = jnp.where(far, 1.0, fields[3])
        strips.append(fields)
    order = (0, 2, 1, 3)
    ring = [stacked([strips[edge][k] for edge in order]) for k in range(7)]
    return ring, [stacked([seams[edge][ch] for edge in order]) for ch in range(4)]


def first_kernel(
    nbr_from, own_ref, other_ref, table_ref, later_ref,
    fields_ref, send_ref, which_ref, kept_ref, nbr_ref, nbr_sem, sem,
):
    fetch = pltpu.make_async_copy(nbr_from, nbr_ref, nbr_sem)
    fetch.start()
    keep = pltpu.make_async_copy(later_ref, kept_ref, sem)
    keep.start()
    table = Table(table_ref, 0)
    core = lax.axis_index("fy") % 2
    face = lax.axis_index("face")
    fields = []
    for k in range(8):
        own = own_ref[pl.ds(k, 64, 8), :]
        other = other_ref[pl.ds(k, 64, 8), :]
        even = jnp.where(core == 0, own, other)
        odd = jnp.where(core == 0, other, own)
        pieces = []
        for x in range(4):
            pieces += [even[16 * x : 16 * x + 16], odd[16 * x : 16 * x + 16]]
        fields.append(stacked(pieces))
    u, v, t, volume, m_xx, m_yy, m_xy, planet = fields
    contra_u = m_xx * u + m_xy * v
    contra_v = m_xy * u + m_yy * v
    energy = 0.5 * (u * contra_u + v * contra_v) + t
    grad_x, grad_y = gradient(stacked([u, v, t, energy]), table)
    dy_u, dx_v = grad_y[:ROWS], grad_x[ROWS : 2 * ROWS]
    dx_t, dy_t = grad_x[2 * ROWS : 3 * ROWS], grad_y[2 * ROWS : 3 * ROWS]
    dx_e, dy_e = grad_x[3 * ROWS :], grad_y[3 * ROWS :]
    absolute = dx_v - dy_u + planet * volume
    mass = mass_weight() * volume
    raw_u = u + time_step * (absolute * contra_v - dx_e)
    raw_v = v + time_step * (-absolute * contra_u - dy_e)
    raw_t = t - time_step * (contra_u * dx_t + contra_v * dy_t)
    values = stacked([mass * raw_u, mass * raw_v, mass * raw_t, mass])
    sums = dot_halves(stacked(split(values), 1), stacked([table.whole("both")] * 3))
    for ch in range(4):
        part = slice(ROWS * ch, ROWS * ch + ROWS)
        fields_ref[part, :] = assembled(sums[part, :LANES], sums[part, LANES:])
    for k, field in enumerate([m_xx, m_xy, m_yy]):
        fields_ref[ROWS * (4 + k) : ROWS * (5 + k), :] = volume * field
    fetch.wait()
    for edge in range(8):
        which_ref[edge : edge + 1, :] = jnp.full((1, LANES), nbr_ref[edge % EDGES, face], jnp.int32)
    put_strips(fields_ref, nbr_ref, face, send_ref, table)
    keep.wait()


def laplace(fields, metric, table, parts):
    flux_xx, flux_xy, flux_yy = metric
    count = flux_xx.shape[0]
    grad_x, grad_y = gradient(stacked(fields), table, parts)
    flux = []
    for ch in range(3):
        part = slice(count * ch, count * ch + count)
        flux.append(
            stacked(
                [
                    flux_xx * grad_x[part] + flux_xy * grad_y[part],
                    flux_xy * grad_x[part] + flux_yy * grad_y[part],
                ],
                1,
            )
        )
    high, mid, low = split(stacked(flux))
    terms = [(high, 0), (mid, 0), (high, 1), (low, 0), (mid, 1), (high, 2)][: 3 * parts - 3]
    right = [table.part("spread", n, 2 * LANES) for _, n in terms]
    sums = dot_halves(stacked([part for part, _ in terms], 1), stacked(right))
    return [
        assembled(sums[count * ch : count * ch + count, :LANES], sums[count * ch : count * ch + count, LANES:])
        for ch in range(3)
    ]


def second_kernel(which_ref, got_ref, fields_ref, table_ref, out_ref, total_ref):
    table = Table(table_ref, 1)
    core = lax.axis_index("fy") % 2
    ring_fields, seams = ring_of(which_ref, got_ref, table)
    metric = [
        stacked([fields_ref[ROWS * k : ROWS * k + ROWS, :], ring_fields[k]]) for k in range(4, 7)
    ]
    total_ref[...] = fields_ref[: 4 * ROWS, :]
    ring = join(total_ref, ring_fields[:4], 4, seams)
    share = 1.0 / stacked([total_ref[3 * ROWS : 4 * ROWS, :], ring[3]])
    fields = [
        stacked([total_ref[ROWS * ch : ROWS * ch + ROWS, :], ring[ch]]) * share for ch in range(3)
    ]
    sectioned = [field[:ROWS] for field in fields]
    for step in range(2):
        sums = laplace(fields, metric, table, 3 - step)
        for ch in range(3):
            total_ref[ROWS * ch : ROWS * ch + ROWS, :] = sums[ch][:ROWS]
        ring = [field[ROWS:] for field in sums]
        ends = [placed_ends(part) for part in ends_meet(ring, 3, table)] if step == 0 else None
        ring = join(total_ref, ring, 3, ends)
        if step == 0:
            fields = [
                stacked([total_ref[ROWS * ch : ROWS * ch + ROWS, :], ring[ch]]) * share
                for ch in range(3)
            ]
    for ch in range(3):
        second_lap = total_ref[ROWS * ch : ROWS * ch + ROWS, :] * share[:ROWS]
        updated = sectioned[ch] - hyper_coeff * second_lap
        for x in range(4):
            even, odd = updated[32 * x : 32 * x + 16], updated[32 * x + 16 : 32 * x + 32]
            out_ref[16 * x : 16 * x + 16, 0, LANES * ch : LANES * ch + LANES] = jnp.where(
                core == 0, even, odd
            )


def unpack_kernel(got_ref, out_ref):
    levels = got_ref[...]
    columns = stacked([levels[:, 0, LANES * ch : LANES * ch + LANES] for ch in range(3)])
    out_ref[...] = jnp.transpose(columns)


def f32(*shape):
    return jax.ShapeDtypeStruct(shape, jnp.float32)


def near(*shape):
    return pltpu.VMEM(shape, jnp.float32)


def kept(table):
    return pltpu.VMEM(table.shape, jnp.bfloat16)


def held(values):
    return pltpu.with_memory_space_constraint(values, pltpu.VMEM)


VMEM = pl.BlockSpec(memory_space=pltpu.VMEM)
ANY = pl.BlockSpec(memory_space=pl.ANY)


def call(kernel, outs, ins, scratch=(), name=None):
    return pl.pallas_call(
        kernel,
        out_shape=outs,
        in_specs=ins,
        out_specs=jax.tree.map(lambda _: VMEM, outs),
        scratch_shapes=scratch,
        name=name,
    )


def level_groups():
    return [
        [(8 * face + 2 * x + core) * 16 + fx for x in range(4) for fx in range(16)]
        for face in range(FACES)
        for core in range(2)
    ]


def per_device(state, jacobian, metric_diag, metric_cross, coriolis, nbr_face, nbr_edge):
    axes = ("face", "fy", "fx")
    groups = level_groups()
    tables = [jnp.asarray(table) for table in TABLES]
    packed = call(pack_kernel, near(512, LANES), [VMEM] * 5, name="pack")(
        state.reshape(128, 192),
        jacobian[0].T,
        metric_diag[:, 0].transpose(0, 2, 1),
        metric_cross[0].T,
        coriolis[0].T,
    )
    own = lax.all_to_all(
        packed.reshape(64, 8, LANES), axes, 0, 0, axis_index_groups=groups, tiled=True
    )
    other = lax.ppermute(own, "fy", [(i, i ^ 1) for i in range(8)])
    table = call(
        keep_kernel,
        kept(TABLES[0]),
        [VMEM, ANY],
        [pltpu.SemaphoreType.DMA],
        name="keep",
    )(held(own.reshape(512, LANES)), tables[0])
    fields, send, which, table = call(
        first_kernel,
        [
            near(7 * ROWS, LANES),
            near(SLOT * FACES, LANES),
            pltpu.VMEM((8, LANES), jnp.int32),
            kept(TABLES[1]),
        ],
        [ANY] + [VMEM] * 3 + [ANY],
        [
            pltpu.SMEM((EDGES, FACES), jnp.int32),
            pltpu.SemaphoreType.DMA,
            pltpu.SemaphoreType.DMA,
        ],
        name="first",
    )(
        nbr_face.T,
        held(own.reshape(512, LANES)),
        held(other.reshape(512, LANES)),
        held(table),
        tables[1],
    )
    got = lax.all_to_all(send.reshape(FACES, SLOT, LANES), "face", 0, 0, tiled=True)
    updated = call(
        second_kernel,
        near(64, 1, 3 * LANES),
        [VMEM] * 4,
        [pltpu.VMEM((4 * ROWS, LANES), jnp.float32)],
        name="second",
    )(held(which), held(got.reshape(SLOT * FACES, LANES)), held(fields), held(table))
    back = lax.all_to_all(
        updated, axes, 0, 0, axis_index_groups=groups, tiled=True
    )
    nodes = call(unpack_kernel, f32(128, 192), [VMEM], name="unpack")(
        held(back)
    )
    return nodes.reshape(1, 16, 8, 192)


def solution(mesh):
    return jax.shard_map(
        per_device,
        mesh=mesh,
        in_specs=(
            P("face", "fy", "fx", None),
            P("face", "fy", "fx"),
            P(None, "face", "fy", "fx"),
            P("face", "fy", "fx"),
            P("face", "fy", "fx"),
            P(),
            P(),
        ),
        out_specs=P("face", "fy", "fx", None),
        check_vma=False,
    )
```

```python
import jax
import jax.numpy as jnp
import ml_dtypes
import numpy as np
from jax import lax
from jax.experimental import pallas as pl
from jax.experimental.pallas import tpu as pltpu
from jax.sharding import PartitionSpec as P

time_step = 0.05
hyper_coeff = 0.0005

FACES = 6
ROWS = 128
LANES = 128
EDGES = 4
RING_ROWS = 48
ALL_ROWS = ROWS + RING_ROWS
SLOT = 56
ENDS = ("S0", "S15", "N0", "N15", "E0", "E7", "W0", "W7")
END_ROWS = (0, 15, 16, 31, 32, 39, 40, 47)
MEETS = (6, 4, 7, 5, 1, 3, 0, 2)
TURNS = (1, -1, -1, 1, 1, -1, -1, 1)


def deriv_table():
    gll_nodes = np.array([-1.0, -1.0 / np.sqrt(5.0), 1.0 / np.sqrt(5.0), 1.0])
    bary_weights = np.ones(4)
    for j in range(4):
        for m in range(4):
            if m != j:
                bary_weights[j] = bary_weights[j] / (gll_nodes[j] - gll_nodes[m])
    matrix = np.zeros((4, 4))
    for i in range(4):
        for j in range(4):
            if i != j:
                matrix[i, j] = bary_weights[j] / bary_weights[i] / (gll_nodes[i] - gll_nodes[j])
        matrix[i, i] = -np.sum(matrix[i])
    return matrix


def in_parts(matrix):
    rest = np.asarray(matrix, np.float64)
    parts = []
    for _ in range(3):
        part = rest.astype(ml_dtypes.bfloat16)
        parts.append(part)
        rest = rest - part.astype(np.float64)
    return parts


def face_node(edge, depth, k):
    row, col = ((depth, k), (k, 127 - depth), (127 - depth, 127 - k), (127 - k, depth))[edge]
    return row // 16, col // 8, 8 * (row % 16) + col % 8


def ring_node(edge, depth, k):
    if edge == 1:
        return k // 16, 8 * (k % 16) + depth
    row = 127 - k
    return row // 16, 8 * (row % 16) + 7 - depth


def end_lane(end, depth):
    return {
        "S0": 8 * (15 - depth),
        "S15": 8 * (15 - depth) + 7,
        "N0": 8 * depth,
        "N15": 8 * depth + 7,
        "E0": depth,
        "E7": 120 + depth,
        "W0": 7 - depth,
        "W7": 127 - depth,
    }[end]


def tables():
    deriv = deriv_table()
    along_x = np.kron(np.eye(32), deriv.T)
    along_y = np.kron(np.kron(np.eye(4), deriv.T), np.eye(8))
    lane = np.arange(LANES)
    r, c = lane // 8, lane % 8
    weights = np.array([1.0, 5.0, 5.0, 1.0]) / 6.0
    within = np.eye(LANES)
    across = np.zeros((LANES, LANES))
    for l in range(LANES):
        if c[l] in (3, 4):
            within[l, l + 1 if c[l] == 3 else l - 1] = 1.0
        if c[l] == 7:
            across[l, l - 7] = 1.0
        if c[l] == 0:
            across[l, l + 7] = 1.0
    both = np.concatenate([within, across], 1)
    gradient = in_parts(np.concatenate([along_x, along_y], 1))
    weighted = np.diag(weights[r % 4] * weights[c % 4])
    spread = in_parts(np.concatenate([along_x @ weighted @ both, along_y @ weighted @ both], 0))

    out, out_rows, into, into_rows = [], [], [], []
    for edge in (1, 3):
        out.append(np.zeros((2, LANES, LANES)))
        out_rows.append(np.zeros((LANES, LANES)))
        into.append(np.zeros((2, LANES, LANES)))
        into_rows.append(np.zeros((LANES, LANES)))
        for k in range(128):
            j, i = k // 8, k % 8
            j2, i2 = (127 - k) // 8, (127 - k) % 8
            for depth in range(8):
                fy, _, at = face_node(edge, depth, k)
                out[-1][j % 2, at, 8 * depth + i] = 1.0
                ring_fy, ring_at = ring_node(edge, depth, k)
                into[-1][j2 % 2, 8 * depth + i2, ring_at] = 1.0
                for field in range(8):
                    out_rows[-1][16 * field + j, 64 * (j % 2) + 8 * field + fy] = 1.0
                    into_rows[-1][64 * (j2 % 2) + 8 * field + ring_fy, 16 * field + j2] = 1.0
    take = np.zeros((LANES, LANES))
    give = np.zeros((LANES, LANES))
    masks = np.zeros((32, 2 * LANES))
    for t, end in enumerate(ENDS):
        for depth in range(8):
            take[end_lane(end, depth), 8 * t + depth] = 1.0
            give[8 * t + depth, end_lane(ENDS[MEETS[t]], depth)] = 1.0
            masks[t, end_lane(end, depth)] = 1.0
            masks[8 + t, 8 * t + depth] = 1.0
            masks[16 + t, 8 * MEETS[t] + depth] = 1.0
        masks[24 + t] = TURNS[t]

    def pair(left, right):
        return np.concatenate([left, right], 1)

    reverse = pair(np.eye(LANES)[::-1], np.kron(np.eye(8), np.eye(16)[::-1]))
    groups = (
        {
            "gradient": np.concatenate(gradient, 0),
            "both": both,
            "east_out": pair(*out[0]),
            "west_out": pair(*out[1]),
            "out_rows": pair(*out_rows),
            "reverse": reverse,
        },
        {
            "gradient": np.concatenate(gradient, 0),
            "spread": np.concatenate(spread, 0),
            "east_in": pair(*into[0]),
            "west_in": pair(*into[1]),
            "in_rows": pair(*into_rows),
            "reverse": reverse,
            "ends": pair(take, give),
            "masks": masks,
        },
    )
    arrays, places = [], []
    for group in groups:
        start = 0
        places.append({})
        for name, matrix in group.items():
            places[-1][name] = (start, start + matrix.shape[0])
            start += matrix.shape[0]
        arrays.append(np.concatenate([m.astype(ml_dtypes.bfloat16) for m in group.values()], 0))
    return arrays, places


TABLES, PLACES = tables()


class Table:
    def __init__(self, ref, which):
        self.ref, self.places = ref, PLACES[which]

    def whole(self, name):
        start, end = self.places[name]
        return self.ref[start:end, :]

    def left(self, name):
        start, end = self.places[name]
        return self.ref[start:end, :LANES]

    def right(self, name):
        start, end = self.places[name]
        return self.ref[start:end, LANES:]

    def part(self, name, n, rows):
        start = self.places[name][0] + n * rows
        return self.ref[start : start + rows, :]


def roll(values, shift, axis):
    return pltpu.roll(values, shift % values.shape[axis], axis)


def iota(shape, dim):
    return lax.broadcasted_iota(jnp.int32, shape, dim)


def dot(a, b):
    return jnp.dot(a, b, preferred_element_type=jnp.float32)


def dot_halves(a, b):
    half = a.shape[0] // 32 * 16
    return jnp.concatenate([dot(a[:half], b), dot(a[half:], b)], axis=0)


def stacked(parts, axis=0):
    return jnp.concatenate(parts, axis=axis)


def split(values):
    high = values.astype(jnp.bfloat16)
    rest = values - high.astype(jnp.float32)
    mid = rest.astype(jnp.bfloat16)
    return high, mid, (rest - mid.astype(jnp.float32)).astype(jnp.bfloat16)


def gradient(values, table, parts=3):
    high, mid, low = split(values)
    left = [high, mid, high, mid, low, high][: 2 * parts]
    right = [table.part("gradient", n, LANES) for n in (0, 0, 1, 1, 0, 2)[: 2 * parts]]
    both = dot_halves(stacked(left, 1), stacked(right))
    return both[:, :LANES], both[:, LANES:]


def mass_weight():
    lane = iota((1, LANES), 1)
    r, c = lane // 8 % 4, lane % 4
    along_y = jnp.where((r == 0) | (r == 3), 1.0 / 6.0, 5.0 / 6.0)
    return along_y * jnp.where((c == 0) | (c == 3), 1.0 / 6.0, 5.0 / 6.0)


def assembled(inner, outer):
    shape = inner.shape
    row = iota(shape, 0)
    lane = iota(shape, 1)
    c = lane % 8
    r = lane // 8
    here = row < ROWS + 32
    from_before = here & (c == 0) & (row % 16 > 0)
    from_after = here & (c == 7) & (row % 16 < 15)
    summed = (
        inner
        + jnp.where(from_before, roll(outer, 1, 0), 0.0)
        + jnp.where(from_after, roll(outer, -1, 0), 0.0)
    )
    above = roll(summed, 8, 1)
    below = roll(summed, -8, 1)
    total = (
        summed
        + jnp.where((r % 4 == 0) & (r > 0), above, 0.0)
        + jnp.where((r % 4 == 3) & (r < 15), below, 0.0)
    )
    edge_rows = jnp.zeros((16, LANES), jnp.float32)
    above_block = [edge_rows, above[: ROWS - 16]]
    below_block = [below[16:ROWS], edge_rows]
    if shape[0] > ROWS:
        sides = slice(ROWS + 32, ROWS + 48)
        fy = iota((16, LANES), 0) % 8
        above_block += [edge_rows] * 2 + [jnp.where(fy > 0, roll(above[sides], 1, 0), 0.0)]
        below_block += [edge_rows] * 2 + [jnp.where(fy < 7, roll(below[sides], -1, 0), 0.0)]
    return (
        total
        + jnp.where(r == 0, stacked(above_block), 0.0)
        + jnp.where(r == 15, stacked(below_block), 0.0)
    )


def rim_rows(edge, base=0):
    if edge == 0:
        return pl.ds(base, 16)
    if edge == 1:
        return pl.ds(base + 15, 8, 16)
    if edge == 2:
        return pl.ds(base + 112, 16)
    return pl.ds(base, 8, 16)


def turned(u, v, quarter):
    quarter = quarter % 4
    if quarter == 0:
        return u, v
    if quarter == 1:
        return -v, u
    if quarter == 2:
        return -u, -v
    return v, -u


def ends_meet(ring, channels, table):
    ends = stacked(
        [ring[ch][row : row + 1] for ch in range(channels) for row in END_ROWS]
    )
    masks = table.left("masks").astype(jnp.float32)
    own = stacked([masks[0:8]] * channels)
    taken = dot(stacked(split(ends * own), 1), stacked([table.left("ends")] * 3))
    lines = []
    for ch in range(channels):
        line = jnp.sum(taken[8 * ch : 8 * ch + 8] * masks[8:16], axis=0, keepdims=True)
        lines.append(line * masks[16:24])
    given = dot(stacked(split(stacked(lines)), 1), stacked([table.right("ends")] * 3))
    given = [given[8 * ch : 8 * ch + 8] for ch in range(channels)]
    sense = masks[24:32]
    return [-sense * given[1], sense * given[0], *given[2:]]


def placed_ends(ends):
    block, fy = iota((16, LANES), 0), iota((8, LANES), 0)
    parts = []
    for side, position, count in ((0, block, 16), (1, block, 16), (2, fy, 8), (3, fy, 8)):
        first, last = ends[2 * side : 2 * side + 1], ends[2 * side + 1 : 2 * side + 2]
        parts.append(
            jnp.where(position == 0, first, jnp.where(position == count - 1, last, 0.0))
        )
    return stacked(parts)


def join(face_ref, ring, channels, ends=None):
    totals = []
    lane = iota((16, LANES), 1)
    lane_8 = iota((8, LANES), 1)
    for ch in range(channels):
        south, north = ring[ch][0:16], ring[ch][16:32]
        east, west = ring[ch][32:40], ring[ch][40:48]
        rows = [rim_rows(edge, ROWS * ch) for edge in range(EDGES)]
        if ends is not None:
            rims = [
                jnp.where(lane // 8 == 15, roll(face_ref[rows[0], :], -8, 1), 0.0),
                jnp.where(lane // 8 == 0, roll(face_ref[rows[2], :], 8, 1), 0.0),
                jnp.where(lane_8 % 8 == 0, roll(face_ref[rows[1], :], -7, 1), 0.0),
                jnp.where(lane_8 % 8 == 7, roll(face_ref[rows[3], :], 7, 1), 0.0),
            ]
            totals.append(ring[ch] + ends[ch] + stacked(rims))
        from_south = jnp.where(lane // 8 == 0, roll(south, 8, 1), 0.0)
        from_north = jnp.where(lane // 8 == 15, roll(north, -8, 1), 0.0)
        from_east = jnp.where(lane_8 % 8 == 7, roll(east, 7, 1), 0.0)
        from_west = jnp.where(lane_8 % 8 == 0, roll(west, -7, 1), 0.0)
        for edge, part in enumerate((from_south, from_east, from_north, from_west)):
            face_ref[rows[edge], :] = face_ref[rows[edge], :] + part
    return totals


def pack_kernel(state_ref, jac_ref, diag_ref, cross_ref, cor_ref, out_ref):
    turned_state = jnp.transpose(state_ref[...])
    for part in range(3):
        out_ref[pl.ds(part, 64, 8), :] = turned_state[64 * part : 64 * part + 64]
    spread = jnp.where(iota((16, LANES), 1) // 8 == iota((16, LANES), 0), 1.0, 0.0)
    mask = jnp.where(iota((8, LANES), 1) % 8 == iota((8, LANES), 0), 1.0, 0.0)
    fields = [jac_ref[...], diag_ref[0], diag_ref[1], cross_ref[...], cor_ref[...]]
    lines = jnp.dot(
        stacked(fields),
        spread,
        precision=lax.Precision.HIGHEST,
        preferred_element_type=jnp.float32,
    )
    for k in range(5):
        line = jnp.sum(lines[8 * k : 8 * k + 8] * mask, axis=0, keepdims=True)
        out_ref[pl.ds(3 + k, 64, 8), :] = jnp.broadcast_to(line, (64, LANES))


def weighted_raw(blocks_ref, table):
    u, v, t, volume, m_xx, m_yy, m_xy, planet = [
        blocks_ref[pl.ds(k, 64, 8), :] for k in range(8)
    ]
    contra_u = m_xx * u + m_xy * v
    contra_v = m_xy * u + m_yy * v
    energy = 0.5 * (u * contra_u + v * contra_v) + t
    grad_x, grad_y = gradient(stacked([u, v, t, energy]), table)
    dy_u, dx_v = grad_y[:64], grad_x[64:128]
    dx_t, dy_t = grad_x[128:192], grad_y[128:192]
    dx_e, dy_e = grad_x[192:], grad_y[192:]
    absolute = dx_v - dy_u + planet * volume
    mass = mass_weight() * volume
    raw_u = u + time_step * (absolute * contra_v - dx_e)
    raw_v = v + time_step * (-absolute * contra_u - dy_e)
    raw_t = t - time_step * (contra_u * dx_t + contra_v * dy_t)
    metric = [volume * m_xx, volume * m_xy, volume * m_yy]
    return [mass * raw_u, mass * raw_v, mass * raw_t, mass, *metric]


def early_kernel(own_ref, table_from, table_ref, half_ref, sem, late_sem):
    rows = PLACES[0]["gradient"][1]
    soon = pltpu.make_async_copy(table_from.at[:rows], table_ref.at[:rows], sem)
    late = pltpu.make_async_copy(table_from.at[rows:], table_ref.at[rows:], late_sem)
    soon.start()
    late.start()
    soon.wait()
    for k, field in enumerate(weighted_raw(own_ref, Table(table_ref, 0))):
        half_ref[64 * k : 64 * k + 64, :] = field
    late.wait()


def reversed_blocks(rows, table):
    parts = stacked([part.astype(jnp.float32) for part in split(rows)]).astype(jnp.bfloat16)
    moved = dot(parts, table.left("reverse"))
    count = rows.shape[0]
    moved = stacked([moved[n * count : n * count + count] for n in range(3)], 1)
    moved = dot(table.right("reverse"), moved.astype(jnp.bfloat16))
    return moved[:, :LANES] + moved[:, LANES : 2 * LANES] + moved[:, 2 * LANES :]


def strip_of(edge, fields_ref, table):
    rows = [fields_ref[rim_rows(edge, ROWS * k), :] for k in range(7)]
    rows = stacked([*rows, jnp.zeros_like(rows[0])])
    if edge == 0:
        return rows
    if edge == 2:
        return reversed_blocks(rows, table)
    name = "east" if edge == 1 else "west"
    moved = dot(stacked(split(rows)), table.whole(name + "_out"))
    halves = stacked([moved[:, :LANES], moved[:, LANES:]], 0)
    moved = stacked(
        [stacked([halves[64 * n : 64 * n + 64], halves[192 + 64 * n : 256 + 64 * n]]) for n in range(3)],
        1,
    )
    order = table.left("out_rows") if edge == 1 else table.right("out_rows")
    moved = dot(order, moved.astype(jnp.bfloat16))
    return moved[:, :LANES] + moved[:, LANES : 2 * LANES] + moved[:, 2 * LANES :]


def put_strips(fields_ref, nbr_ref, face, send_ref, table):
    near = iota((16, LANES), 1) < 64
    strips = [strip_of(edge, fields_ref, table) for edge in range(EDGES)]
    for edge, rows in enumerate(strips):
        u, v, t, mass, flux_xx, flux_xy, flux_yy = [rows[16 * k : 16 * k + 16] for k in range(7)]
        u, v = turned(u, v, -edge)
        if edge % 2:
            flux_xx, flux_xy, flux_yy = flux_yy, -flux_xy, flux_xx
        slot = [
            jnp.where(near, low, roll(high, 64, 1))
            for low, high in ((u, v), (t, mass), (flux_xx, flux_xy))
        ]
        slot.append(jnp.where(near[:8], flux_yy[:8], roll(flux_yy[8:], 64, 1)))
        start = pl.multiple_of(SLOT * nbr_ref[edge, face], 8)
        send_ref[pl.ds(start, SLOT), :] = stacked(slot)


def ring_of(which_ref, got_ref, table):
    lane = iota((16, LANES), 1)
    block = iota((16, LANES), 0)
    near = lane < 64
    first = (block == 0) & (lane % 8 == 0) & (lane >= 8)
    last = (block == 15) & (lane % 8 == 7) & (lane >= 8)
    got, strips, seams = [], [], []
    for edge in range(EDGES):
        slot = got_ref[:SLOT, :]
        which = jnp.broadcast_to(which_ref[edge : edge + 1, :], (SLOT, LANES))
        for other in range(1, FACES):
            slot = jnp.where(which == other, got_ref[SLOT * other : SLOT * other + SLOT, :], slot)
        fields = []
        for n in range(3):
            rows = slot[16 * n : 16 * n + 16]
            fields += [jnp.where(near, rows, 0.0), jnp.where(near, roll(rows, 64, 1), 0.0)]
        rows = slot[48:56]
        fields.append(stacked([rows, roll(rows, 64, 1)]))
        fields[6] = jnp.where(near, fields[6], 0.0)
        got.append(fields)
    for edge in range(EDGES):
        fields = list(got[edge])
        corner = jnp.zeros((16, LANES), jnp.float32)
        for ch in range(4):
            after, before = got[(edge + 1) % EDGES][ch], got[(edge - 1) % EDGES][ch]
            at_first = (block == 0) & (lane == 8 * ch)
            at_last = (block == 15) & (lane == 8 * ch + 7)
            corner = jnp.where(at_first, roll(after[15:16], 8 * ch - 7, 1), corner)
            corner = jnp.where(at_last, roll(before[0:1], 8 * ch + 7, 1), corner)
            fields[ch] = (
                fields[ch]
                + jnp.where(first, roll(after[15:16], -7, 1), 0.0)
                + jnp.where(last, roll(before[0:1], 7, 1), 0.0)
            )
        rows = stacked([*fields, corner])
        count = 16
        if edge == 0:
            rows = reversed_blocks(rows, table)
        elif edge % 2:
            name = "east" if edge == 1 else "west"
            order = table.left("in_rows") if edge == 1 else table.right("in_rows")
            moved = dot(order, stacked(split(rows), 1))
            moved = stacked([moved[:64], moved[64:]], 1)
            into = [table.left(name + "_in")] * 3 + [table.right(name + "_in")] * 3
            rows = dot(moved.astype(jnp.bfloat16), stacked(into))
            count = 8
        fields = [rows[count * k : count * k + count] for k in range(7)]
        corner = rows[7 * count : 8 * count]
        low, high = ((120, 127), (0, 120), (0, 7), (7, 127))[edge]
        position, at = iota((count, LANES), 0), iota((count, LANES), 1)
        here = ((position == 0) & (at == low)) | ((position == count - 1) & (at == high))
        step = (8, -1, -8, 1)[edge]
        seam = [jnp.where(here, roll(corner, step * ch, 1), 0.0) for ch in range(4)]
        seams.append([*turned(seam[0], seam[1], edge + 2), *seam[2:]])
        fields[0], fields[1] = turned(fields[0], fields[1], edge + 2)
        if edge % 2:
            fields[4], fields[5], fields[6] = fields[6], -fields[5], fields[4]
        else:
            far = near if edge == 0 else ~near
            fields[3] = jnp.where(far, 1.0, fields[3])
        strips.append(fields)
    order = (0, 2, 1, 3)
    ring = [stacked([strips[edge][k] for edge in order]) for k in range(7)]
    return ring, [stacked([seams[edge][ch] for edge in order]) for ch in range(4)]


def first_kernel(
    nbr_from, half_ref, other_ref, table_ref, later_ref,
    fields_ref, send_ref, which_ref, kept_ref, nbr_ref, nbr_sem, sem,
):
    fetch = pltpu.make_async_copy(nbr_from, nbr_ref, nbr_sem)
    fetch.start()
    keep = pltpu.make_async_copy(later_ref, kept_ref, sem)
    keep.start()
    table = Table(table_ref, 0)
    core = lax.axis_index("fy") % 2
    face = lax.axis_index("face")
    fields = []
    for k, other in enumerate(weighted_raw(other_ref, table)):
        own = half_ref[64 * k : 64 * k + 64, :]
        even = jnp.where(core == 0, own, other)
        odd = jnp.where(core == 0, other, own)
        pieces = []
        for x in range(4):
            pieces += [even[16 * x : 16 * x + 16], odd[16 * x : 16 * x + 16]]
        fields.append(stacked(pieces))
    values = stacked(fields[:4])
    sums = dot_halves(stacked(split(values), 1), stacked([table.whole("both")] * 3))
    for ch in range(4):
        part = slice(ROWS * ch, ROWS * ch + ROWS)
        fields_ref[part, :] = assembled(sums[part, :LANES], sums[part, LANES:])
    for k in range(4, 7):
        fields_ref[ROWS * k : ROWS * k + ROWS, :] = fields[k]
    fetch.wait()
    for edge in range(8):
        which_ref[edge : edge + 1, :] = jnp.full((1, LANES), nbr_ref[edge % EDGES, face], jnp.int32)
    put_strips(fields_ref, nbr_ref, face, send_ref, table)
    keep.wait()


def laplace(fields, metric, table, parts):
    flux_xx, flux_xy, flux_yy = metric
    count = flux_xx.shape[0]
    grad_x, grad_y = gradient(stacked(fields), table, parts)
    flux = []
    for ch in range(3):
        part = slice(count * ch, count * ch + count)
        flux.append(
            stacked(
                [
                    flux_xx * grad_x[part] + flux_xy * grad_y[part],
                    flux_xy * grad_x[part] + flux_yy * grad_y[part],
                ],
                1,
            )
        )
    high, mid, low = split(stacked(flux))
    terms = [(high, 0), (mid, 0), (high, 1), (low, 0), (mid, 1), (high, 2)][: 3 * parts - 3]
    right = [table.part("spread", n, 2 * LANES) for _, n in terms]
    sums = dot_halves(stacked([part for part, _ in terms], 1), stacked(right))
    return [
        assembled(sums[count * ch : count * ch + count, :LANES], sums[count * ch : count * ch + count, LANES:])
        for ch in range(3)
    ]


def second_kernel(which_ref, got_ref, fields_ref, table_ref, out_ref, total_ref):
    table = Table(table_ref, 1)
    core = lax.axis_index("fy") % 2
    ring_fields, seams = ring_of(which_ref, got_ref, table)
    metric = [
        stacked([fields_ref[ROWS * k : ROWS * k + ROWS, :], ring_fields[k]]) for k in range(4, 7)
    ]
    total_ref[...] = fields_ref[: 4 * ROWS, :]
    ring = join(total_ref, ring_fields[:4], 4, seams)
    share = 1.0 / stacked([total_ref[3 * ROWS : 4 * ROWS, :], ring[3]])
    fields = [
        stacked([total_ref[ROWS * ch : ROWS * ch + ROWS, :], ring[ch]]) * share for ch in range(3)
    ]
    sectioned = [field[:ROWS] for field in fields]
    for step in range(2):
        sums = laplace(fields, metric, table, 3 - step)
        for ch in range(3):
            total_ref[ROWS * ch : ROWS * ch + ROWS, :] = sums[ch][:ROWS]
        ring = [field[ROWS:] for field in sums]
        ends = [placed_ends(part) for part in ends_meet(ring, 3, table)] if step == 0 else None
        ring = join(total_ref, ring, 3, ends)
        if step == 0:
            fields = [
                stacked([total_ref[ROWS * ch : ROWS * ch + ROWS, :], ring[ch]]) * share
                for ch in range(3)
            ]
    for ch in range(3):
        second_lap = total_ref[ROWS * ch : ROWS * ch + ROWS, :] * share[:ROWS]
        updated = sectioned[ch] - hyper_coeff * second_lap
        for x in range(4):
            even, odd = updated[32 * x : 32 * x + 16], updated[32 * x + 16 : 32 * x + 32]
            out_ref[16 * x : 16 * x + 16, 0, LANES * ch : LANES * ch + LANES] = jnp.where(
                core == 0, even, odd
            )


def unpack_kernel(got_ref, out_ref):
    levels = got_ref[...]
    columns = stacked([levels[:, 0, LANES * ch : LANES * ch + LANES] for ch in range(3)])
    out_ref[...] = jnp.transpose(columns)


def f32(*shape):
    return jax.ShapeDtypeStruct(shape, jnp.float32)


def near(*shape):
    return pltpu.VMEM(shape, jnp.float32)


def kept(table):
    return pltpu.VMEM(table.shape, jnp.bfloat16)


def held(values):
    return pltpu.with_memory_space_constraint(values, pltpu.VMEM)


VMEM = pl.BlockSpec(memory_space=pltpu.VMEM)
ANY = pl.BlockSpec(memory_space=pl.ANY)


def call(kernel, outs, ins, scratch=(), name=None):
    return pl.pallas_call(
        kernel,
        out_shape=outs,
        in_specs=ins,
        out_specs=jax.tree.map(lambda _: VMEM, outs),
        scratch_shapes=scratch,
        name=name,
    )


def level_groups():
    return [
        [(8 * face + 2 * x + core) * 16 + fx for x in range(4) for fx in range(16)]
        for face in range(FACES)
        for core in range(2)
    ]


def per_device(state, jacobian, metric_diag, metric_cross, coriolis, nbr_face, nbr_edge):
    axes = ("face", "fy", "fx")
    groups = level_groups()
    tables = [jnp.asarray(table) for table in TABLES]
    packed = call(pack_kernel, near(512, LANES), [VMEM] * 5, name="pack")(
        state.reshape(128, 192),
        jacobian[0].T,
        metric_diag[:, 0].transpose(0, 2, 1),
        metric_cross[0].T,
        coriolis[0].T,
    )
    own = lax.all_to_all(
        packed.reshape(64, 8, LANES), axes, 0, 0, axis_index_groups=groups, tiled=True
    )
    other = lax.ppermute(own, "fy", [(i, i ^ 1) for i in range(8)])
    table, half = call(
        early_kernel,
        [kept(TABLES[0]), near(7 * 64, LANES)],
        [VMEM, ANY],
        [pltpu.SemaphoreType.DMA, pltpu.SemaphoreType.DMA],
        name="early",
    )(held(own.reshape(512, LANES)), tables[0])
    fields, send, which, table = call(
        first_kernel,
        [
            near(7 * ROWS, LANES),
            near(SLOT * FACES, LANES),
            pltpu.VMEM((8, LANES), jnp.int32),
            kept(TABLES[1]),
        ],
        [ANY] + [VMEM] * 3 + [ANY],
        [
            pltpu.SMEM((EDGES, FACES), jnp.int32),
            pltpu.SemaphoreType.DMA,
            pltpu.SemaphoreType.DMA,
        ],
        name="first",
    )(
        nbr_face.T,
        held(half),
        held(other.reshape(512, LANES)),
        held(table),
        tables[1],
    )
    got = lax.all_to_all(send.reshape(FACES, SLOT, LANES), "face", 0, 0, tiled=True)
    updated = call(
        second_kernel,
        near(64, 1, 3 * LANES),
        [VMEM] * 4,
        [pltpu.VMEM((4 * ROWS, LANES), jnp.float32)],
        name="second",
    )(held(which), held(got.reshape(SLOT * FACES, LANES)), held(fields), held(table))
    back = lax.all_to_all(
        updated, axes, 0, 0, axis_index_groups=groups, tiled=True
    )
    nodes = call(unpack_kernel, f32(128, 192), [VMEM], name="unpack")(
        held(back)
    )
    return nodes.reshape(1, 16, 8, 192)


def solution(mesh):
    return jax.shard_map(
        per_device,
        mesh=mesh,
        in_specs=(
            P("face", "fy", "fx", None),
            P("face", "fy", "fx"),
            P(None, "face", "fy", "fx"),
            P("face", "fy", "fx"),
            P("face", "fy", "fx"),
            P(),
            P(),
        ),
        out_specs=P("face", "fy", "fx", None),
        check_vma=False,
    )
```

```python
import jax
import jax.numpy as jnp
import ml_dtypes
import numpy as np
from jax import lax
from jax.experimental import pallas as pl
from jax.experimental.pallas import tpu as pltpu
from jax.sharding import PartitionSpec as P

time_step = 0.05
hyper_coeff = 0.0005

FACES = 6
ROWS = 128
LANES = 128
EDGES = 4
RING_ROWS = 32
ALL_ROWS = ROWS + RING_ROWS
SLOT = 56
ENDS = ("S0", "S15", "N0", "N15", "E0", "E7", "W0", "W7")
END_ROWS = (0, 15, 0, 15, 16, 23, 24, 31)
MEETS = (6, 4, 7, 5, 1, 3, 0, 2)
TURNS = (1, -1, -1, 1, 1, -1, -1, 1)


def deriv_table():
    gll_nodes = np.array([-1.0, -1.0 / np.sqrt(5.0), 1.0 / np.sqrt(5.0), 1.0])
    bary_weights = np.ones(4)
    for j in range(4):
        for m in range(4):
            if m != j:
                bary_weights[j] = bary_weights[j] / (gll_nodes[j] - gll_nodes[m])
    matrix = np.zeros((4, 4))
    for i in range(4):
        for j in range(4):
            if i != j:
                matrix[i, j] = bary_weights[j] / bary_weights[i] / (gll_nodes[i] - gll_nodes[j])
        matrix[i, i] = -np.sum(matrix[i])
    return matrix


def in_parts(matrix):
    rest = np.asarray(matrix, np.float64)
    parts = []
    for _ in range(3):
        part = rest.astype(ml_dtypes.bfloat16)
        parts.append(part)
        rest = rest - part.astype(np.float64)
    return parts


def face_node(edge, depth, k):
    row, col = ((depth, k), (k, 127 - depth), (127 - depth, 127 - k), (127 - k, depth))[edge]
    return row // 16, col // 8, 8 * (row % 16) + col % 8


def ring_node(edge, depth, k):
    if edge == 1:
        return k // 16, 8 * (k % 16) + depth
    row = 127 - k
    return row // 16, 8 * (row % 16) + 7 - depth


def end_lane(end, depth):
    return {
        "S0": 8 * (15 - depth),
        "S15": 8 * (15 - depth) + 7,
        "N0": 8 * depth,
        "N15": 8 * depth + 7,
        "E0": depth,
        "E7": 120 + depth,
        "W0": 7 - depth,
        "W7": 127 - depth,
    }[end]


def tables():
    deriv = deriv_table()
    along_x = np.kron(np.eye(32), deriv.T)
    along_y = np.kron(np.kron(np.eye(4), deriv.T), np.eye(8))
    lane = np.arange(LANES)
    r, c = lane // 8, lane % 8
    weights = np.array([1.0, 5.0, 5.0, 1.0]) / 6.0
    within = np.eye(LANES)
    across = np.zeros((LANES, LANES))
    for l in range(LANES):
        if c[l] in (3, 4):
            within[l, l + 1 if c[l] == 3 else l - 1] = 1.0
        if c[l] == 7:
            across[l, l - 7] = 1.0
        if c[l] == 0:
            across[l, l + 7] = 1.0
    both = np.concatenate([within, across], 1)
    gradient = in_parts(np.concatenate([along_x, along_y], 1))
    weighted = np.diag(weights[r % 4] * weights[c % 4])
    spread = in_parts(np.concatenate([along_x @ weighted @ both, along_y @ weighted @ both], 0))

    out, out_rows, into, into_rows = [], [], [], []
    for edge in (1, 3):
        out.append(np.zeros((2, LANES, LANES)))
        out_rows.append(np.zeros((LANES, LANES)))
        into.append(np.zeros((2, LANES, LANES)))
        into_rows.append(np.zeros((LANES, LANES)))
        for k in range(128):
            j, i = k // 8, k % 8
            j2, i2 = (127 - k) // 8, (127 - k) % 8
            for depth in range(8):
                fy, _, at = face_node(edge, depth, k)
                out[-1][j % 2, at, 8 * depth + i] = 1.0
                ring_fy, ring_at = ring_node(edge, depth, k)
                into[-1][j2 % 2, 8 * depth + i2, ring_at] = 1.0
                for field in range(8):
                    out_rows[-1][16 * field + j, 64 * (j % 2) + 8 * field + fy] = 1.0
                    into_rows[-1][64 * (j2 % 2) + 8 * field + ring_fy, 16 * field + j2] = 1.0
    take = np.zeros((LANES, LANES))
    give = np.zeros((LANES, LANES))
    masks = np.zeros((32, 2 * LANES))
    for t, end in enumerate(ENDS):
        for depth in range(8):
            take[end_lane(end, depth), 8 * t + depth] = 1.0
            give[8 * t + depth, end_lane(ENDS[MEETS[t]], depth)] = 1.0
            masks[t, end_lane(end, depth)] = 1.0
            masks[8 + t, 8 * t + depth] = 1.0
            masks[16 + t, 8 * MEETS[t] + depth] = 1.0
        masks[24 + t] = TURNS[t]

    def pair(left, right):
        return np.concatenate([left, right], 1)

    reverse = pair(np.eye(LANES)[::-1], np.kron(np.eye(8), np.eye(16)[::-1]))
    groups = (
        {
            "gradient": np.concatenate(gradient, 0),
            "both": both,
            "east_out": pair(*out[0]),
            "west_out": pair(*out[1]),
            "out_rows": pair(*out_rows),
            "reverse": reverse,
        },
        {
            "gradient": np.concatenate(gradient, 0),
            "spread": np.concatenate(spread, 0),
            "east_in": pair(*into[0]),
            "west_in": pair(*into[1]),
            "in_rows": pair(*into_rows),
            "reverse": reverse,
            "ends": pair(take, give),
            "masks": masks,
        },
    )
    arrays, places = [], []
    for group in groups:
        start = 0
        places.append({})
        for name, matrix in group.items():
            places[-1][name] = (start, start + matrix.shape[0])
            start += matrix.shape[0]
        arrays.append(np.concatenate([m.astype(ml_dtypes.bfloat16) for m in group.values()], 0))
    return arrays, places


TABLES, PLACES = tables()


class Table:
    def __init__(self, ref, which):
        self.ref, self.places = ref, PLACES[which]

    def whole(self, name):
        start, end = self.places[name]
        return self.ref[start:end, :]

    def left(self, name):
        start, end = self.places[name]
        return self.ref[start:end, :LANES]

    def right(self, name):
        start, end = self.places[name]
        return self.ref[start:end, LANES:]

    def part(self, name, n, rows):
        start = self.places[name][0] + n * rows
        return self.ref[start : start + rows, :]


def roll(values, shift, axis):
    return pltpu.roll(values, shift % values.shape[axis], axis)


def iota(shape, dim):
    return lax.broadcasted_iota(jnp.int32, shape, dim)


def dot(a, b):
    return jnp.dot(a, b, preferred_element_type=jnp.float32)


def dot_halves(a, b):
    half = a.shape[0] // 32 * 16
    return jnp.concatenate([dot(a[:half], b), dot(a[half:], b)], axis=0)


def stacked(parts, axis=0):
    return jnp.concatenate(parts, axis=axis)


def split(values):
    high = values.astype(jnp.bfloat16)
    rest = values - high.astype(jnp.float32)
    mid = rest.astype(jnp.bfloat16)
    return high, mid, (rest - mid.astype(jnp.float32)).astype(jnp.bfloat16)


def gradient(values, table, parts=3):
    high, mid, low = split(values)
    left = [high, mid, high, mid, low, high][: 2 * parts]
    right = [table.part("gradient", n, LANES) for n in (0, 0, 1, 1, 0, 2)[: 2 * parts]]
    both = dot_halves(stacked(left, 1), stacked(right))
    return both[:, :LANES], both[:, LANES:]


def mass_weight():
    lane = iota((1, LANES), 1)
    r, c = lane // 8 % 4, lane % 4
    along_y = jnp.where((r == 0) | (r == 3), 1.0 / 6.0, 5.0 / 6.0)
    return along_y * jnp.where((c == 0) | (c == 3), 1.0 / 6.0, 5.0 / 6.0)


def assembled(inner, outer):
    shape = inner.shape
    row = iota(shape, 0)
    lane = iota(shape, 1)
    c = lane % 8
    r = lane // 8
    here = row < ROWS + 16
    from_before = here & (c == 0) & (row % 16 > 0)
    from_after = here & (c == 7) & (row % 16 < 15)
    summed = (
        inner
        + jnp.where(from_before, roll(outer, 1, 0), 0.0)
        + jnp.where(from_after, roll(outer, -1, 0), 0.0)
    )
    above = roll(summed, 8, 1)
    below = roll(summed, -8, 1)
    total = (
        summed
        + jnp.where((r % 4 == 0) & (r > 0), above, 0.0)
        + jnp.where((r % 4 == 3) & (r < 15), below, 0.0)
    )
    edge_rows = jnp.zeros((16, LANES), jnp.float32)
    above_block = [edge_rows, above[: ROWS - 16]]
    below_block = [below[16:ROWS], edge_rows]
    if shape[0] > ROWS:
        sides = slice(ROWS + 16, ROWS + 32)
        fy = iota((16, LANES), 0) % 8
        above_block += [edge_rows, jnp.where(fy > 0, roll(above[sides], 1, 0), 0.0)]
        below_block += [edge_rows, jnp.where(fy < 7, roll(below[sides], -1, 0), 0.0)]
    return (
        total
        + jnp.where(r == 0, stacked(above_block), 0.0)
        + jnp.where(r == 15, stacked(below_block), 0.0)
    )


def rim_rows(edge, base=0):
    if edge == 0:
        return pl.ds(base, 16)
    if edge == 1:
        return pl.ds(base + 15, 8, 16)
    if edge == 2:
        return pl.ds(base + 112, 16)
    return pl.ds(base, 8, 16)


def turned(u, v, quarter):
    quarter = quarter % 4
    if quarter == 0:
        return u, v
    if quarter == 1:
        return -v, u
    if quarter == 2:
        return -u, -v
    return v, -u


def ends_meet(ring, channels, table):
    ends = stacked(
        [ring[ch][row : row + 1] for ch in range(channels) for row in END_ROWS]
    )
    masks = table.left("masks").astype(jnp.float32)
    own = stacked([masks[0:8]] * channels)
    taken = dot(stacked(split(ends * own), 1), stacked([table.left("ends")] * 3))
    lines = []
    for ch in range(channels):
        line = jnp.sum(taken[8 * ch : 8 * ch + 8] * masks[8:16], axis=0, keepdims=True)
        lines.append(line * masks[16:24])
    given = dot(stacked(split(stacked(lines)), 1), stacked([table.right("ends")] * 3))
    given = [given[8 * ch : 8 * ch + 8] for ch in range(channels)]
    sense = masks[24:32]
    return [-sense * given[1], sense * given[0], *given[2:]]


def placed_ends(ends):
    block, fy = iota((16, LANES), 0), iota((8, LANES), 0)
    parts = []
    for side, position, count in ((0, block, 16), (1, block, 16), (2, fy, 8), (3, fy, 8)):
        first, last = ends[2 * side : 2 * side + 1], ends[2 * side + 1 : 2 * side + 2]
        parts.append(
            jnp.where(position == 0, first, jnp.where(position == count - 1, last, 0.0))
        )
    return stacked([parts[0] + parts[1], parts[2], parts[3]])


def join(face_ref, ring, channels, ends=None):
    totals = []
    lane = iota((16, LANES), 1)
    lane_8 = iota((8, LANES), 1)
    for ch in range(channels):
        outer, east, west = ring[ch][0:16], ring[ch][16:24], ring[ch][24:32]
        rows = [rim_rows(edge, ROWS * ch) for edge in range(EDGES)]
        if ends is not None:
            rims = [
                jnp.where(
                    lane // 8 == 15,
                    roll(face_ref[rows[0], :], -8, 1),
                    jnp.where(lane // 8 == 0, roll(face_ref[rows[2], :], 8, 1), 0.0),
                ),
                jnp.where(lane_8 % 8 == 0, roll(face_ref[rows[1], :], -7, 1), 0.0),
                jnp.where(lane_8 % 8 == 7, roll(face_ref[rows[3], :], 7, 1), 0.0),
            ]
            totals.append(ring[ch] + ends[ch] + stacked(rims))
        from_south = jnp.where(lane // 8 == 0, roll(outer, 8, 1), 0.0)
        from_north = jnp.where(lane // 8 == 15, roll(outer, -8, 1), 0.0)
        from_east = jnp.where(lane_8 % 8 == 7, roll(east, 7, 1), 0.0)
        from_west = jnp.where(lane_8 % 8 == 0, roll(west, -7, 1), 0.0)
        for edge, part in enumerate((from_south, from_east, from_north, from_west)):
            face_ref[rows[edge], :] = face_ref[rows[edge], :] + part
    return totals


def pack_kernel(state_ref, jac_ref, diag_ref, cross_ref, cor_ref, out_ref):
    turned_state = jnp.transpose(state_ref[...])
    for part in range(3):
        out_ref[pl.ds(part, 64, 8), :] = turned_state[64 * part : 64 * part + 64]
    spread = jnp.where(iota((16, LANES), 1) // 8 == iota((16, LANES), 0), 1.0, 0.0)
    mask = jnp.where(iota((8, LANES), 1) % 8 == iota((8, LANES), 0), 1.0, 0.0)
    fields = [jac_ref[...], diag_ref[0], diag_ref[1], cross_ref[...], cor_ref[...]]
    lines = jnp.dot(
        stacked(fields),
        spread,
        precision=lax.Precision.HIGHEST,
        preferred_element_type=jnp.float32,
    )
    for k in range(5):
        line = jnp.sum(lines[8 * k : 8 * k + 8] * mask, axis=0, keepdims=True)
        out_ref[pl.ds(3 + k, 64, 8), :] = jnp.broadcast_to(line, (64, LANES))


def weighted_raw(blocks_ref, table):
    u, v, t, volume, m_xx, m_yy, m_xy, planet = [
        blocks_ref[pl.ds(k, 64, 8), :] for k in range(8)
    ]
    contra_u = m_xx * u + m_xy * v
    contra_v = m_xy * u + m_yy * v
    energy = 0.5 * (u * contra_u + v * contra_v) + t
    grad_x, grad_y = gradient(stacked([u, v, t, energy]), table)
    dy_u, dx_v = grad_y[:64], grad_x[64:128]
    dx_t, dy_t = grad_x[128:192], grad_y[128:192]
    dx_e, dy_e = grad_x[192:], grad_y[192:]
    absolute = dx_v - dy_u + planet * volume
    mass = mass_weight() * volume
    raw_u = u + time_step * (absolute * contra_v - dx_e)
    raw_v = v + time_step * (-absolute * contra_u - dy_e)
    raw_t = t - time_step * (contra_u * dx_t + contra_v * dy_t)
    metric = [volume * m_xx, volume * m_xy, volume * m_yy]
    return [mass * raw_u, mass * raw_v, mass * raw_t, mass, *metric]


def early_kernel(own_ref, table_from, table_ref, half_ref, sem, late_sem):
    rows = PLACES[0]["gradient"][1]
    soon = pltpu.make_async_copy(table_from.at[:rows], table_ref.at[:rows], sem)
    late = pltpu.make_async_copy(table_from.at[rows:], table_ref.at[rows:], late_sem)
    soon.start()
    late.start()
    soon.wait()
    for k, field in enumerate(weighted_raw(own_ref, Table(table_ref, 0))):
        half_ref[64 * k : 64 * k + 64, :] = field
    late.wait()


def reversed_blocks(rows, table):
    parts = stacked([part.astype(jnp.float32) for part in split(rows)]).astype(jnp.bfloat16)
    moved = dot(parts, table.left("reverse"))
    count = rows.shape[0]
    moved = stacked([moved[n * count : n * count + count] for n in range(3)], 1)
    moved = dot(table.right("reverse"), moved.astype(jnp.bfloat16))
    return moved[:, :LANES] + moved[:, LANES : 2 * LANES] + moved[:, 2 * LANES :]


def strip_of(edge, fields_ref, table):
    rows = [fields_ref[rim_rows(edge, ROWS * k), :] for k in range(7)]
    rows = stacked([*rows, jnp.zeros_like(rows[0])])
    if edge == 0:
        return rows
    if edge == 2:
        return reversed_blocks(rows, table)
    name = "east" if edge == 1 else "west"
    moved = dot(stacked(split(rows)), table.whole(name + "_out"))
    halves = stacked([moved[:, :LANES], moved[:, LANES:]], 0)
    moved = stacked(
        [stacked([halves[64 * n : 64 * n + 64], halves[192 + 64 * n : 256 + 64 * n]]) for n in range(3)],
        1,
    )
    order = table.left("out_rows") if edge == 1 else table.right("out_rows")
    moved = dot(order, moved.astype(jnp.bfloat16))
    return moved[:, :LANES] + moved[:, LANES : 2 * LANES] + moved[:, 2 * LANES :]


def put_strips(fields_ref, nbr_ref, face, send_ref, table):
    near = iota((16, LANES), 1) < 64
    strips = [strip_of(edge, fields_ref, table) for edge in range(EDGES)]
    for edge, rows in enumerate(strips):
        u, v, t, mass, flux_xx, flux_xy, flux_yy = [rows[16 * k : 16 * k + 16] for k in range(7)]
        u, v = turned(u, v, -edge)
        if edge % 2:
            flux_xx, flux_xy, flux_yy = flux_yy, -flux_xy, flux_xx
        slot = [
            jnp.where(near, low, roll(high, 64, 1))
            for low, high in ((u, v), (t, mass), (flux_xx, flux_xy))
        ]
        slot.append(jnp.where(near[:8], flux_yy[:8], roll(flux_yy[8:], 64, 1)))
        start = pl.multiple_of(SLOT * nbr_ref[edge, face], 8)
        send_ref[pl.ds(start, SLOT), :] = stacked(slot)


def ring_of(which_ref, got_ref, table):
    lane = iota((16, LANES), 1)
    block = iota((16, LANES), 0)
    near = lane < 64
    first = (block == 0) & (lane % 8 == 0) & (lane >= 8)
    last = (block == 15) & (lane % 8 == 7) & (lane >= 8)
    got, strips, seams = [], [], []
    for edge in range(EDGES):
        slot = got_ref[:SLOT, :]
        which = jnp.broadcast_to(which_ref[edge : edge + 1, :], (SLOT, LANES))
        for other in range(1, FACES):
            slot = jnp.where(which == other, got_ref[SLOT * other : SLOT * other + SLOT, :], slot)
        fields = []
        for n in range(3):
            rows = slot[16 * n : 16 * n + 16]
            fields += [jnp.where(near, rows, 0.0), jnp.where(near, roll(rows, 64, 1), 0.0)]
        rows = slot[48:56]
        fields.append(stacked([rows, roll(rows, 64, 1)]))
        fields[6] = jnp.where(near, fields[6], 0.0)
        got.append(fields)
    for edge in range(EDGES):
        fields = list(got[edge])
        corner = jnp.zeros((16, LANES), jnp.float32)
        for ch in range(4):
            after, before = got[(edge + 1) % EDGES][ch], got[(edge - 1) % EDGES][ch]
            at_first = (block == 0) & (lane == 8 * ch)
            at_last = (block == 15) & (lane == 8 * ch + 7)
            corner = jnp.where(at_first, roll(after[15:16], 8 * ch - 7, 1), corner)
            corner = jnp.where(at_last, roll(before[0:1], 8 * ch + 7, 1), corner)
            fields[ch] = (
                fields[ch]
                + jnp.where(first, roll(after[15:16], -7, 1), 0.0)
                + jnp.where(last, roll(before[0:1], 7, 1), 0.0)
            )
        rows = stacked([*fields, corner])
        count = 16
        if edge == 0:
            rows = reversed_blocks(rows, table)
        elif edge % 2:
            name = "east" if edge == 1 else "west"
            order = table.left("in_rows") if edge == 1 else table.right("in_rows")
            moved = dot(order, stacked(split(rows), 1))
            moved = stacked([moved[:64], moved[64:]], 1)
            into = [table.left(name + "_in")] * 3 + [table.right(name + "_in")] * 3
            rows = dot(moved.astype(jnp.bfloat16), stacked(into))
            count = 8
        fields = [rows[count * k : count * k + count] for k in range(7)]
        corner = rows[7 * count : 8 * count]
        low, high = ((120, 127), (0, 120), (0, 7), (7, 127))[edge]
        position, at = iota((count, LANES), 0), iota((count, LANES), 1)
        here = ((position == 0) & (at == low)) | ((position == count - 1) & (at == high))
        step = (8, -1, -8, 1)[edge]
        seam = [jnp.where(here, roll(corner, step * ch, 1), 0.0) for ch in range(4)]
        seams.append([*turned(seam[0], seam[1], edge + 2), *seam[2:]])
        fields[0], fields[1] = turned(fields[0], fields[1], edge + 2)
        if edge % 2:
            fields[4], fields[5], fields[6] = fields[6], -fields[5], fields[4]
        strips.append(fields)
    def around(sides, k):
        south, east, north, west = [side[k] for side in sides]
        return stacked([south + north, east, west])

    return [around(strips, k) for k in range(7)], [around(seams, ch) for ch in range(4)]


def first_kernel(
    nbr_from, half_ref, other_ref, table_ref, later_ref,
    fields_ref, send_ref, which_ref, kept_ref, nbr_ref, nbr_sem, sem,
):
    fetch = pltpu.make_async_copy(nbr_from, nbr_ref, nbr_sem)
    fetch.start()
    keep = pltpu.make_async_copy(later_ref, kept_ref, sem)
    keep.start()
    table = Table(table_ref, 0)
    core = lax.axis_index("fy") % 2
    face = lax.axis_index("face")
    fields = []
    for k, other in enumerate(weighted_raw(other_ref, table)):
        own = half_ref[64 * k : 64 * k + 64, :]
        even = jnp.where(core == 0, own, other)
        odd = jnp.where(core == 0, other, own)
        pieces = []
        for x in range(4):
            pieces += [even[16 * x : 16 * x + 16], odd[16 * x : 16 * x + 16]]
        fields.append(stacked(pieces))
    values = stacked(fields[:4])
    sums = dot_halves(stacked(split(values), 1), stacked([table.whole("both")] * 3))
    for ch in range(4):
        part = slice(ROWS * ch, ROWS * ch + ROWS)
        fields_ref[part, :] = assembled(sums[part, :LANES], sums[part, LANES:])
    for k in range(4, 7):
        fields_ref[ROWS * k : ROWS * k + ROWS, :] = fields[k]
    fetch.wait()
    for edge in range(8):
        which_ref[edge : edge + 1, :] = jnp.full((1, LANES), nbr_ref[edge % EDGES, face], jnp.int32)
    put_strips(fields_ref, nbr_ref, face, send_ref, table)
    keep.wait()


def laplace(fields, metric, table, parts):
    flux_xx, flux_xy, flux_yy = metric
    count = flux_xx.shape[0]
    grad_x, grad_y = gradient(stacked(fields), table, parts)
    flux = []
    for ch in range(3):
        part = slice(count * ch, count * ch + count)
        flux.append(
            stacked(
                [
                    flux_xx * grad_x[part] + flux_xy * grad_y[part],
                    flux_xy * grad_x[part] + flux_yy * grad_y[part],
                ],
                1,
            )
        )
    high, mid, low = split(stacked(flux))
    terms = [(high, 0), (mid, 0), (high, 1), (low, 0), (mid, 1), (high, 2)][: 3 * parts - 3]
    right = [table.part("spread", n, 2 * LANES) for _, n in terms]
    sums = dot_halves(stacked([part for part, _ in terms], 1), stacked(right))
    return [
        assembled(sums[count * ch : count * ch + count, :LANES], sums[count * ch : count * ch + count, LANES:])
        for ch in range(3)
    ]


def second_kernel(which_ref, got_ref, fields_ref, table_ref, out_ref, total_ref):
    table = Table(table_ref, 1)
    core = lax.axis_index("fy") % 2
    ring_fields, seams = ring_of(which_ref, got_ref, table)
    metric = [
        stacked([fields_ref[ROWS * k : ROWS * k + ROWS, :], ring_fields[k]]) for k in range(4, 7)
    ]
    total_ref[...] = fields_ref[: 4 * ROWS, :]
    ring = join(total_ref, ring_fields[:4], 4, seams)
    share = 1.0 / stacked([total_ref[3 * ROWS : 4 * ROWS, :], ring[3]])
    fields = [
        stacked([total_ref[ROWS * ch : ROWS * ch + ROWS, :], ring[ch]]) * share for ch in range(3)
    ]
    sectioned = [field[:ROWS] for field in fields]
    for step in range(2):
        sums = laplace(fields, metric, table, 3 - step)
        for ch in range(3):
            total_ref[ROWS * ch : ROWS * ch + ROWS, :] = sums[ch][:ROWS]
        ring = [field[ROWS:] for field in sums]
        ends = [placed_ends(part) for part in ends_meet(ring, 3, table)] if step == 0 else None
        ring = join(total_ref, ring, 3, ends)
        if step == 0:
            fields = [
                stacked([total_ref[ROWS * ch : ROWS * ch + ROWS, :], ring[ch]]) * share
                for ch in range(3)
            ]
    for ch in range(3):
        second_lap = total_ref[ROWS * ch : ROWS * ch + ROWS, :] * share[:ROWS]
        updated = sectioned[ch] - hyper_coeff * second_lap
        for x in range(4):
            even, odd = updated[32 * x : 32 * x + 16], updated[32 * x + 16 : 32 * x + 32]
            out_ref[16 * x : 16 * x + 16, 0, LANES * ch : LANES * ch + LANES] = jnp.where(
                core == 0, even, odd
            )


def unpack_kernel(got_ref, out_ref):
    levels = got_ref[...]
    columns = stacked([levels[:, 0, LANES * ch : LANES * ch + LANES] for ch in range(3)])
    out_ref[...] = jnp.transpose(columns)


def f32(*shape):
    return jax.ShapeDtypeStruct(shape, jnp.float32)


def near(*shape):
    return pltpu.VMEM(shape, jnp.float32)


def kept(table):
    return pltpu.VMEM(table.shape, jnp.bfloat16)


def held(values):
    return pltpu.with_memory_space_constraint(values, pltpu.VMEM)


VMEM = pl.BlockSpec(memory_space=pltpu.VMEM)
ANY = pl.BlockSpec(memory_space=pl.ANY)


def call(kernel, outs, ins, scratch=(), name=None):
    return pl.pallas_call(
        kernel,
        out_shape=outs,
        in_specs=ins,
        out_specs=jax.tree.map(lambda _: VMEM, outs),
        scratch_shapes=scratch,
        name=name,
    )


def level_groups():
    return [
        [(8 * face + 2 * x + core) * 16 + fx for x in range(4) for fx in range(16)]
        for face in range(FACES)
        for core in range(2)
    ]


def per_device(state, jacobian, metric_diag, metric_cross, coriolis, nbr_face, nbr_edge):
    axes = ("face", "fy", "fx")
    groups = level_groups()
    tables = [jnp.asarray(table) for table in TABLES]
    packed = call(pack_kernel, near(512, LANES), [VMEM] * 5, name="pack")(
        state.reshape(128, 192),
        jacobian[0].T,
        metric_diag[:, 0].transpose(0, 2, 1),
        metric_cross[0].T,
        coriolis[0].T,
    )
    own = lax.all_to_all(
        packed.reshape(64, 8, LANES), axes, 0, 0, axis_index_groups=groups, tiled=True
    )
    other = lax.ppermute(own, "fy", [(i, i ^ 1) for i in range(8)])
    table, half = call(
        early_kernel,
        [kept(TABLES[0]), near(7 * 64, LANES)],
        [VMEM, ANY],
        [pltpu.SemaphoreType.DMA, pltpu.SemaphoreType.DMA],
        name="early",
    )(held(own.reshape(512, LANES)), tables[0])
    fields, send, which, table = call(
        first_kernel,
        [
            near(7 * ROWS, LANES),
            near(SLOT * FACES, LANES),
            pltpu.VMEM((8, LANES), jnp.int32),
            kept(TABLES[1]),
        ],
        [ANY] + [VMEM] * 3 + [ANY],
        [
            pltpu.SMEM((EDGES, FACES), jnp.int32),
            pltpu.SemaphoreType.DMA,
            pltpu.SemaphoreType.DMA,
        ],
        name="first",
    )(
        nbr_face.T,
        held(half),
        held(other.reshape(512, LANES)),
        held(table),
        tables[1],
    )
    got = lax.all_to_all(send.reshape(FACES, SLOT, LANES), "face", 0, 0, tiled=True)
    updated = call(
        second_kernel,
        near(64, 1, 3 * LANES),
        [VMEM] * 4,
        [pltpu.VMEM((4 * ROWS, LANES), jnp.float32)],
        name="second",
    )(held(which), held(got.reshape(SLOT * FACES, LANES)), held(fields), held(table))
    back = lax.all_to_all(
        updated, axes, 0, 0, axis_index_groups=groups, tiled=True
    )
    nodes = call(unpack_kernel, f32(128, 192), [VMEM], name="unpack")(
        held(back)
    )
    return nodes.reshape(1, 16, 8, 192)


def solution(mesh):
    return jax.shard_map(
        per_device,
        mesh=mesh,
        in_specs=(
            P("face", "fy", "fx", None),
            P("face", "fy", "fx"),
            P(None, "face", "fy", "fx"),
            P("face", "fy", "fx"),
            P("face", "fy", "fx"),
            P(),
            P(),
        ),
        out_specs=P("face", "fy", "fx", None),
        check_vma=False,
    )
```

```python
import jax
import jax.numpy as jnp
import ml_dtypes
import numpy as np
from jax import lax
from jax.experimental import pallas as pl
from jax.experimental.pallas import tpu as pltpu
from jax.sharding import PartitionSpec as P

time_step = 0.05
hyper_coeff = 0.0005

FACES = 6
ROWS = 128
LANES = 128
EDGES = 4
RING_ROWS = 32
ALL_ROWS = ROWS + RING_ROWS
SLOT = 56
ENDS = ("S0", "S15", "N0", "N15", "E0", "E7", "W0", "W7")
END_ROWS = (0, 15, 0, 15, 16, 23, 24, 31)
MEETS = (6, 4, 7, 5, 1, 3, 0, 2)
TURNS = (1, -1, -1, 1, 1, -1, -1, 1)


def deriv_table():
    gll_nodes = np.array([-1.0, -1.0 / np.sqrt(5.0), 1.0 / np.sqrt(5.0), 1.0])
    bary_weights = np.ones(4)
    for j in range(4):
        for m in range(4):
            if m != j:
                bary_weights[j] = bary_weights[j] / (gll_nodes[j] - gll_nodes[m])
    matrix = np.zeros((4, 4))
    for i in range(4):
        for j in range(4):
            if i != j:
                matrix[i, j] = bary_weights[j] / bary_weights[i] / (gll_nodes[i] - gll_nodes[j])
        matrix[i, i] = -np.sum(matrix[i])
    return matrix


def in_parts(matrix):
    rest = np.asarray(matrix, np.float64)
    parts = []
    for _ in range(3):
        part = rest.astype(ml_dtypes.bfloat16)
        parts.append(part)
        rest = rest - part.astype(np.float64)
    return parts


def face_node(edge, depth, k):
    row, col = ((depth, k), (k, 127 - depth), (127 - depth, 127 - k), (127 - k, depth))[edge]
    return row // 16, col // 8, 8 * (row % 16) + col % 8


def ring_node(edge, depth, k):
    if edge == 1:
        return k // 16, 8 * (k % 16) + depth
    row = 127 - k
    return row // 16, 8 * (row % 16) + 7 - depth


def end_lane(end, depth):
    return {
        "S0": 8 * (15 - depth),
        "S15": 8 * (15 - depth) + 7,
        "N0": 8 * depth,
        "N15": 8 * depth + 7,
        "E0": depth,
        "E7": 120 + depth,
        "W0": 7 - depth,
        "W7": 127 - depth,
    }[end]


def tables():
    deriv = deriv_table()
    along_x = np.kron(np.eye(32), deriv.T)
    along_y = np.kron(np.kron(np.eye(4), deriv.T), np.eye(8))
    lane = np.arange(LANES)
    r, c = lane // 8, lane % 8
    weights = np.array([1.0, 5.0, 5.0, 1.0]) / 6.0
    within = np.eye(LANES)
    across = np.zeros((LANES, LANES))
    for l in range(LANES):
        if c[l] in (3, 4):
            within[l, l + 1 if c[l] == 3 else l - 1] = 1.0
        if c[l] == 7:
            across[l, l - 7] = 1.0
        if c[l] == 0:
            across[l, l + 7] = 1.0
    both = np.concatenate([within, across], 1)
    gradient = in_parts(np.concatenate([along_x, along_y], 1))
    weighted = np.diag(weights[r % 4] * weights[c % 4])
    spread = in_parts(np.concatenate([along_x @ weighted @ both, along_y @ weighted @ both], 0))

    out, out_rows, into, into_rows = [], [], [], []
    for edge in (1, 3):
        out.append(np.zeros((2, LANES, LANES)))
        out_rows.append(np.zeros((LANES, LANES)))
        into.append(np.zeros((2, LANES, LANES)))
        into_rows.append(np.zeros((LANES, LANES)))
        for k in range(128):
            j, i = k // 8, k % 8
            j2, i2 = (127 - k) // 8, (127 - k) % 8
            for depth in range(8):
                fy, _, at = face_node(edge, depth, k)
                out[-1][j % 2, at, 8 * depth + i] = 1.0
                ring_fy, ring_at = ring_node(edge, depth, k)
                into[-1][j2 % 2, 8 * depth + i2, ring_at] = 1.0
                for field in range(8):
                    out_rows[-1][16 * field + j, 64 * (j % 2) + 8 * field + fy] = 1.0
                    into_rows[-1][64 * (j2 % 2) + 8 * field + ring_fy, 16 * field + j2] = 1.0
    take = np.zeros((LANES, LANES))
    give = np.zeros((LANES, LANES))
    masks = np.zeros((32, 2 * LANES))
    for t, end in enumerate(ENDS):
        for depth in range(8):
            take[end_lane(end, depth), 8 * t + depth] = 1.0
            give[8 * t + depth, end_lane(ENDS[MEETS[t]], depth)] = 1.0
            masks[t, end_lane(end, depth)] = 1.0
            masks[8 + t, 8 * t + depth] = 1.0
            masks[16 + t, 8 * MEETS[t] + depth] = 1.0
        masks[24 + t] = TURNS[t]

    def pair(left, right):
        return np.concatenate([left, right], 1)

    reverse = pair(np.eye(LANES)[::-1], np.kron(np.eye(8), np.eye(16)[::-1]))
    groups = (
        {
            "gradient": np.concatenate(gradient, 0),
            "both": both,
            "east_out": pair(*out[0]),
            "west_out": pair(*out[1]),
            "out_rows": pair(*out_rows),
            "reverse": reverse,
        },
        {
            "gradient": np.concatenate(gradient, 0),
            "spread": np.concatenate(spread, 0),
            "east_in": pair(*into[0]),
            "west_in": pair(*into[1]),
            "in_rows": pair(*into_rows),
            "reverse": reverse,
            "ends": pair(take, give),
            "masks": masks,
        },
    )
    arrays, places = [], []
    for group in groups:
        start = 0
        places.append({})
        for name, matrix in group.items():
            places[-1][name] = (start, start + matrix.shape[0])
            start += matrix.shape[0]
        arrays.append(np.concatenate([m.astype(ml_dtypes.bfloat16) for m in group.values()], 0))
    return arrays, places


TABLES, PLACES = tables()


class Table:
    def __init__(self, ref, which):
        self.ref, self.places = ref, PLACES[which]

    def whole(self, name):
        start, end = self.places[name]
        return self.ref[start:end, :]

    def left(self, name):
        start, end = self.places[name]
        return self.ref[start:end, :LANES]

    def right(self, name):
        start, end = self.places[name]
        return self.ref[start:end, LANES:]

    def part(self, name, n, rows):
        start = self.places[name][0] + n * rows
        return self.ref[start : start + rows, :]


def roll(values, shift, axis):
    return pltpu.roll(values, shift % values.shape[axis], axis)


def iota(shape, dim):
    return lax.broadcasted_iota(jnp.int32, shape, dim)


def dot(a, b):
    return jnp.dot(a, b, preferred_element_type=jnp.float32)


def dot_halves(a, b):
    half = a.shape[0] // 32 * 16
    return jnp.concatenate([dot(a[:half], b), dot(a[half:], b)], axis=0)


def stacked(parts, axis=0):
    return jnp.concatenate(parts, axis=axis)


def split(values):
    high = values.astype(jnp.bfloat16)
    rest = values - high.astype(jnp.float32)
    mid = rest.astype(jnp.bfloat16)
    return high, mid, (rest - mid.astype(jnp.float32)).astype(jnp.bfloat16)


def gradient(values, table, parts=3):
    high, mid, low = split(values)
    left = [high, mid, high, mid, low, high][: 2 * parts]
    right = [table.part("gradient", n, LANES) for n in (0, 0, 1, 1, 0, 2)[: 2 * parts]]
    both = dot_halves(stacked(left, 1), stacked(right))
    return both[:, :LANES], both[:, LANES:]


def mass_weight():
    lane = iota((1, LANES), 1)
    r, c = lane // 8 % 4, lane % 4
    along_y = jnp.where((r == 0) | (r == 3), 1.0 / 6.0, 5.0 / 6.0)
    return along_y * jnp.where((c == 0) | (c == 3), 1.0 / 6.0, 5.0 / 6.0)


def assembled(inner, outer):
    shape = inner.shape
    row = iota(shape, 0)
    lane = iota(shape, 1)
    c = lane % 8
    r = lane // 8
    here = row < ROWS + 16
    from_before = here & (c == 0) & (row % 16 > 0)
    from_after = here & (c == 7) & (row % 16 < 15)
    summed = (
        inner
        + jnp.where(from_before, roll(outer, 1, 0), 0.0)
        + jnp.where(from_after, roll(outer, -1, 0), 0.0)
    )
    above = roll(summed, 8, 1)
    below = roll(summed, -8, 1)
    total = (
        summed
        + jnp.where((r % 4 == 0) & (r > 0), above, 0.0)
        + jnp.where((r % 4 == 3) & (r < 15), below, 0.0)
    )
    edge_rows = jnp.zeros((16, LANES), jnp.float32)
    above_block = [edge_rows, above[: ROWS - 16]]
    below_block = [below[16:ROWS], edge_rows]
    if shape[0] > ROWS:
        sides = slice(ROWS + 16, ROWS + 32)
        fy = iota((16, LANES), 0) % 8
        above_block += [edge_rows, jnp.where(fy > 0, roll(above[sides], 1, 0), 0.0)]
        below_block += [edge_rows, jnp.where(fy < 7, roll(below[sides], -1, 0), 0.0)]
    return (
        total
        + jnp.where(r == 0, stacked(above_block), 0.0)
        + jnp.where(r == 15, stacked(below_block), 0.0)
    )


def rim_rows(edge, base=0):
    if edge == 0:
        return pl.ds(base, 16)
    if edge == 1:
        return pl.ds(base + 15, 8, 16)
    if edge == 2:
        return pl.ds(base + 112, 16)
    return pl.ds(base, 8, 16)


def turned(u, v, quarter):
    quarter = quarter % 4
    if quarter == 0:
        return u, v
    if quarter == 1:
        return -v, u
    if quarter == 2:
        return -u, -v
    return v, -u


def ends_meet(ring, channels, table):
    ends = stacked(
        [ring[ch][row : row + 1] for ch in range(channels) for row in END_ROWS]
    )
    masks = table.left("masks").astype(jnp.float32)
    own = stacked([masks[0:8]] * channels)
    taken = dot(stacked(split(ends * own), 1), stacked([table.left("ends")] * 3))
    lines = []
    for ch in range(channels):
        line = jnp.sum(taken[8 * ch : 8 * ch + 8] * masks[8:16], axis=0, keepdims=True)
        lines.append(line * masks[16:24])
    given = dot(stacked(split(stacked(lines)), 1), stacked([table.right("ends")] * 3))
    given = [given[8 * ch : 8 * ch + 8] for ch in range(channels)]
    sense = masks[24:32]
    return [-sense * given[1], sense * given[0], *given[2:]]


def placed_ends(ends):
    block, fy = iota((16, LANES), 0), iota((8, LANES), 0)
    parts = []
    for side, position, count in ((0, block, 16), (1, block, 16), (2, fy, 8), (3, fy, 8)):
        first, last = ends[2 * side : 2 * side + 1], ends[2 * side + 1 : 2 * side + 2]
        parts.append(
            jnp.where(position == 0, first, jnp.where(position == count - 1, last, 0.0))
        )
    return stacked([parts[0] + parts[1], parts[2], parts[3]])


def join(face_ref, ring, channels, ends=None):
    totals = []
    lane = iota((16, LANES), 1)
    lane_8 = iota((8, LANES), 1)
    for ch in range(channels):
        outer, east, west = ring[ch][0:16], ring[ch][16:24], ring[ch][24:32]
        rows = [rim_rows(edge, ROWS * ch) for edge in range(EDGES)]
        if ends is not None:
            rims = [
                jnp.where(
                    lane // 8 == 15,
                    roll(face_ref[rows[0], :], -8, 1),
                    jnp.where(lane // 8 == 0, roll(face_ref[rows[2], :], 8, 1), 0.0),
                ),
                jnp.where(lane_8 % 8 == 0, roll(face_ref[rows[1], :], -7, 1), 0.0),
                jnp.where(lane_8 % 8 == 7, roll(face_ref[rows[3], :], 7, 1), 0.0),
            ]
            totals.append(ring[ch] + ends[ch] + stacked(rims))
        from_south = jnp.where(lane // 8 == 0, roll(outer, 8, 1), 0.0)
        from_north = jnp.where(lane // 8 == 15, roll(outer, -8, 1), 0.0)
        from_east = jnp.where(lane_8 % 8 == 7, roll(east, 7, 1), 0.0)
        from_west = jnp.where(lane_8 % 8 == 0, roll(west, -7, 1), 0.0)
        for edge, part in enumerate((from_south, from_east, from_north, from_west)):
            face_ref[rows[edge], :] = face_ref[rows[edge], :] + part
    return totals


def pack_kernel(state_ref, jac_ref, diag_ref, cross_ref, cor_ref, out_ref):
    turned_state = jnp.transpose(state_ref[...])
    for part in range(3):
        out_ref[pl.ds(part, 64, 8), :] = turned_state[64 * part : 64 * part + 64]
    spread = jnp.where(iota((16, LANES), 1) // 8 == iota((16, LANES), 0), 1.0, 0.0)
    mask = jnp.where(iota((8, LANES), 1) % 8 == iota((8, LANES), 0), 1.0, 0.0)
    fields = [jac_ref[...], diag_ref[0], diag_ref[1], cross_ref[...], cor_ref[...]]
    lines = jnp.dot(
        stacked(fields),
        spread,
        precision=lax.Precision.HIGHEST,
        preferred_element_type=jnp.float32,
    )
    for k in range(5):
        line = jnp.sum(lines[8 * k : 8 * k + 8] * mask, axis=0, keepdims=True)
        out_ref[pl.ds(3 + k, 64, 8), :] = jnp.broadcast_to(line, (64, LANES))


def weighted_raw(blocks_ref, table):
    u, v, t, volume, m_xx, m_yy, m_xy, planet = [
        blocks_ref[pl.ds(k, 64, 8), :] for k in range(8)
    ]
    contra_u = m_xx * u + m_xy * v
    contra_v = m_xy * u + m_yy * v
    energy = 0.5 * (u * contra_u + v * contra_v) + t
    grad_x, grad_y = gradient(stacked([u, v, t, energy]), table)
    dy_u, dx_v = grad_y[:64], grad_x[64:128]
    dx_t, dy_t = grad_x[128:192], grad_y[128:192]
    dx_e, dy_e = grad_x[192:], grad_y[192:]
    absolute = dx_v - dy_u + planet * volume
    mass = mass_weight() * volume
    raw_u = u + time_step * (absolute * contra_v - dx_e)
    raw_v = v + time_step * (-absolute * contra_u - dy_e)
    raw_t = t - time_step * (contra_u * dx_t + contra_v * dy_t)
    metric = [volume * m_xx, volume * m_xy, volume * m_yy]
    return [mass * raw_u, mass * raw_v, mass * raw_t, mass, *metric]


def early_kernel(own_ref, table_from, table_ref, half_ref, sem, late_sem):
    rows = PLACES[0]["gradient"][1]
    soon = pltpu.make_async_copy(table_from.at[:rows], table_ref.at[:rows], sem)
    late = pltpu.make_async_copy(table_from.at[rows:], table_ref.at[rows:], late_sem)
    soon.start()
    late.start()
    soon.wait()
    for k, field in enumerate(weighted_raw(own_ref, Table(table_ref, 0))):
        half_ref[64 * k : 64 * k + 64, :] = field
    late.wait()


def reversed_blocks(rows, table, product):
    parts = stacked([part.astype(jnp.float32) for part in split(rows)]).astype(jnp.bfloat16)
    moved = product(parts, table.left("reverse"))
    count = rows.shape[0]
    moved = stacked([moved[n * count : n * count + count] for n in range(3)], 1)
    moved = dot(table.right("reverse"), moved.astype(jnp.bfloat16))
    return moved[:, :LANES] + moved[:, LANES : 2 * LANES] + moved[:, 2 * LANES :]


def strip_of(edge, fields_ref, table):
    rows = [fields_ref[rim_rows(edge, ROWS * k), :] for k in range(7)]
    rows = stacked([*rows, jnp.zeros_like(rows[0])])
    if edge == 0:
        return rows
    if edge == 2:
        return reversed_blocks(rows, table, dot)
    name = "east" if edge == 1 else "west"
    moved = dot(stacked(split(rows)), table.whole(name + "_out"))
    halves = stacked([moved[:, :LANES], moved[:, LANES:]], 0)
    moved = stacked(
        [stacked([halves[64 * n : 64 * n + 64], halves[192 + 64 * n : 256 + 64 * n]]) for n in range(3)],
        1,
    )
    order = table.left("out_rows") if edge == 1 else table.right("out_rows")
    moved = dot(order, moved.astype(jnp.bfloat16))
    return moved[:, :LANES] + moved[:, LANES : 2 * LANES] + moved[:, 2 * LANES :]


def put_strips(fields_ref, nbr_ref, face, send_ref, table):
    near = iota((16, LANES), 1) < 64
    strips = [strip_of(edge, fields_ref, table) for edge in range(EDGES)]
    for edge, rows in enumerate(strips):
        u, v, t, mass, flux_xx, flux_xy, flux_yy = [rows[16 * k : 16 * k + 16] for k in range(7)]
        u, v = turned(u, v, -edge)
        if edge % 2:
            flux_xx, flux_xy, flux_yy = flux_yy, -flux_xy, flux_xx
        slot = [
            jnp.where(near, low, roll(high, 64, 1))
            for low, high in ((u, v), (t, mass), (flux_xx, flux_xy))
        ]
        slot.append(jnp.where(near[:8], flux_yy[:8], roll(flux_yy[8:], 64, 1)))
        start = pl.multiple_of(SLOT * nbr_ref[edge, face], 8)
        send_ref[pl.ds(start, SLOT), :] = stacked(slot)


def ring_of(which_ref, got_ref, table):
    lane = iota((16, LANES), 1)
    block = iota((16, LANES), 0)
    near = lane < 64
    first = (block == 0) & (lane % 8 == 0) & (lane >= 8)
    last = (block == 15) & (lane % 8 == 7) & (lane >= 8)
    got, strips, seams = [], [], []
    for edge in range(EDGES):
        slot = got_ref[:SLOT, :]
        which = jnp.broadcast_to(which_ref[edge : edge + 1, :], (SLOT, LANES))
        for other in range(1, FACES):
            slot = jnp.where(which == other, got_ref[SLOT * other : SLOT * other + SLOT, :], slot)
        fields = []
        for n in range(3):
            rows = slot[16 * n : 16 * n + 16]
            fields += [jnp.where(near, rows, 0.0), jnp.where(near, roll(rows, 64, 1), 0.0)]
        rows = slot[48:56]
        fields.append(stacked([rows, roll(rows, 64, 1)]))
        fields[6] = jnp.where(near, fields[6], 0.0)
        got.append(fields)
    for edge in range(EDGES):
        fields = list(got[edge])
        corner = jnp.zeros((16, LANES), jnp.float32)
        for ch in range(4):
            after, before = got[(edge + 1) % EDGES][ch], got[(edge - 1) % EDGES][ch]
            at_first = (block == 0) & (lane == 8 * ch)
            at_last = (block == 15) & (lane == 8 * ch + 7)
            corner = jnp.where(at_first, roll(after[15:16], 8 * ch - 7, 1), corner)
            corner = jnp.where(at_last, roll(before[0:1], 8 * ch + 7, 1), corner)
            fields[ch] = (
                fields[ch]
                + jnp.where(first, roll(after[15:16], -7, 1), 0.0)
                + jnp.where(last, roll(before[0:1], 7, 1), 0.0)
            )
        rows = stacked([*fields, corner])
        count = 16
        if edge == 0:
            rows = reversed_blocks(rows, table, dot_halves)
        elif edge % 2:
            name = "east" if edge == 1 else "west"
            order = table.left("in_rows") if edge == 1 else table.right("in_rows")
            moved = dot(order, stacked(split(rows), 1))
            moved = stacked([moved[:64], moved[64:]], 1)
            into = [table.left(name + "_in")] * 3 + [table.right(name + "_in")] * 3
            rows = dot(moved.astype(jnp.bfloat16), stacked(into))
            count = 8
        fields = [rows[count * k : count * k + count] for k in range(7)]
        corner = rows[7 * count : 8 * count]
        low, high = ((120, 127), (0, 120), (0, 7), (7, 127))[edge]
        position, at = iota((count, LANES), 0), iota((count, LANES), 1)
        here = ((position == 0) & (at == low)) | ((position == count - 1) & (at == high))
        step = (8, -1, -8, 1)[edge]
        seam = [jnp.where(here, roll(corner, step * ch, 1), 0.0) for ch in range(4)]
        seams.append([*turned(seam[0], seam[1], edge + 2), *seam[2:]])
        fields[0], fields[1] = turned(fields[0], fields[1], edge + 2)
        if edge % 2:
            fields[4], fields[5], fields[6] = fields[6], -fields[5], fields[4]
        strips.append(fields)
    def around(sides, k):
        south, east, north, west = [side[k] for side in sides]
        return stacked([south + north, east, west])

    return [around(strips, k) for k in range(7)], [around(seams, ch) for ch in range(4)]


def first_kernel(
    nbr_from, half_ref, other_ref, table_ref, later_ref,
    fields_ref, send_ref, which_ref, kept_ref, nbr_ref, nbr_sem, sem,
):
    fetch = pltpu.make_async_copy(nbr_from, nbr_ref, nbr_sem)
    fetch.start()
    keep = pltpu.make_async_copy(later_ref, kept_ref, sem)
    keep.start()
    table = Table(table_ref, 0)
    core = lax.axis_index("fy") % 2
    face = lax.axis_index("face")
    fields = []
    for k, other in enumerate(weighted_raw(other_ref, table)):
        own = half_ref[64 * k : 64 * k + 64, :]
        even = jnp.where(core == 0, own, other)
        odd = jnp.where(core == 0, other, own)
        pieces = []
        for x in range(4):
            pieces += [even[16 * x : 16 * x + 16], odd[16 * x : 16 * x + 16]]
        fields.append(stacked(pieces))
    values = stacked(fields[:4])
    sums = dot_halves(stacked(split(values), 1), stacked([table.whole("both")] * 3))
    for ch in range(4):
        part = slice(ROWS * ch, ROWS * ch + ROWS)
        fields_ref[part, :] = assembled(sums[part, :LANES], sums[part, LANES:])
    for k in range(4, 7):
        fields_ref[ROWS * k : ROWS * k + ROWS, :] = fields[k]
    fetch.wait()
    for edge in range(8):
        which_ref[edge : edge + 1, :] = jnp.full((1, LANES), nbr_ref[edge % EDGES, face], jnp.int32)
    put_strips(fields_ref, nbr_ref, face, send_ref, table)
    keep.wait()


def laplace(fields, metric, table, parts):
    flux_xx, flux_xy, flux_yy = metric
    count = flux_xx.shape[0]
    grad_x, grad_y = gradient(stacked(fields), table, parts)
    flux = []
    for ch in range(3):
        part = slice(count * ch, count * ch + count)
        flux.append(
            stacked(
                [
                    flux_xx * grad_x[part] + flux_xy * grad_y[part],
                    flux_xy * grad_x[part] + flux_yy * grad_y[part],
                ],
                1,
            )
        )
    high, mid, low = split(stacked(flux))
    terms = [(high, 0), (mid, 0), (high, 1), (low, 0), (mid, 1), (high, 2)][: 3 * parts - 3]
    right = [table.part("spread", n, 2 * LANES) for _, n in terms]
    sums = dot_halves(stacked([part for part, _ in terms], 1), stacked(right))
    return [
        assembled(sums[count * ch : count * ch + count, :LANES], sums[count * ch : count * ch + count, LANES:])
        for ch in range(3)
    ]


def second_kernel(which_ref, got_ref, fields_ref, table_ref, out_ref, total_ref):
    table = Table(table_ref, 1)
    core = lax.axis_index("fy") % 2
    ring_fields, seams = ring_of(which_ref, got_ref, table)
    metric = [
        stacked([fields_ref[ROWS * k : ROWS * k + ROWS, :], ring_fields[k]]) for k in range(4, 7)
    ]
    total_ref[...] = fields_ref[: 4 * ROWS, :]
    ring = join(total_ref, ring_fields[:4], 4, seams)
    share = 1.0 / stacked([total_ref[3 * ROWS : 4 * ROWS, :], ring[3]])
    fields = [
        stacked([total_ref[ROWS * ch : ROWS * ch + ROWS, :], ring[ch]]) * share for ch in range(3)
    ]
    sectioned = [field[:ROWS] for field in fields]
    for step in range(2):
        sums = laplace(fields, metric, table, 3 - step)
        for ch in range(3):
            total_ref[ROWS * ch : ROWS * ch + ROWS, :] = sums[ch][:ROWS]
        ring = [field[ROWS:] for field in sums]
        ends = [placed_ends(part) for part in ends_meet(ring, 3, table)] if step == 0 else None
        ring = join(total_ref, ring, 3, ends)
        if step == 0:
            fields = [
                stacked([total_ref[ROWS * ch : ROWS * ch + ROWS, :], ring[ch]]) * share
                for ch in range(3)
            ]
    for ch in range(3):
        second_lap = total_ref[ROWS * ch : ROWS * ch + ROWS, :] * share[:ROWS]
        updated = sectioned[ch] - hyper_coeff * second_lap
        for x in range(4):
            even, odd = updated[32 * x : 32 * x + 16], updated[32 * x + 16 : 32 * x + 32]
            out_ref[16 * x : 16 * x + 16, 0, LANES * ch : LANES * ch + LANES] = jnp.where(
                core == 0, even, odd
            )


def unpack_kernel(got_ref, out_ref):
    levels = got_ref[...]
    columns = stacked([levels[:, 0, LANES * ch : LANES * ch + LANES] for ch in range(3)])
    out_ref[...] = jnp.transpose(columns)


def f32(*shape):
    return jax.ShapeDtypeStruct(shape, jnp.float32)


def near(*shape):
    return pltpu.VMEM(shape, jnp.float32)


def kept(table):
    return pltpu.VMEM(table.shape, jnp.bfloat16)


def held(values):
    return pltpu.with_memory_space_constraint(values, pltpu.VMEM)


VMEM = pl.BlockSpec(memory_space=pltpu.VMEM)
ANY = pl.BlockSpec(memory_space=pl.ANY)


def call(kernel, outs, ins, scratch=(), name=None):
    return pl.pallas_call(
        kernel,
        out_shape=outs,
        in_specs=ins,
        out_specs=jax.tree.map(lambda _: VMEM, outs),
        scratch_shapes=scratch,
        name=name,
    )


def level_groups():
    return [
        [(8 * face + 2 * x + core) * 16 + fx for x in range(4) for fx in range(16)]
        for face in range(FACES)
        for core in range(2)
    ]


def per_device(state, jacobian, metric_diag, metric_cross, coriolis, nbr_face, nbr_edge):
    axes = ("face", "fy", "fx")
    groups = level_groups()
    tables = [jnp.asarray(table) for table in TABLES]
    packed = call(pack_kernel, near(512, LANES), [VMEM] * 5, name="pack")(
        state.reshape(128, 192),
        jacobian[0].T,
        metric_diag[:, 0].transpose(0, 2, 1),
        metric_cross[0].T,
        coriolis[0].T,
    )
    own = lax.all_to_all(
        packed.reshape(64, 8, LANES), axes, 0, 0, axis_index_groups=groups, tiled=True
    )
    other = lax.ppermute(own, "fy", [(i, i ^ 1) for i in range(8)])
    table, half = call(
        early_kernel,
        [kept(TABLES[0]), near(7 * 64, LANES)],
        [VMEM, ANY],
        [pltpu.SemaphoreType.DMA, pltpu.SemaphoreType.DMA],
        name="early",
    )(held(own.reshape(512, LANES)), tables[0])
    fields, send, which, table = call(
        first_kernel,
        [
            near(7 * ROWS, LANES),
            near(SLOT * FACES, LANES),
            pltpu.VMEM((8, LANES), jnp.int32),
            kept(TABLES[1]),
        ],
        [ANY] + [VMEM] * 3 + [ANY],
        [
            pltpu.SMEM((EDGES, FACES), jnp.int32),
            pltpu.SemaphoreType.DMA,
            pltpu.SemaphoreType.DMA,
        ],
        name="first",
    )(
        nbr_face.T,
        held(half),
        held(other.reshape(512, LANES)),
        held(table),
        tables[1],
    )
    got = lax.all_to_all(send.reshape(FACES, SLOT, LANES), "face", 0, 0, tiled=True)
    updated = call(
        second_kernel,
        near(64, 1, 3 * LANES),
        [VMEM] * 4,
        [pltpu.VMEM((4 * ROWS, LANES), jnp.float32)],
        name="second",
    )(held(which), held(got.reshape(SLOT * FACES, LANES)), held(fields), held(table))
    back = lax.all_to_all(
        updated, axes, 0, 0, axis_index_groups=groups, tiled=True
    )
    nodes = call(unpack_kernel, f32(128, 192), [VMEM], name="unpack")(
        held(back)
    )
    return nodes.reshape(1, 16, 8, 192)


def solution(mesh):
    return jax.shard_map(
        per_device,
        mesh=mesh,
        in_specs=(
            P("face", "fy", "fx", None),
            P("face", "fy", "fx"),
            P(None, "face", "fy", "fx"),
            P("face", "fy", "fx"),
            P("face", "fy", "fx"),
            P(),
            P(),
        ),
        out_specs=P("face", "fy", "fx", None),
        check_vma=False,
    )
```
